512 devices in a mesh: band: 16 (over z), ga: 32 (over y, x, core).
Axes of the slice: x: 4, y: 4, z: 16, core: 2. Of those that a mesh axis runs over, the one named last changes fastest.
Arguments:
- waves: bfloat16 [2, 512, 32768], P(None, 'band', 'ga'), may hold values from -6 to 6
- occupations: float32 [512], P('band'), may hold values from 0.000390625 to 0.0078125
- beta_table: float32 [72, 32768], P(None, 'ga'), may hold values from -0.0234375 to 0.0234375
- wave_miller: int32 [3, 32768], P(None, 'ga'), may hold values from 0 to 223
- atom_kinds: int32 [256], replicated, may hold values from 0 to 3
- atom_sites: int32 [3, 256], replicated, may hold values from 0 to 223
- aug_table: bfloat16 [684, 917504], P(None, ('band', 'ga')), may hold values from -0.00015258789 to 0.00015258789
- stick_columns: int32 [4096], P(('band', 'ga')), may hold values from -1 to 3599, as said below
Outputs:
- density: float32 [2, 224, 240, 240], P(None, 'ga', 'band')
The draws below stay inside these ranges and needn't reach their ends.
Inputs may be any that keep to these rules, and one draw needn't show every extreme that they name: `stick_columns`: entry t is a slot of the device at place t // 8 in band-major order, of band index t // 256. -1 marks an empty slot; otherwise the entry c names the column x = (t // 256) * 15 + c // 240, y = c mod 240. Live columns of one band index are distinct. On each device the live slots come first and at least one is live; in each band index some device has all 8 slots live.
All inputs are finite; a program needn't handle non-finite values.
Results may differ from the reference program's by a relative error of at most 0.0035.
Values sent between devices are 32-bit elements; how exact they have to be, the bound alone decides.
A program may use at most 64 MiB of HBM per device.

```python
import math
import jax
import jax.numpy as jnp
import numpy as np
from jax import lax

NX = 240
NY = 240
NZ = 224
NH = 18
PAIRS = 171
SPECIES = 4
ATOMS = 256
BANDS = 512
GW = 32768
STK = 8
STICKS = 4096
BLOCK_STICKS = 256
NXB = 15


def draw_stick_columns(key, part):
    groups = STICKS // BLOCK_STICKS
    devices = BLOCK_STICKS // STK
    group_keys = jax.random.split(jax.random.fold_in(key, 11), groups)

    def one_group(group_key):
        perm_key, count_key, full_key = jax.random.split(group_key, 3)
        chosen = jax.random.permutation(perm_key, NXB * NY)[:BLOCK_STICKS].astype(jnp.int32).reshape(devices, STK)
        live_count = jax.random.randint(count_key, (devices,), 1, STK // 2 + 1)
        fullest = jax.random.randint(full_key, (), 0, devices)
        live_count = jnp.where(jnp.arange(devices) == fullest, STK, live_count)
        slot_index = jnp.arange(STK)[None, :]
        return jnp.where(slot_index < live_count[:, None], chosen, -1).reshape(-1)
    return jax.vmap(one_group)(group_keys).reshape(-1).astype(jnp.int32)


def place_ends(values, own_key, least, high):
    longest = values.shape.index(max(values.shape))
    spots = []
    for shift in (0, 1):
        where = [jax.random.randint(jax.random.fold_in(own_key, axis), (), 0, length) for axis, length in enumerate(values.shape)]
        where[longest] = (where[longest] + shift) % values.shape[longest]
        spots.append(tuple(where))
    return values.at[spots[0]].set(least).at[spots[1]].set(high)


def levels(stream_key, extent, shards, low, top_value):
    level = 1.0
    for position, parts in shards:
        heights = jax.random.uniform(jax.random.fold_in(jax.random.fold_in(stream_key, 6), position), (parts,), jnp.float32, low / len(shards), top_value / len(shards))
        level = level * jnp.repeat(jnp.exp(heights), extent[position] // parts).reshape((-1,) + (1,) * (len(extent) - 1 - position))
    return level


def centred(key, extent, spread, limit, cuts=(), held_as=jnp.bfloat16):
    values = jax.random.normal(key, extent, jnp.float32) * spread
    if len(cuts) > 0:
        values = levels(key, extent, cuts, -0.22, 0.18) * values
    return jnp.clip(values, min=-limit, max=limit).astype(held_as)


def setup_inputs(seed: int = 0) -> dict:
    key_of = jax.random.split(jax.random.key(seed), 9)
    return {
        "waves": centred(key_of[0], (2, BANDS, GW), 1.0, 6.0, ((1, 16), (2, 32))),
        "occupations": jnp.clip(jnp.exp(math.log(0.0078125) - 2.9957323 * jax.random.uniform(key_of[1], (BANDS,), jnp.float32) ** levels(key_of[1], (BANDS,), ((0, 16),), -0.2, 0.2)), 0.000390625, 0.0078125),
        "beta_table": centred(key_of[2], (SPECIES * NH, GW), (2 * GW) ** -0.5, 0.0234375, ((1, 32),), jnp.float32),
        "wave_miller": place_ends(jax.random.randint(key_of[3], (3, GW), 0, min(NX, min(NY, NZ))), jax.random.fold_in(key_of[3], 1), 0, (min(NX, min(NY, NZ))) - 1).astype(jnp.int32),
        "atom_kinds": place_ends(jax.random.randint(key_of[4], (ATOMS,), 0, SPECIES), jax.random.fold_in(key_of[4], 1), 0, SPECIES - 1).astype(jnp.int32),
        "atom_sites": place_ends(jax.random.randint(key_of[5], (3, ATOMS), 0, min(NX, min(NY, NZ))), jax.random.fold_in(key_of[5], 1), 0, (min(NX, min(NY, NZ))) - 1).astype(jnp.int32),
        "aug_table": centred(key_of[6], (SPECIES * PAIRS, STICKS * NZ), ((40.0 * ATOMS * STICKS * NZ) ** -0.5), 0.00015258789, ((1, 512),)),
        "stick_columns": draw_stick_columns(jax.random.fold_in(key_of[8], 71), 0),
    }


highest = lax.Precision.HIGHEST


def pair_tables(proj_count):
    ell_values = np.array([0, 0] + [1] * 6 + [2] * 10)
    pair_first, pair_second = np.triu_indices(proj_count)
    factors = np.where(pair_first == pair_second, 1.0, 2.0).astype(np.float32)
    parity = ((ell_values[pair_first] + ell_values[pair_second]) % 2).astype(np.float32)
    return pair_first * proj_count + pair_second, factors, parity


def phase_coefficients():
    ell_values = np.array([0, 0] + [1] * 6 + [2] * 10)
    coef_real = np.array([1.0, 0.0, -1.0])[ell_values]
    coef_imag = np.array([0.0, -1.0, 0.0])[ell_values]
    return jnp.asarray(coef_real, jnp.float32), jnp.asarray(coef_imag, jnp.float32)


def phase_angle(site_block, first, second, third):
    turn_count = ((site_block[0][:, None] * first[None, :]) % NX) * (NY * NZ)
    turn_count = turn_count + ((site_block[1][:, None] * second[None, :]) % NY) * (NX * NZ)
    turn_count = turn_count + ((site_block[2][:, None] * third[None, :]) % NZ) * (NX * NY)
    turn_count = (turn_count % (NX * NY * NZ)).astype(jnp.int32)
    angle_value = turn_count.astype(jnp.float32) * (2.0 * np.pi / (NX * NY * NZ))
    return jnp.cos(angle_value), -jnp.sin(angle_value)


def structure_factor(site_block, miller):
    return phase_angle(site_block, miller[0], miller[1], miller[2])


def projector_rows(site_block, kinds_block, beta_table, wave_miller):
    struct_re, struct_im = structure_factor(site_block, wave_miller)
    kind_onehot = (kinds_block[:, None] == jnp.arange(SPECIES, dtype=jnp.int32)[None, :]).astype(jnp.float32)
    table_three = beta_table.reshape(SPECIES, NH, -1)
    radial = jnp.einsum("as,sig->aig", kind_onehot, table_three, precision=highest)
    coef_real, coef_imag = phase_coefficients()
    part_re = radial * struct_re[:, None, :]
    part_im = radial * struct_im[:, None, :]
    vkb_re = coef_real[None, :, None] * part_re - coef_imag[None, :, None] * part_im
    vkb_im = coef_real[None, :, None] * part_im + coef_imag[None, :, None] * part_re
    return vkb_re.astype(jnp.bfloat16), vkb_im.astype(jnp.bfloat16)


def augment_weights(becsum, atom_kinds):
    pair_index, factors, parity = pair_tables(NH)
    kind_onehot = (atom_kinds[None, :] == jnp.arange(SPECIES, dtype=jnp.int32)[:, None]).astype(jnp.float32)
    parity_col = jnp.asarray(parity, jnp.float32)[:, None]
    even_rows = becsum.T * (1.0 - parity_col)
    odd_rows = -(becsum.T * parity_col)
    real_part = kind_onehot[:, None, :] * even_rows[None, :, :]
    imag_part = kind_onehot[:, None, :] * odd_rows[None, :, :]
    stacked = jnp.concatenate([real_part, imag_part], axis=2)
    return stacked.reshape(-1, stacked.shape[2]).astype(jnp.bfloat16)


def dense_augmentation(coefficients, atom_sites, column_x, column_y):
    slot_total = column_x.shape[0]
    zeros_z = jnp.zeros((1, NZ), jnp.int32)
    flat_x = (column_x[:, None] + zeros_z).reshape(-1).astype(jnp.int32)
    flat_y = (column_y[:, None] + zeros_z).reshape(-1).astype(jnp.int32)
    flat_z = (jnp.zeros((slot_total, 1), jnp.int32) + jnp.arange(NZ, dtype=jnp.int32)[None, :]).reshape(-1)
    struct_re, struct_im = phase_angle(atom_sites, flat_x, flat_y, flat_z)
    atom_total = coefficients.shape[0] // 2
    amp_re = coefficients[:atom_total]
    amp_im = coefficients[atom_total:]
    aug_re = jnp.sum(amp_re * struct_re - amp_im * struct_im, axis=0)
    aug_im = jnp.sum(amp_re * struct_im + amp_im * struct_re, axis=0)
    return aug_re.reshape(slot_total, NZ), aug_im.reshape(slot_total, NZ)


def reference(waves, occupations, beta_table, wave_miller, atom_kinds, atom_sites, aug_table, stick_columns):
    block_atoms = math.gcd(ATOMS, 8)
    wave_re = waves[0].astype(jnp.float32).T
    wave_im = waves[1].astype(jnp.float32).T

    def project_block(block_index):
        first_atom = block_index * block_atoms
        site_block = lax.dynamic_slice_in_dim(atom_sites, first_atom, block_atoms, 1)
        kinds_block = lax.dynamic_slice_in_dim(atom_kinds, first_atom, block_atoms, 0)
        vkb_re, vkb_im = projector_rows(site_block, kinds_block, beta_table, wave_miller)
        vkb_re = vkb_re.reshape(block_atoms * NH, -1).astype(jnp.float32)
        vkb_im = vkb_im.reshape(block_atoms * NH, -1).astype(jnp.float32)
        proj_re = jnp.dot(vkb_re, wave_re, precision=highest, preferred_element_type=jnp.float32) + jnp.dot(vkb_im, wave_im, precision=highest, preferred_element_type=jnp.float32)
        proj_im = jnp.dot(vkb_re, wave_im, precision=highest, preferred_element_type=jnp.float32) - jnp.dot(vkb_im, wave_re, precision=highest, preferred_element_type=jnp.float32)
        return proj_re.reshape(block_atoms, NH, -1), proj_im.reshape(block_atoms, NH, -1)

    becp_re, becp_im = lax.map(project_block, jnp.arange(ATOMS // block_atoms, dtype=jnp.int32))
    becp_re = becp_re.reshape(ATOMS, NH, -1)
    becp_im = becp_im.reshape(ATOMS, NH, -1)
    full_square = jnp.einsum("aic,ajc->aij", becp_re * occupations[None, None, :], becp_re, precision=highest)
    full_square = full_square + jnp.einsum("aic,ajc->aij", becp_im * occupations[None, None, :], becp_im, precision=highest)
    pair_index, factors, parity = pair_tables(NH)
    becsum = full_square.reshape(ATOMS, NH * NH)[:, pair_index] * factors[None, :]

    aug_weights = augment_weights(becsum, atom_kinds).astype(jnp.float32)
    stick_block = math.gcd(STICKS, 16)

    def dense_block(block_index):
        first_stick = block_index * stick_block
        columns = lax.dynamic_slice_in_dim(stick_columns, first_stick, stick_block, 0)
        table_block = lax.dynamic_slice_in_dim(aug_table, first_stick * NZ, stick_block * NZ, 1).astype(jnp.float32)
        stick_ids = first_stick + jnp.arange(stick_block, dtype=jnp.int32)
        column_x = (stick_ids // BLOCK_STICKS) * NXB + columns // NY
        column_y = columns % NY
        coefficients = jnp.dot(aug_weights.T, table_block, precision=highest, preferred_element_type=jnp.float32)
        aug_re, aug_im = dense_augmentation(coefficients, atom_sites, column_x, column_y)
        flat_rows = jnp.where(columns < 0, NX * NY, column_x * NY + column_y).astype(jnp.int32)
        return aug_re, aug_im, flat_rows

    aug_re, aug_im, flat_rows = lax.map(dense_block, jnp.arange(STICKS // stick_block, dtype=jnp.int32))
    flat_rows = flat_rows.reshape(-1)
    grid_re = jnp.zeros((NX * NY, NZ), jnp.float32).at[flat_rows].add(aug_re.reshape(-1, NZ), mode="drop")
    grid_im = jnp.zeros((NX * NY, NZ), jnp.float32).at[flat_rows].add(aug_im.reshape(-1, NZ), mode="drop")
    grid_values = lax.complex(grid_re, grid_im).reshape(NX, NY, NZ)
    density_field = jnp.fft.ifftn(grid_values) * (NX * NY * NZ)
    density_field = jnp.transpose(density_field, (2, 1, 0))
    return jnp.stack([jnp.real(density_field), jnp.imag(density_field)]).astype(jnp.float32)
```

```python
import functools

import jax
import jax.numpy as jnp
import numpy as np
from jax import lax
from jax.experimental import pallas as pl
from jax.experimental.pallas import tpu as pltpu
from jax.sharding import PartitionSpec as P

NH = 18
PAIRS = 171
SPECIES = 4
NXB = 15
NPL = 7
STK = 8
OWN_ATOMS = 8
HALF = NH // 2
ROWS = HALF * OWN_ATOMS
DESTS = 4
LANES = 128
KLANES = 768

ELL = [0] * 2 + [1] * 6 + [2] * 10
COS = (0.999999989, -19.7392045, 64.9391175, -85.4501395, 60.167631, -25.9675992, 6.52865816)
SIN = (6.28318492, -41.3415892, 81.5999433, -76.6144725, 41.3428824, -12.4712435)

MESH = pl.DeviceIdType.MESH
F32 = jnp.float32
BF16 = jnp.bfloat16
highest = lax.Precision.HIGHEST


def round_up(value, step):
    return (value + step - 1) // step * step


def cos_sin(turns):
    u = turns - jnp.floor(turns + 0.5)
    w = u * u
    c = COS[-1]
    for a in COS[-2::-1]:
        c = c * w + a
    s = SIN[-1]
    for a in SIN[-2::-1]:
        s = s * w + a
    return c, s * u


def turns_of(product, length):
    inverse = 1.0 / length
    return (product - length * jnp.floor(product * inverse)) * inverse


def split(x):
    hi = x.astype(BF16)
    return hi, (x - hi.astype(F32)).astype(BF16)


def dot_nt(a, b, **kw):
    return lax.dot_general(a, b, (((1,), (1,)), ((), ())), preferred_element_type=F32, **kw)


def dot_nn(a, b, **kw):
    return lax.dot_general(a, b, (((1,), (0,)), ((), ())), preferred_element_type=F32, **kw)


def kernel(
    nb,
    ng,
    gt_lanes,
    waves_ref,
    occ_ref,
    beta_ref,
    mil_ref,
    kinds_ref,
    sites_ref,
    tab_hbm,
    sticks_ref,
    tz_hbm,
    tx_hbm,
    even_ref,
    out_ref,
    tab,
    tz,
    tx,
    local_sem,
    colb,
    mil,
    wmat,
    acc,
    send_p,
    recv_p,
    send_b,
    recv_b,
    send_c,
    recv_c,
    occ_row,
    phase,
    send_z,
    recv_z,
    send_a,
    recv_a,
    wre,
    wim,
    augrow,
    send_v,
    recv_v,
    ey,
    onehot,
    vexp,
    send_y,
    recv_y,
    p_ssem,
    p_rsem,
    b_ssem,
    b_rsem,
    c_ssem,
    c_rsem,
    z_ssem,
    z_rsem,
    a_ssem,
    a_rsem,
    v_ssem,
    v_rsem,
    y_ssem,
    y_rsem,
):
    nx, nz = NXB * nb, NPL * ng
    atoms = OWN_ATOMS * ng
    slots = STK * ng
    band_dev, wave_count = waves_ref.shape[1], waves_ref.shape[2]
    tiles = wave_count // gt_lanes
    steps = ng // 2 // DESTS
    cy = 4 if ng == 32 else 2
    cx = ng // 2 // cy
    columns = STK * nz
    ct = columns // NPL
    b = lax.axis_index("band")
    j = lax.axis_index("ga")
    core = j % 2
    chip = j // 2
    chip_y = chip // cx
    chip_x = chip % cx

    local = [
        pltpu.make_async_copy(tab_hbm, tab, local_sem.at[0]),
        pltpu.make_async_copy(tz_hbm, tz, local_sem.at[1]),
        pltpu.make_async_copy(tx_hbm, tx, local_sem.at[2]),
    ]
    for copy in local:
        copy.start()

    barrier = pltpu.get_barrier_semaphore()

    def greet_ga(k, carry):
        pl.semaphore_signal(barrier, inc=1, device_id=(b, (j + k) % ng), device_id_type=MESH)
        return carry

    def greet_band(k, carry):
        pl.semaphore_signal(barrier, inc=1, device_id=((b + k) % nb, j), device_id_type=MESH)
        return carry

    lax.fori_loop(1, nb, greet_band, 0)
    lax.fori_loop(1, ng, greet_ga, 0)

    cols = jnp.concatenate(
        [
            sites_ref[...].astype(F32),
            kinds_ref[...].astype(F32),
            jnp.zeros((4, atoms), F32),
        ],
        axis=0,
    ).T
    for n in range(4):
        colb[n] = jnp.broadcast_to(cols[:, n : n + 1], (atoms, LANES))
    mil[0:3, :] = mil_ref[...].astype(F32)
    occ_row[...] = jnp.zeros(occ_row.shape, F32)
    occ_row[0:1, 0:band_dev] = occ_ref[...]
    stick = [sticks_ref[t].astype(F32) for t in range(STK)]
    slot_row = lax.broadcasted_iota(jnp.int32, (STK, LANES), 0)
    mine = jnp.zeros((STK, LANES), F32)
    for t in range(STK):
        mine = jnp.where(slot_row == t, stick[t], mine)
    send_c[...] = mine
    recv_c[j] = mine

    width = 2 * band_dev
    for g in range(tiles):
        lanes = slice(g * gt_lanes, (g + 1) * gt_lanes)
        wr = waves_ref[0, :, lanes].astype(F32)
        wi = waves_ref[1, :, lanes].astype(F32)
        none = jnp.zeros((LANES - width, gt_lanes), F32)
        with_cos = jnp.concatenate([wr, wi], axis=0)
        with_sin = jnp.concatenate([-wi, wr], axis=0)
        for h in range(2):
            for n, part in enumerate((with_cos, with_sin)):
                full = jnp.concatenate([part, none] if h == 0 else [none, part], axis=0)
                wmat[g, (2 * h + n) * gt_lanes : (2 * h + n + 1) * gt_lanes, :] = full.T.astype(BF16)

    def wide(x, lanes):
        return jnp.concatenate([x] * (lanes // LANES), axis=1) if lanes > LANES else x[:, :lanes]

    def chip_of(index):
        e = cy * cx - 1 - index
        return ((chip_y + e // cx) % cy) * cx + (chip_x + e % cx) % cx

    def project(step, parity):
        acc[...] = jnp.zeros(acc.shape, F32)

        def tile(g, carry):
            lanes = pl.ds(pl.multiple_of(g * gt_lanes, gt_lanes), gt_lanes)
            m1, m2, m3 = mil[0:1, lanes], mil[1:2, lanes], mil[2:3, lanes]
            parts = [[], [], [], []]
            for d in range(DESTS):
                dest = 2 * chip_of(step * DESTS + d) + parity
                rows = pl.ds(pl.multiple_of(dest * OWN_ATOMS, OWN_ATOMS), OWN_ATOMS)
                p1, p2, p3, kind = (wide(colb[n, rows, :], gt_lanes) for n in range(4))
                turns = turns_of(p1 * m1 + p2 * m2, nx) + turns_of(p3 * m3, nz)
                c, s = cos_sin(turns)
                pair = ((c, s), (-s, c), (-c, -s))
                upper = kind > 1.5
                odd_low = kind > 0.5
                odd_high = kind > 2.5
                for i in range(NH):
                    beta = [beta_ref[n * NH + i : n * NH + i + 1, lanes] for n in range(SPECIES)]
                    radial = jnp.where(
                        upper,
                        jnp.where(odd_high, beta[3], beta[2]),
                        jnp.where(odd_low, beta[1], beta[0]),
                    )
                    first, second = pair[ELL[i]]
                    h = i // HALF
                    parts[2 * h].append(radial * first)
                    parts[2 * h + 1].append(radial * second)
            left = jnp.concatenate([jnp.concatenate(p, axis=0).astype(BF16) for p in parts], axis=1)
            acc[...] += dot_nn(left, wmat[g])
            return carry

        lax.fori_loop(0, tiles, tile, 0)

    def for_partner(step, carry):
        project(step, 1 - core)
        send_p[step] = acc[...]
        return carry

    lax.fori_loop(0, steps, for_partner, 0)
    pl.semaphore_wait(barrier, (nb - 1) + (ng - 1))

    def copy_p(step):
        return pltpu.make_async_remote_copy(
            send_p.at[step],
            recv_p.at[step],
            p_ssem.at[step],
            p_rsem.at[step],
            device_id=(b, chip * 2 + 1 - core),
            device_id_type=MESH,
        )

    def copy_ga(source, target, ssem, rsem, k):
        return pltpu.make_async_remote_copy(
            source,
            target,
            ssem.at[k],
            rsem.at[k],
            device_id=(b, (j + k) % ng),
            device_id_type=MESH,
        )

    def band_offset(k):
        half = nb // 2
        m = (k + 1) // 2
        return half + m * (1 - 2 * (k % 2))

    def copy_band(source, target, ssem, rsem, off):
        return pltpu.make_async_remote_copy(
            source,
            target,
            ssem.at[off],
            rsem.at[off],
            device_id=((b + off) % nb, j),
            device_id_type=MESH,
        )

    def loop(low, high, body):
        def step(k, carry):
            body(k)
            return carry

        lax.fori_loop(low, high, step, 0)

    loop(0, steps, lambda s: copy_p(s).start())
    loop(1, ng, lambda k: copy_ga(send_c, recv_c.at[j], c_ssem, c_rsem, k).start())

    def copy_b(index):
        return pltpu.make_async_remote_copy(
            send_b.at[index],
            recv_b.at[index],
            b_ssem.at[index],
            b_rsem.at[index],
            device_id=(b, 2 * chip_of(index) + core),
            device_id_type=MESH,
        )

    last = cy * cx - 1

    def for_owners(step, carry):
        project(step, core)
        copy_p(step).wait_recv()
        for d in range(DESTS):
            index = step * DESTS + d
            block = acc[d * ROWS : (d + 1) * ROWS, :] + recv_p[step, d * ROWS : (d + 1) * ROWS, :]
            send_b[index] = block

            @pl.when(index < last)
            def _():
                copy_b(index).start()

        return carry

    lax.fori_loop(0, steps, for_owners, 0)

    def phases(t):
        lanes = pl.ds(pl.multiple_of(t * ct, ct), ct)
        g = (lax.broadcasted_iota(jnp.int32, (1, ct), 1) + t * ct).astype(F32)
        slot = jnp.floor((g + 0.5) * (1.0 / nz))
        z = g - slot * nz
        column = jnp.zeros((1, ct), F32)
        for n in range(STK):
            column = jnp.where(slot == n, stick[n], column)
        x = jnp.floor((column + 0.5) * (1.0 / nx))
        y = column - x * nx
        x = x + (b * NXB).astype(F32)

        def row(r):
            rows = pl.ds(pl.multiple_of(r * 8, 8), 8)
            p1, p2, p3 = (wide(colb[n, rows, :], ct) for n in range(3))
            turns = turns_of(p1 * x + p2 * y, nx) + turns_of(p3 * z, nz)
            c, s = cos_sin(turns)
            phase[0, rows, lanes] = c
            phase[1, rows, lanes] = s

        loop(0, atoms // 8, row)

    loop(0, NPL, phases)

    def wait_b(index):
        copy_b(index).wait_recv()

    loop(0, last, wait_b)
    becp = send_b[last]
    for index in range(last):
        becp = becp + recv_b[index]
    occ = occ_row[...]
    occ = sum((pltpu.roll(occ, n * band_dev, 1) for n in range(1, LANES // band_dev)), occ)[0:1]
    lane = lax.broadcasted_iota(jnp.int32, (1, LANES), 1)
    occ = jnp.where(lane < width, occ, 0.0)
    both = jnp.concatenate([becp, pltpu.roll(becp, LANES - width, 1)], axis=0)
    gram = dot_nt(both * occ, both, precision=highest)
    rows = NH * OWN_ATOMS
    row_id = lax.broadcasted_iota(jnp.int32, (rows, rows), 0)
    col_id = lax.broadcasted_iota(jnp.int32, (rows, rows), 1)
    gram = jnp.where(row_id % OWN_ATOMS == col_id % OWN_ATOMS, gram, 0.0)
    pick = (
        lax.broadcasted_iota(jnp.int32, (rows, LANES), 0) // OWN_ATOMS
        == lax.broadcasted_iota(jnp.int32, (rows, LANES), 1)
    ).astype(F32)
    square = dot_nn(gram, pick, precision=highest)
    total = jnp.zeros((OWN_ATOMS, 2 * LANES), F32)
    for i in range(NH):
        factor = jnp.where(lane < i, 0.0, jnp.where(lane == i, 1.0, 2.0))
        factor = jnp.where(lane < NH, factor, 0.0)
        piece = square[i * OWN_ATOMS : (i + 1) * OWN_ATOMS] * factor
        piece = jnp.concatenate([piece, jnp.zeros((OWN_ATOMS, LANES), F32)], axis=1)
        shift = i * NH - i * (i - 1) // 2 - i
        total = total + (pltpu.roll(piece, shift, 1) if shift else piece)
    send_z[...] = total
    recv_z[0] = total

    def send_band(k):
        off = band_offset(k)
        copy_band(send_z, recv_z.at[off], z_ssem, z_rsem, off).start()

    loop(0, nb - 1, send_band)

    loop(1, ng, lambda k: copy_ga(send_c, recv_c.at[j], c_ssem, c_rsem, k).wait_recv())
    column = recv_c[...].reshape(slots, LANES)
    slot_x = jnp.floor((column + 0.5) * (1.0 / nx))
    slot_y = column - slot_x * nx
    hot = (slot_x == lax.broadcasted_iota(jnp.int32, (slots, LANES), 1).astype(F32)).astype(F32)
    onehot[...] = hot.T[0:16].astype(BF16)
    lane_y = (lax.broadcasted_iota(jnp.int32, (1, LANES), 1) % 16).astype(F32)

    def y_phases(n):
        turns = turns_of(slot_y * (lane_y + (n * NXB).astype(F32)), nx)
        c, s = cos_sin(turns)
        ey[n, 0] = c
        ey[n, 1] = s

    loop(0, nb, y_phases)

    def wait_band(k):
        off = band_offset(k)
        copy_band(send_z, recv_z.at[off], z_ssem, z_rsem, off).wait_recv()

    loop(0, nb - 1, wait_band)
    total = recv_z[0]
    for n in range(1, nb):
        total = total + recv_z[n]
    send_a[...] = total
    recv_a[j] = total
    loop(1, ng, lambda k: copy_ga(send_a, recv_a.at[j], a_ssem, a_rsem, k).start())
    for copy in local:
        copy.wait()
    loop(1, ng, lambda k: copy_ga(send_a, recv_a.at[j], a_ssem, a_rsem, k).wait_recv())

    even = even_ref[0:1, :]
    odd = even_ref[1:2, :]

    def weights(r):
        values = recv_a[pl.ds(2 * r, 2)].reshape(16, 2 * LANES)
        values = jnp.concatenate([values, jnp.zeros((16, KLANES - 2 * LANES), F32)], axis=1)
        rows = pl.ds(pl.multiple_of(r * 16, 16), 16)
        kind = wide(colb[3, rows, :], KLANES)
        placed = jnp.where(kind < 0.5, values, 0.0)
        for n in range(1, SPECIES):
            moved = pltpu.roll(values, n * PAIRS, 1)
            placed = jnp.where((kind > n - 0.5) & (kind < n + 0.5), moved, placed)
        wre[rows, :] = (placed * even).astype(BF16)
        wim[rows, :] = (placed * odd).astype(BF16)

    loop(0, atoms // 16, weights)
    depth = SPECIES * PAIRS

    def coefficients(t):
        lanes = pl.ds(pl.multiple_of(t * ct, ct), ct)
        table = tab[:, lanes]
        amp_re = dot_nn(wre[:, :depth], table)
        amp_im = dot_nn(wim[:, :depth], table)
        c, s = phase[0, :, lanes], phase[1, :, lanes]
        augrow[0:1, lanes] = jnp.sum(amp_re * c + amp_im * s, axis=0, keepdims=True)
        augrow[1:2, lanes] = jnp.sum(amp_im * c - amp_re * s, axis=0, keepdims=True)

    loop(0, NPL, coefficients)

    pad_z = tz.shape[2] // 2
    wide_row = round_up(columns, LANES)
    shape = (STK, pad_z)
    slot_id = lax.broadcasted_iota(jnp.int32, shape, 0)
    lane_id = lax.broadcasted_iota(jnp.int32, shape, 1)
    values = []
    for n in range(2):
        row = augrow[n : n + 1, :]
        picked = jnp.zeros(shape, F32)
        for t in range(STK):
            moved = pltpu.roll(row, wide_row - t * nz, 1) if t else row
            picked = jnp.where(slot_id == t, moved[:, :pad_z], picked)
        values.append(jnp.where(lane_id < nz, picked, 0.0))
    a_re, a_im = values
    pair = jnp.concatenate(
        [jnp.concatenate([a_re, -a_im], axis=1), jnp.concatenate([a_im, a_re], axis=1)], axis=0
    )
    group = lax.broadcasted_iota(jnp.int32, (LANES, 1), 0) // (2 * STK)
    placed = jnp.where(group == j % 8, jnp.concatenate([pair] * 8, axis=0), 0.0)
    hi, lo = split(placed)
    planes = dot_nt(tz[0], hi) + dot_nt(tz[0], lo) + dot_nt(tz[1], hi)
    send_v[...] = planes.reshape(ng, 8, LANES)
    recv_v[j] = send_v[j]

    def copy_v(k):
        return copy_ga(send_v.at[(j + k) % ng], recv_v.at[j], v_ssem, v_rsem, k)

    loop(1, ng, lambda k: copy_v(k).start())
    loop(1, ng, lambda k: copy_v(k).wait_recv())

    groups = max(ng // 8, 1)
    expand = (
        lax.broadcasted_iota(jnp.int32, (8, LANES), 1) // 16
        == lax.broadcasted_iota(jnp.int32, (8, LANES), 0)
    ).astype(BF16)
    for q in range(groups):
        tile = recv_v[8 * q]
        for n in range(1, 8):
            tile = tile + recv_v[8 * q + n]
        hi, lo = split(tile.T)
        spread = dot_nn(hi, expand) + dot_nn(lo, expand)
        spread = spread.reshape(8, 2, STK, LANES)
        for n in range(2):
            vexp[n, q * 8 * STK : (q + 1) * 8 * STK, :] = spread[:, n].reshape(8 * STK, LANES)

    def y_block(n):
        c, s = ey[n, 0], ey[n, 1]
        v_re, v_im = vexp[0], vexp[1]
        z = jnp.concatenate([v_re * c - v_im * s, v_re * s + v_im * c], axis=1)
        hi, lo = split(z)
        hot = onehot[...]
        return dot_nn(hot, hi) + dot_nn(hot, lo)

    def copy_y(k):
        off = band_offset(k)
        return copy_band(send_y.at[off], recv_y.at[b], y_ssem, y_rsem, off)

    def send_block(k):
        off = band_offset(k)
        send_y[off] = y_block((b + off) % nb)
        copy_y(k).start()

    loop(0, nb - 1, send_block)
    recv_y[b] = y_block(b)
    loop(0, nb - 1, lambda k: copy_y(k).wait_recv())

    field = recv_y[...].reshape(nb * 16, 2 * LANES).T
    f_re, f_im = field[:LANES], field[LANES:]
    left = jnp.concatenate(
        [jnp.concatenate([f_re, -f_im], axis=1), jnp.concatenate([f_im, f_re], axis=1)], axis=0
    )
    hi, lo = split(left)
    result = dot_nn(hi, tx[0]) + dot_nn(lo, tx[0]) + dot_nn(hi, tx[1])
    for n in range(2):
        for p in range(NPL):
            first = n * LANES + p * 16
            out_ref[n, p] = result[first : first + NXB, :nx]

    loop(0, steps, lambda s: copy_p(s).wait_send())
    loop(0, last, lambda i: copy_b(i).wait_send())
    loop(1, ng, lambda k: copy_ga(send_c, recv_c.at[j], c_ssem, c_rsem, k).wait_send())
    loop(1, ng, lambda k: copy_ga(send_a, recv_a.at[j], a_ssem, a_rsem, k).wait_send())
    loop(1, ng, lambda k: copy_v(k).wait_send())

    def end_band(k):
        off = band_offset(k)
        copy_band(send_z, recv_z.at[off], z_ssem, z_rsem, off).wait_send()
        copy_y(k).wait_send()

    loop(0, nb - 1, end_band)


def both_parts(table):
    hi = table.astype(jnp.bfloat16)
    lo = (table - hi.astype(np.float64)).astype(jnp.bfloat16)
    return np.stack([hi, lo])


def tables(nb, ng):
    nx, nz = NXB * nb, NPL * ng
    pad_z = round_up(nz, LANES)
    plane = np.arange(8 * ng) // 8 * NPL + np.arange(8 * ng) % 8
    angle = (plane[:, None] * np.arange(nz)[None, :] % nz) * (2 * np.pi / nz)
    real = (np.arange(8 * ng) % 8 < NPL)[:, None]
    tz = np.zeros((8 * ng, 2 * pad_z))
    tz[:, :nz] = np.where(real, np.cos(angle), 0.0)
    tz[:, pad_z : pad_z + nz] = np.where(real, np.sin(angle), 0.0)
    pad_x = round_up(nx, LANES)
    row = np.arange(16 * nb)
    x = row // 16 * NXB + row % 16
    angle = (x[:, None] * np.arange(nx)[None, :] % nx) * (2 * np.pi / nx)
    real = (row % 16 < NXB)[:, None]
    tx = np.zeros((2 * 16 * nb, pad_x))
    tx[: 16 * nb, :nx] = np.where(real, np.cos(angle), 0.0)
    tx[16 * nb :, :nx] = np.where(real, np.sin(angle), 0.0)
    first, second = np.triu_indices(NH)
    ell = np.array(ELL)
    parity = np.tile((ell[first] + ell[second]) % 2, SPECIES)
    even = np.zeros((2, KLANES), np.float32)
    even[0, : SPECIES * PAIRS] = 1 - parity
    even[1, : SPECIES * PAIRS] = -parity
    return jnp.asarray(both_parts(tz)), jnp.asarray(both_parts(tx)), jnp.asarray(even)


def on_device(
    waves, occupations, beta_table, wave_miller, atom_kinds, atom_sites, aug_table, stick_columns
):
    nb, ng = lax.axis_size("band"), lax.axis_size("ga")
    nx, nz = NXB * nb, NPL * ng
    atoms, slots = OWN_ATOMS * ng, STK * ng
    wave_count = waves.shape[2]
    gt_lanes = min(256, wave_count)
    tiles = wave_count // gt_lanes
    columns = STK * nz
    steps = ng // 2 // DESTS
    chips = ng // 2
    tz, tx, even = tables(nb, ng)
    vmem = pl.BlockSpec(memory_space=pltpu.VMEM)
    hbm = pl.BlockSpec(memory_space=pl.ANY)
    smem = pl.BlockSpec(memory_space=pltpu.SMEM)
    dma = pltpu.SemaphoreType.DMA
    return pl.pallas_call(
        functools.partial(kernel, nb, ng, gt_lanes),
        out_shape=jax.ShapeDtypeStruct((2, NPL, NXB, nx), F32),
        in_specs=[vmem, vmem, vmem, vmem, vmem, vmem, hbm, smem, hbm, hbm, vmem],
        out_specs=vmem,
        scratch_shapes=[
            pltpu.VMEM(aug_table.shape, BF16),
            pltpu.VMEM(tz.shape, BF16),
            pltpu.VMEM(tx.shape, BF16),
            dma((3,)),
            pltpu.VMEM((4, atoms, LANES), F32),
            pltpu.VMEM((8, wave_count), F32),
            pltpu.VMEM((tiles, 4 * gt_lanes, LANES), BF16),
            pltpu.VMEM((DESTS * ROWS, LANES), F32),
            pltpu.VMEM((steps, DESTS * ROWS, LANES), F32),
            pltpu.VMEM((steps, DESTS * ROWS, LANES), F32),
            pltpu.VMEM((chips, ROWS, LANES), F32),
            pltpu.VMEM((chips, ROWS, LANES), F32),
            pltpu.VMEM((STK, LANES), F32),
            pltpu.VMEM((ng, STK, LANES), F32),
            pltpu.VMEM((8, LANES), F32),
            pltpu.VMEM((2, atoms, columns), F32),
            pltpu.VMEM((OWN_ATOMS, 2 * LANES), F32),
            pltpu.VMEM((nb, OWN_ATOMS, 2 * LANES), F32),
            pltpu.VMEM((OWN_ATOMS, 2 * LANES), F32),
            pltpu.VMEM((ng, OWN_ATOMS, 2 * LANES), F32),
            pltpu.VMEM((atoms, KLANES), BF16),
            pltpu.VMEM((atoms, KLANES), BF16),
            pltpu.VMEM((8, round_up(columns, LANES)), F32),
            pltpu.VMEM((ng, 8, LANES), F32),
            pltpu.VMEM((ng, 8, LANES), F32),
            pltpu.VMEM((nb, 2, slots, LANES), F32),
            pltpu.VMEM((16, slots), BF16),
            pltpu.VMEM((2, slots, LANES), F32),
            pltpu.VMEM((nb, 16, 2 * LANES), F32),
            pltpu.VMEM((nb, 16, 2 * LANES), F32),
            dma((steps,)),
            dma((steps,)),
            dma((chips,)),
            dma((chips,)),
            dma((ng,)),
            dma((ng,)),
            dma((nb,)),
            dma((nb,)),
            dma((ng,)),
            dma((ng,)),
            dma((ng,)),
            dma((ng,)),
            dma((nb,)),
            dma((nb,)),
        ],
        compiler_params=pltpu.CompilerParams(
            collective_id=0, has_side_effects=True, vmem_limit_bytes=48 * 1024 * 1024
        ),
    )(
        waves,
        occupations[None],
        beta_table,
        wave_miller,
        atom_kinds[None],
        atom_sites,
        aug_table,
        stick_columns,
        tz,
        tx,
        even,
    )


def solution(mesh):
    in_specs = (
        P(None, "band", "ga"),
        P("band"),
        P(None, "ga"),
        P(None, "ga"),
        P(),
        P(),
        P(None, ("band", "ga")),
        P(("band", "ga")),
    )
    out_specs = P(None, "ga", "band", None)
    return jax.shard_map(
        on_device, mesh=mesh, in_specs=in_specs, out_specs=out_specs, check_vma=False
    )
```

```python
import functools

import jax
import jax.numpy as jnp
import numpy as np
from jax import lax
from jax.experimental import pallas as pl
from jax.experimental.pallas import tpu as pltpu
from jax.sharding import PartitionSpec as P

NH = 18
PAIRS = 171
SPECIES = 4
NXB = 15
NPL = 7
STK = 8
OWN_ATOMS = 8
HALF = NH // 2
ROWS = HALF * OWN_ATOMS
DESTS = 4
LANES = 128
KLANES = 768
FOLD = OWN_ATOMS * 3 // 2
VMEM_LIMIT = 67043328
UNROLL = 4

ELL = [0] * 2 + [1] * 6 + [2] * 10
COS = (0.999999989, -19.7392045, 64.9391175, -85.4501395, 60.167631, -25.9675992, 6.52865816)
SIN = (6.28318492, -41.3415892, 81.5999433, -76.6144725, 41.3428824, -12.4712435)

MESH = pl.DeviceIdType.MESH
F32 = jnp.float32
BF16 = jnp.bfloat16
highest = lax.Precision.HIGHEST


def round_up(value, step):
    return (value + step - 1) // step * step


def cos_sin(turns):
    u = turns - jnp.floor(turns + 0.5)
    w = u * u
    c = COS[-1]
    for a in COS[-2::-1]:
        c = c * w + a
    s = SIN[-1]
    for a in SIN[-2::-1]:
        s = s * w + a
    return c, s * u


def turns_of(product, length):
    inverse = 1.0 / length
    return (product - length * jnp.floor(product * inverse)) * inverse


def split(x):
    hi = x.astype(BF16)
    return hi, (x - hi.astype(F32)).astype(BF16)


def dot_nt(a, b, **kw):
    return lax.dot_general(a, b, (((1,), (1,)), ((), ())), preferred_element_type=F32, **kw)


def dot_nn(a, b, **kw):
    return lax.dot_general(a, b, (((1,), (0,)), ((), ())), preferred_element_type=F32, **kw)


def kernel(
    nb,
    ng,
    gt_lanes,
    waves_hbm,
    occ_hbm,
    beta_hbm,
    mil_hbm,
    kinds_hbm,
    sites_hbm,
    tab_hbm,
    sticks_hbm,
    tz_hbm,
    tx_hbm,
    even_hbm,
    out_ref,
    waves_ref,
    occ_ref,
    beta_ref,
    mil_ref,
    kinds_ref,
    sites_ref,
    sticks_ref,
    even_ref,
    tab,
    tz,
    tx,
    local_sem,
    colb,
    kindb,
    species,
    mil,
    wmat,
    acc,
    send_p,
    recv_p,
    send_b,
    recv_b,
    send_c,
    recv_c,
    occ_row,
    phase,
    send_z,
    recv_z,
    send_a,
    recv_a,
    wre,
    wim,
    augrow,
    send_v,
    recv_v,
    ey,
    onehot,
    vexp,
    send_y,
    recv_y,
    p_ssem,
    p_rsem,
    b_ssem,
    b_rsem,
    c_ssem,
    c_rsem,
    z_ssem,
    z_rsem,
    a_ssem,
    a_rsem,
    v_ssem,
    v_rsem,
    y_ssem,
    y_rsem,
):
    nx, nz = NXB * nb, NPL * ng
    atoms = OWN_ATOMS * ng
    slots = STK * ng
    band_dev, wave_count = waves_ref.shape[1], waves_ref.shape[2]
    tiles = wave_count // gt_lanes
    steps = ng // 2 // DESTS
    cy = 4 if ng == 32 else 2
    cx = ng // 2 // cy
    columns = STK * nz
    ct = columns // NPL
    b = lax.axis_index("band")
    j = lax.axis_index("ga")
    core = j % 2
    chip = j // 2
    chip_y = chip // cx
    chip_x = chip % cx

    ends = [
        (sites_hbm, sites_ref),
        (kinds_hbm, kinds_ref),
        (mil_hbm, mil_ref),
        (sticks_hbm, sticks_ref),
        (waves_hbm, waves_ref),
        (beta_hbm, beta_ref),
        (occ_hbm, occ_ref),
        (even_hbm, even_ref),
        (tz_hbm, tz),
        (tx_hbm, tx),
        (tab_hbm, tab),
    ]
    local = [pltpu.make_async_copy(*pair, local_sem.at[n]) for n, pair in enumerate(ends)]
    for copy in local:
        copy.start()

    barrier = pltpu.get_barrier_semaphore()

    def greet_ga(k, carry):
        pl.semaphore_signal(barrier, inc=1, device_id=(b, (j + k) % ng), device_id_type=MESH)
        return carry

    def greet_band(k, carry):
        pl.semaphore_signal(barrier, inc=1, device_id=((b + k) % nb, j), device_id_type=MESH)
        return carry

    lax.fori_loop(1, nb, greet_band, 0)
    lax.fori_loop(1, ng, greet_ga, 0)

    for copy in local[:7]:
        copy.wait()

    cols = jnp.concatenate(
        [
            sites_ref[...].astype(F32),
            kinds_ref[...].astype(F32),
            jnp.zeros((4, atoms), F32),
        ],
        axis=0,
    ).T
    for n in range(4):
        colb[n] = jnp.broadcast_to(cols[:, n : n + 1], (atoms, LANES))
    kindb[...] = colb[3].astype(jnp.int32)
    kind_row = lax.broadcasted_iota(jnp.int32, (8, wave_count), 0)
    for i in range(NH):
        beta = [beta_ref[n * NH + i : n * NH + i + 1, :] for n in range(SPECIES)]
        species[i] = jnp.where(
            kind_row < 2,
            jnp.where(kind_row < 1, beta[0], beta[1]),
            jnp.where(kind_row < 3, beta[2], beta[3]),
        )
    mil[0:3, :] = mil_ref[...].astype(F32)
    occ_row[...] = jnp.zeros(occ_row.shape, F32)
    occ_row[0:1, 0:band_dev] = occ_ref[...]
    stick = [sticks_ref[t].astype(F32) for t in range(STK)]
    slot_row = lax.broadcasted_iota(jnp.int32, (STK, LANES), 0)
    mine = jnp.zeros((STK, LANES), F32)
    for t in range(STK):
        mine = jnp.where(slot_row == t, stick[t], mine)
    send_c[...] = mine
    recv_c[j] = mine

    width = 2 * band_dev
    for g in range(tiles):
        lanes = slice(g * gt_lanes, (g + 1) * gt_lanes)
        wr = waves_ref[0, :, lanes].astype(F32)
        wi = waves_ref[1, :, lanes].astype(F32)
        none = jnp.zeros((LANES - width, gt_lanes), F32)
        with_cos = jnp.concatenate([wr, wi], axis=0)
        with_sin = jnp.concatenate([-wi, wr], axis=0)
        for h in range(2):
            for n, part in enumerate((with_cos, with_sin)):
                full = jnp.concatenate([part, none] if h == 0 else [none, part], axis=0)
                wmat[g, (2 * h + n) * gt_lanes : (2 * h + n + 1) * gt_lanes, :] = full.T.astype(BF16)

    def wide(x, lanes):
        return jnp.concatenate([x] * (lanes // LANES), axis=1) if lanes > LANES else x[:, :lanes]

    def chip_of(index):
        e = cy * cx - 1 - index
        return ((chip_y + e // cx) % cy) * cx + (chip_x + e % cx) % cx

    def project(step, parity):
        def rows_of(d):
            dest = 2 * chip_of(step * DESTS + d) + parity
            return pl.ds(pl.multiple_of(dest * OWN_ATOMS, OWN_ATOMS), OWN_ATOMS)

        def tile(g):
            whole = [[], [], [], []]
            for piece in range(gt_lanes // LANES):
                lanes = pl.ds(pl.multiple_of(g * gt_lanes + piece * LANES, LANES), LANES)
                m1, m2, m3 = mil[0:1, lanes], mil[1:2, lanes], mil[2:3, lanes]
                pairs, kinds = [], []
                for d in range(DESTS):
                    rows = rows_of(d)
                    p1, p2, p3 = (colb[n, rows, :] for n in range(3))
                    kinds.append(kindb[rows, :])
                    turns = turns_of(p1 * m1 + p2 * m2, nx) + turns_of(p3 * m3, nz)
                    c, s = cos_sin(turns)
                    pairs.append(((c, s), (-s, c), (-c, -s)))
                parts = [[[None] * HALF for d in range(DESTS)] for n in range(4)]
                for i in range(NH):
                    beta = species[i, :, lanes]
                    for d in range(DESTS):
                        radial = jnp.take_along_axis(beta, kinds[d], axis=0)
                        first, second = pairs[d][ELL[i]]
                        h = i // HALF
                        parts[2 * h][d][i % HALF] = radial * first
                        parts[2 * h + 1][d][i % HALF] = radial * second
                for n in range(4):
                    whole[n].append(jnp.concatenate(sum(parts[n], []), axis=0).astype(BF16))
            left = jnp.concatenate(sum(whole, []), axis=1)
            return dot_nn(left, wmat[g])

        together = min(UNROLL, tiles)

        def some(n, carry):
            total = tile(n * together)
            for g in range(1, together):
                total = total + tile(n * together + g)
            acc[...] = total if together == tiles else acc[...] + total
            return carry

        if together == tiles:
            some(0, 0)
        else:
            acc[...] = jnp.zeros(acc.shape, F32)
            lax.fori_loop(0, tiles // together, some, 0)

    def for_partner(step, carry):
        project(step, 1 - core)
        send_p[step] = acc[...]
        return carry

    lax.fori_loop(0, steps, for_partner, 0)
    pl.semaphore_wait(barrier, (nb - 1) + (ng - 1))

    def copy_p(step):
        return pltpu.make_async_remote_copy(
            send_p.at[step],
            recv_p.at[step],
            p_ssem.at[step],
            p_rsem.at[step],
            device_id=(b, chip * 2 + 1 - core),
            device_id_type=MESH,
        )

    def copy_ga(source, target, ssem, rsem, k):
        return pltpu.make_async_remote_copy(
            source,
            target,
            ssem.at[k],
            rsem.at[k],
            device_id=(b, (j + k) % ng),
            device_id_type=MESH,
        )

    def band_offset(k):
        half = nb // 2
        m = (k + 1) // 2
        return half + m * (1 - 2 * (k % 2))

    def copy_band(source, target, ssem, rsem, off):
        return pltpu.make_async_remote_copy(
            source,
            target,
            ssem.at[off],
            rsem.at[off],
            device_id=((b + off) % nb, j),
            device_id_type=MESH,
        )

    def loop(low, high, body):
        def step(k, carry):
            body(k)
            return carry

        lax.fori_loop(low, high, step, 0)

    loop(0, steps, lambda s: copy_p(s).start())
    loop(1, ng, lambda k: copy_ga(send_c, recv_c.at[j], c_ssem, c_rsem, k).start())

    def copy_b(index):
        return pltpu.make_async_remote_copy(
            send_b.at[index],
            recv_b.at[index],
            b_ssem.at[index],
            b_rsem.at[index],
            device_id=(b, 2 * chip_of(index) + core),
            device_id_type=MESH,
        )

    last = cy * cx - 1

    def for_owners(step, carry):
        project(step, core)
        copy_p(step).wait_recv()
        for d in range(DESTS):
            index = step * DESTS + d
            block = acc[d * ROWS : (d + 1) * ROWS, :] + recv_p[step, d * ROWS : (d + 1) * ROWS, :]
            send_b[index] = block

            @pl.when(index < last)
            def _():
                copy_b(index).start()

        return carry

    lax.fori_loop(0, steps, for_owners, 0)

    loop(1, ng, lambda k: copy_ga(send_c, recv_c.at[j], c_ssem, c_rsem, k).wait_recv())
    column = recv_c[...].reshape(slots, LANES)
    slot_x = jnp.floor((column + 0.5) * (1.0 / nx))
    slot_y = column - slot_x * nx
    hot = (slot_x == lax.broadcasted_iota(jnp.int32, (slots, LANES), 1).astype(F32)).astype(F32)
    onehot[...] = hot.T[0:16].astype(BF16)
    lane_y = (lax.broadcasted_iota(jnp.int32, (1, LANES), 1) % 16).astype(F32)

    def y_phases(n):
        turns = turns_of(slot_y * (lane_y + (n * NXB).astype(F32)), nx)
        c, s = cos_sin(turns)
        ey[n, 0] = c
        ey[n, 1] = s

    loop(0, nb, y_phases)

    loop(0, steps, lambda s: copy_p(s).wait_send())
    loop(1, ng, lambda k: copy_ga(send_c, recv_c.at[j], c_ssem, c_rsem, k).wait_send())
    def wait_b(index):
        copy_b(index).wait_recv()

    loop(0, last, wait_b)
    becp = send_b[last]
    for index in range(last):
        becp = becp + recv_b[index]
    occ = occ_row[...]
    occ = sum((pltpu.roll(occ, n * band_dev, 1) for n in range(1, LANES // band_dev)), occ)[0:1]
    lane = lax.broadcasted_iota(jnp.int32, (1, LANES), 1)
    occ = jnp.where(lane < width, occ, 0.0)
    both = jnp.concatenate([becp, pltpu.roll(becp, LANES - width, 1)], axis=0)
    gram = dot_nt(both * occ, both, precision=highest)
    rows = NH * OWN_ATOMS
    row_id = lax.broadcasted_iota(jnp.int32, (rows, rows), 0)
    col_id = lax.broadcasted_iota(jnp.int32, (rows, rows), 1)
    gram = jnp.where(row_id % OWN_ATOMS == col_id % OWN_ATOMS, gram, 0.0)
    pick = (
        lax.broadcasted_iota(jnp.int32, (rows, LANES), 0) // OWN_ATOMS
        == lax.broadcasted_iota(jnp.int32, (rows, LANES), 1)
    ).astype(F32)
    square = dot_nn(gram, pick, precision=highest)
    total = jnp.zeros((OWN_ATOMS, 2 * LANES), F32)
    for i in range(NH):
        factor = jnp.where(lane < i, 0.0, jnp.where(lane == i, 1.0, 2.0))
        factor = jnp.where(lane < NH, factor, 0.0)
        piece = square[i * OWN_ATOMS : (i + 1) * OWN_ATOMS] * factor
        piece = jnp.concatenate([piece, jnp.zeros((OWN_ATOMS, LANES), F32)], axis=1)
        shift = i * NH - i * (i - 1) // 2 - i
        total = total + (pltpu.roll(piece, shift, 1) if shift else piece)
    folded = total[:4, LANES:] + pltpu.roll(total[4:, LANES:], LANES // 2, 1)
    total = jnp.concatenate([total[:, :LANES], folded], axis=0)
    send_z[...] = total
    recv_z[0] = total

    def send_band(k):
        off = band_offset(k)
        copy_band(send_z, recv_z.at[off], z_ssem, z_rsem, off).start()

    loop(0, nb - 1, send_band)

    def phases(t):
        lanes = pl.ds(pl.multiple_of(t * ct, ct), ct)
        g = (lax.broadcasted_iota(jnp.int32, (1, ct), 1) + t * ct).astype(F32)
        slot = jnp.floor((g + 0.5) * (1.0 / nz))
        z = g - slot * nz
        column = jnp.zeros((1, ct), F32)
        for n in range(STK):
            column = jnp.where(slot == n, stick[n], column)
        x = jnp.floor((column + 0.5) * (1.0 / nx))
        y = column - x * nx
        x = x + (b * NXB).astype(F32)

        def row(r):
            source = 2 * chip_of(last - r // 2) + r % 2
            atom = pl.ds(pl.multiple_of(source * 8, 8), 8)
            p1, p2, p3 = (wide(colb[n, atom, :], ct) for n in range(3))
            rows = pl.ds(pl.multiple_of(r * 8, 8), 8)
            turns = turns_of(p1 * x + p2 * y, nx) + turns_of(p3 * z, nz)
            c, s = cos_sin(turns)
            phase[0, rows, lanes] = c
            phase[1, rows, lanes] = s

        loop(0, atoms // 8, row)

    loop(0, NPL, phases)

    loop(0, last, lambda i: copy_b(i).wait_send())
    def wait_band(k):
        off = band_offset(k)
        copy_band(send_z, recv_z.at[off], z_ssem, z_rsem, off).wait_recv()

    loop(0, nb - 1, wait_band)
    total = recv_z[0]
    for n in range(1, nb):
        total = total + recv_z[n]
    send_a[...] = total
    recv_a[j] = total
    loop(1, ng, lambda k: copy_ga(send_a, recv_a.at[j], a_ssem, a_rsem, k).start())
    for copy in local[7:]:
        copy.wait()

    even = even_ref[0:1, :]
    odd = even_ref[1:2, :]
    depth = SPECIES * PAIRS
    chips = cy * cx
    part = chips // 2
    augrow[...] = jnp.zeros(augrow.shape, F32)

    def arrive(k):
        copy_ga(send_a, recv_a.at[j], a_ssem, a_rsem, k).wait_recv()

    def weights(index):
        q = chip_of(last - index)

        @pl.when(index == 0)
        def _():
            arrive((j - (chip * 2 + 1 - core)) % ng)

        @pl.when(index > 0)
        def _():
            arrive((j - 2 * q) % ng)
            arrive((j - 2 * q - 1) % ng)

        values = []
        for n in range(2):
            got = recv_a[2 * q + n]
            first, rest = got[:OWN_ATOMS], got[OWN_ATOMS:]
            rest = jnp.concatenate([rest, pltpu.roll(rest, LANES // 2, 1)], axis=0)
            values.append(jnp.concatenate([first, rest], axis=1))
        values = jnp.concatenate(values, axis=0)
        position = lax.broadcasted_iota(jnp.int32, values.shape, 1)
        values = jnp.where(position < PAIRS, values, 0.0)
        values = jnp.concatenate([values, jnp.zeros((16, KLANES - 2 * LANES), F32)], axis=1)
        atom = pl.ds(pl.multiple_of(q * 16, 16), 16)
        rows = pl.ds(pl.multiple_of(index * 16, 16), 16)
        kind = wide(colb[3, atom, :], KLANES)
        placed = jnp.where(kind < 0.5, values, 0.0)
        for n in range(1, SPECIES):
            moved = pltpu.roll(values, n * PAIRS, 1)
            placed = jnp.where((kind > n - 0.5) & (kind < n + 0.5), moved, placed)
        wre[rows, :] = (placed * even).astype(BF16)
        wim[rows, :] = (placed * odd).astype(BF16)

    def half(h):
        loop(part * h, part * (h + 1), weights)
        rows = pl.ds(pl.multiple_of(h * part * 16, part * 16), part * 16)
        for t in range(NPL):
            lanes = slice(t * ct, (t + 1) * ct)
            table = tab[:, lanes]
            amp_re = dot_nn(wre[rows, :depth], table)
            amp_im = dot_nn(wim[rows, :depth], table)
            c, s = phase[0, rows, lanes], phase[1, rows, lanes]
            augrow[0:1, lanes] += jnp.sum(amp_re * c + amp_im * s, axis=0, keepdims=True)
            augrow[1:2, lanes] += jnp.sum(amp_im * c - amp_re * s, axis=0, keepdims=True)

    loop(0, 2, half)

    pad_z = tz.shape[2] // 2
    wide_row = round_up(columns, LANES)
    shape = (STK, pad_z)
    slot_id = lax.broadcasted_iota(jnp.int32, shape, 0)
    lane_id = lax.broadcasted_iota(jnp.int32, shape, 1)
    values = []
    for n in range(2):
        row = augrow[n : n + 1, :]
        picked = jnp.zeros(shape, F32)
        for t in range(STK):
            moved = pltpu.roll(row, wide_row - t * nz, 1) if t else row
            picked = jnp.where(slot_id == t, moved[:, :pad_z], picked)
        values.append(jnp.where(lane_id < nz, picked, 0.0))
    a_re, a_im = values
    pair = jnp.concatenate(
        [jnp.concatenate([a_re, -a_im], axis=1), jnp.concatenate([a_im, a_re], axis=1)], axis=0
    )
    group = lax.broadcasted_iota(jnp.int32, (LANES, 1), 0) // (2 * STK)
    placed = jnp.where(group == j % 8, jnp.concatenate([pair] * 8, axis=0), 0.0)
    hi, lo = split(placed)
    planes = dot_nt(tz[0], hi) + dot_nt(tz[0], lo) + dot_nt(tz[1], hi)
    send_v[...] = planes.reshape(ng, 8, LANES)
    recv_v[j] = send_v[j]

    def copy_v(k):
        return copy_ga(send_v.at[(j + k) % ng], recv_v.at[j], v_ssem, v_rsem, k)

    loop(1, ng, lambda k: copy_v(k).start())
    loop(1, ng, lambda k: copy_v(k).wait_recv())

    groups = max(ng // 8, 1)
    expand = (
        lax.broadcasted_iota(jnp.int32, (8, LANES), 1) // 16
        == lax.broadcasted_iota(jnp.int32, (8, LANES), 0)
    ).astype(BF16)
    for q in range(groups):
        tile = recv_v[8 * q]
        for n in range(1, 8):
            tile = tile + recv_v[8 * q + n]
        hi, lo = split(tile.T)
        spread = dot_nn(hi, expand) + dot_nn(lo, expand)
        spread = spread.reshape(8, 2, STK, LANES)
        for n in range(2):
            vexp[n, q * 8 * STK : (q + 1) * 8 * STK, :] = spread[:, n].reshape(8 * STK, LANES)

    def y_block(n):
        c, s = ey[n, 0], ey[n, 1]
        v_re, v_im = vexp[0], vexp[1]
        z = jnp.concatenate([v_re * c - v_im * s, v_re * s + v_im * c], axis=1)
        hi, lo = split(z)
        hot = onehot[...]
        return (dot_nn(hot, hi) + dot_nn(hot, lo))[:NXB]

    def copy_y(k):
        off = band_offset(k)
        return copy_band(send_y.at[off], recv_y.at[b], y_ssem, y_rsem, off)

    def send_block(k):
        off = band_offset(k)
        send_y[off] = y_block((b + off) % nb)
        copy_y(k).start()

    loop(0, nb - 1, send_block)
    recv_y[b] = y_block(b)

    def end_band(k):
        off = band_offset(k)
        copy_band(send_z, recv_z.at[off], z_ssem, z_rsem, off).wait_send()

    def end_ga(k):
        copy_ga(send_a, recv_a.at[j], a_ssem, a_rsem, k).wait_send()
        copy_v(k).wait_send()

    loop(0, nb - 1, end_band)
    loop(1, ng, end_ga)
    loop(0, nb - 1, lambda k: copy_y(k).wait_recv())

    gap = jnp.zeros((1, 2 * LANES), F32)
    field = jnp.concatenate([x for n in range(nb) for x in (recv_y[n], gap)], axis=0).T
    f_re, f_im = field[:LANES], field[LANES:]
    left = jnp.concatenate(
        [jnp.concatenate([f_re, -f_im], axis=1), jnp.concatenate([f_im, f_re], axis=1)], axis=0
    )
    hi, lo = split(left)
    result = dot_nn(hi, tx[0]) + dot_nn(lo, tx[0]) + dot_nn(hi, tx[1])
    for n in range(2):
        for p in range(NPL):
            first = n * LANES + p * 16
            out_ref[n, p] = result[first : first + NXB, :nx]

    loop(0, nb - 1, lambda k: copy_y(k).wait_send())


def both_parts(table):
    hi = table.astype(jnp.bfloat16)
    lo = (table - hi.astype(np.float64)).astype(jnp.bfloat16)
    return np.stack([hi, lo])


def tables(nb, ng):
    nx, nz = NXB * nb, NPL * ng
    pad_z = round_up(nz, LANES)
    plane = np.arange(8 * ng) // 8 * NPL + np.arange(8 * ng) % 8
    angle = (plane[:, None] * np.arange(nz)[None, :] % nz) * (2 * np.pi / nz)
    real = (np.arange(8 * ng) % 8 < NPL)[:, None]
    tz = np.zeros((8 * ng, 2 * pad_z))
    tz[:, :nz] = np.where(real, np.cos(angle), 0.0)
    tz[:, pad_z : pad_z + nz] = np.where(real, np.sin(angle), 0.0)
    pad_x = round_up(nx, LANES)
    row = np.arange(16 * nb)
    x = row // 16 * NXB + row % 16
    angle = (x[:, None] * np.arange(nx)[None, :] % nx) * (2 * np.pi / nx)
    real = (row % 16 < NXB)[:, None]
    tx = np.zeros((2 * 16 * nb, pad_x))
    tx[: 16 * nb, :nx] = np.where(real, np.cos(angle), 0.0)
    tx[16 * nb :, :nx] = np.where(real, np.sin(angle), 0.0)
    first, second = np.triu_indices(NH)
    ell = np.array(ELL)
    parity = np.tile((ell[first] + ell[second]) % 2, SPECIES)
    even = np.zeros((2, KLANES), np.float32)
    even[0, : SPECIES * PAIRS] = 1 - parity
    even[1, : SPECIES * PAIRS] = -parity
    return jnp.asarray(both_parts(tz)), jnp.asarray(both_parts(tx)), jnp.asarray(even)


def on_device(
    waves, occupations, beta_table, wave_miller, atom_kinds, atom_sites, aug_table, stick_columns
):
    nb, ng = lax.axis_size("band"), lax.axis_size("ga")
    nx, nz = NXB * nb, NPL * ng
    atoms, slots = OWN_ATOMS * ng, STK * ng
    wave_count = waves.shape[2]
    gt_lanes = min(256, wave_count)
    tiles = wave_count // gt_lanes
    columns = STK * nz
    steps = ng // 2 // DESTS
    chips = ng // 2
    tz, tx, even = tables(nb, ng)
    vmem = pl.BlockSpec(memory_space=pltpu.VMEM)
    hbm = pl.BlockSpec(memory_space=pltpu.HBM)
    dma = pltpu.SemaphoreType.DMA
    return pl.pallas_call(
        functools.partial(kernel, nb, ng, gt_lanes),
        out_shape=jax.ShapeDtypeStruct((2, NPL, NXB, nx), F32),
        in_specs=[hbm] * 11,
        out_specs=vmem,
        scratch_shapes=[
            pltpu.VMEM(waves.shape, BF16),
            pltpu.VMEM((1, waves.shape[1]), F32),
            pltpu.VMEM(beta_table.shape, F32),
            pltpu.VMEM(wave_miller.shape, jnp.int32),
            pltpu.VMEM((1, atoms), jnp.int32),
            pltpu.VMEM(atom_sites.shape, jnp.int32),
            pltpu.SMEM(stick_columns.shape, jnp.int32),
            pltpu.VMEM(even.shape, F32),
            pltpu.VMEM(aug_table.shape, BF16),
            pltpu.VMEM(tz.shape, BF16),
            pltpu.VMEM(tx.shape, BF16),
            dma((11,)),
            pltpu.VMEM((4, atoms, LANES), F32),
            pltpu.VMEM((atoms, LANES), jnp.int32),
            pltpu.VMEM((NH, 8, wave_count), F32),
            pltpu.VMEM((8, wave_count), F32),
            pltpu.VMEM((tiles, 4 * gt_lanes, LANES), BF16),
            pltpu.VMEM((DESTS * ROWS, LANES), F32),
            pltpu.VMEM((steps, DESTS * ROWS, LANES), F32),
            pltpu.VMEM((steps, DESTS * ROWS, LANES), F32),
            pltpu.VMEM((chips, ROWS, LANES), F32),
            pltpu.VMEM((chips, ROWS, LANES), F32),
            pltpu.VMEM((STK, LANES), F32),
            pltpu.VMEM((ng, STK, LANES), F32),
            pltpu.VMEM((8, LANES), F32),
            pltpu.VMEM((2, atoms, columns), F32),
            pltpu.VMEM((FOLD, LANES), F32),
            pltpu.VMEM((nb, FOLD, LANES), F32),
            pltpu.VMEM((FOLD, LANES), F32),
            pltpu.VMEM((ng, FOLD, LANES), F32),
            pltpu.VMEM((atoms, KLANES), BF16),
            pltpu.VMEM((atoms, KLANES), BF16),
            pltpu.VMEM((8, round_up(columns, LANES)), F32),
            pltpu.VMEM((ng, 8, LANES), F32),
            pltpu.VMEM((ng, 8, LANES), F32),
            pltpu.VMEM((nb, 2, slots, LANES), F32),
            pltpu.VMEM((16, slots), BF16),
            pltpu.VMEM((2, slots, LANES), F32),
            pltpu.VMEM((nb, NXB, 2 * LANES), F32),
            pltpu.VMEM((nb, NXB, 2 * LANES), F32),
            dma((steps,)),
            dma((steps,)),
            dma((chips,)),
            dma((chips,)),
            dma((ng,)),
            dma((ng,)),
            dma((nb,)),
            dma((nb,)),
            dma((ng,)),
            dma((ng,)),
            dma((ng,)),
            dma((ng,)),
            dma((nb,)),
            dma((nb,)),
        ],
        compiler_params=pltpu.CompilerParams(
            collective_id=0, has_side_effects=True, vmem_limit_bytes=VMEM_LIMIT
        ),
    )(
        waves,
        occupations[None],
        beta_table,
        wave_miller,
        atom_kinds[None],
        atom_sites,
        aug_table,
        stick_columns,
        tz,
        tx,
        even,
    )


def solution(mesh):
    in_specs = (
        P(None, "band", "ga"),
        P("band"),
        P(None, "ga"),
        P(None, "ga"),
        P(),
        P(),
        P(None, ("band", "ga")),
        P(("band", "ga")),
    )
    out_specs = P(None, "ga", "band", None)
    return jax.shard_map(
        on_device, mesh=mesh, in_specs=in_specs, out_specs=out_specs, check_vma=False
    )
```

```python
import functools
import math

import jax
import jax.numpy as jnp
import numpy as np
from jax import lax
from jax.experimental import pallas as pl
from jax.experimental.pallas import tpu as pltpu
from jax.sharding import PartitionSpec as P

NH = 18
PAIRS = 171
SPECIES = 4
NXB = 15
NPL = 7
STK = 8
OWN_ATOMS = 8
HALF = NH // 2
ROWS = HALF * OWN_ATOMS
DESTS = 4
LANES = 128
KLANES = 768
FOLD = OWN_ATOMS * 3 // 2
VMEM_LIMIT = 67043328
UNROLL = 4

ELL = [0] * 2 + [1] * 6 + [2] * 10
COS = (0.999999989, -19.7392045, 64.9391175, -85.4501395, 60.167631, -25.9675992, 6.52865816)
SIN = (6.28318492, -41.3415892, 81.5999433, -76.6144725, 41.3428824, -12.4712435)

FULL = (
    ((0, 2), (1, 2), (2, 2), (3, 2), (2, 0), (2, 3), (0, 3), (3, 0))
    + ((3, 1), (1, 1), (0, 0), (0, 1), (1, 0), (1, 3), (2, 1), (3, 3)),
    {0: (0, 1), 1: (0, 3), 2: (0, 1), 3: (0, 3), 4: (1, 0), 5: (3, 0)},
    {11: (0,), 12: (4,), 13: (1,), 14: (2,), 15: (3, 5)},
)
SMALL = (((1, 1), (1, 0), (0, 1), (0, 0)), {}, {})

MESH = pl.DeviceIdType.MESH
F32 = jnp.float32
BF16 = jnp.bfloat16
highest = lax.Precision.HIGHEST


def round_up(value, step):
    return (value + step - 1) // step * step


def cos_sin(turns):
    u = turns - jnp.floor(turns + 0.5)
    w = u * u
    c = COS[-1]
    for a in COS[-2::-1]:
        c = c * w + a
    s = SIN[-1]
    for a in SIN[-2::-1]:
        s = s * w + a
    return c, s * u


def turns_of(product, length):
    inverse = 1.0 / length
    return (product - length * jnp.floor(product * inverse)) * inverse


def split(x):
    hi = x.astype(BF16)
    return hi, (x - hi.astype(F32)).astype(BF16)


def dot_nt(a, b, **kw):
    return lax.dot_general(a, b, (((1,), (1,)), ((), ())), preferred_element_type=F32, **kw)


def dot_nn(a, b, **kw):
    return lax.dot_general(a, b, (((1,), (0,)), ((), ())), preferred_element_type=F32, **kw)


def kernel(
    nb,
    ng,
    gt_lanes,
    waves_hbm,
    occ_hbm,
    beta_hbm,
    mil_hbm,
    kinds_hbm,
    sites_hbm,
    tab_hbm,
    sticks_hbm,
    tz_hbm,
    tx_hbm,
    even_hbm,
    spread_hbm,
    out_ref,
    waves_ref,
    occ_ref,
    beta_ref,
    mil_ref,
    kinds_ref,
    sites_ref,
    sticks_ref,
    even_ref,
    spread_ref,
    tab,
    tz,
    tx,
    local_sem,
    colb,
    kindb,
    species,
    mil,
    wmat,
    acc,
    send_p,
    recv_p,
    send_b,
    recv_b,
    recv_r,
    send_c,
    recv_c,
    occ_row,
    phase,
    send_z,
    recv_z,
    send_a,
    recv_a,
    wre,
    wim,
    augrow,
    send_v,
    recv_v,
    ey,
    onehot,
    vexp,
    send_y,
    recv_y,
    p_ssem,
    p_rsem,
    b_ssem,
    b_rsem,
    r_rsem,
    c_ssem,
    c_rsem,
    z_ssem,
    z_rsem,
    a_ssem,
    a_rsem,
    v_ssem,
    v_rsem,
    y_ssem,
    y_rsem,
):
    nx, nz = NXB * nb, NPL * ng
    atoms = OWN_ATOMS * ng
    slots = STK * ng
    band_dev, wave_count = waves_ref.shape[1], waves_ref.shape[2]
    tiles = wave_count // gt_lanes
    steps = ng // 2 // DESTS
    cy = 4 if ng == 32 else 2
    cx = ng // 2 // cy
    columns = STK * nz
    ct = columns // NPL
    b = lax.axis_index("band")
    j = lax.axis_index("ga")
    core = j % 2
    chip = j // 2
    chip_y = chip // cx
    chip_x = chip % cx

    ends = [
        (sites_hbm, sites_ref),
        (kinds_hbm, kinds_ref),
        (mil_hbm, mil_ref),
        (sticks_hbm, sticks_ref),
        (waves_hbm, waves_ref),
        (beta_hbm, beta_ref),
        (occ_hbm, occ_ref),
        (even_hbm, even_ref),
        (spread_hbm, spread_ref),
        (tz_hbm, tz),
        (tx_hbm, tx),
        (tab_hbm, tab),
    ]
    local = [pltpu.make_async_copy(*pair, local_sem.at[n]) for n, pair in enumerate(ends)]
    for copy in local:
        copy.start()

    barrier = pltpu.get_barrier_semaphore()

    def greet_ga(k, carry):
        pl.semaphore_signal(barrier, inc=1, device_id=(b, (j + k) % ng), device_id_type=MESH)
        return carry

    def greet_band(k, carry):
        pl.semaphore_signal(barrier, inc=1, device_id=((b + k) % nb, j), device_id_type=MESH)
        return carry

    lax.fori_loop(1, nb, greet_band, 0)
    lax.fori_loop(1, ng, greet_ga, 0)

    for copy in local[:7]:
        copy.wait()

    cols = jnp.concatenate(
        [
            sites_ref[...].astype(F32),
            kinds_ref[...].astype(F32),
            jnp.zeros((4, atoms), F32),
        ],
        axis=0,
    ).T
    for n in range(4):
        colb[n] = jnp.broadcast_to(cols[:, n : n + 1], (atoms, LANES))
    kindb[...] = colb[3].astype(jnp.int32)
    kind_row = lax.broadcasted_iota(jnp.int32, (8, wave_count), 0)
    for i in range(NH):
        beta = [beta_ref[n * NH + i : n * NH + i + 1, :] for n in range(SPECIES)]
        species[i] = jnp.where(
            kind_row < 2,
            jnp.where(kind_row < 1, beta[0], beta[1]),
            jnp.where(kind_row < 3, beta[2], beta[3]),
        )
    mil[0:3, :] = mil_ref[...].astype(F32)
    occ_row[...] = jnp.zeros(occ_row.shape, F32)
    occ_row[0:1, 0:band_dev] = occ_ref[...]
    stick = [sticks_ref[t].astype(F32) for t in range(STK)]
    mine = jnp.zeros((1, LANES), F32)
    for t in range(STK):
        mine = jnp.where(lax.broadcasted_iota(jnp.int32, (1, LANES), 1) == t, stick[t], mine)
    send_c[...] = mine
    recv_c[j] = mine

    width = 2 * band_dev
    for g in range(tiles):
        lanes = slice(g * gt_lanes, (g + 1) * gt_lanes)
        wr = waves_ref[0, :, lanes].astype(F32)
        wi = waves_ref[1, :, lanes].astype(F32)
        none = jnp.zeros((LANES - width, gt_lanes), F32)
        with_cos = jnp.concatenate([wr, wi], axis=0)
        with_sin = jnp.concatenate([-wi, wr], axis=0)
        for h in range(2):
            for n, part in enumerate((with_cos, with_sin)):
                full = jnp.concatenate([part, none] if h == 0 else [none, part], axis=0)
                wmat[g, (2 * h + n) * gt_lanes : (2 * h + n + 1) * gt_lanes, :] = full.T.astype(BF16)

    def wide(x, lanes):
        return jnp.concatenate([x] * (lanes // LANES), axis=1) if lanes > LANES else x[:, :lanes]

    order, relays, added = FULL if ng == 32 else SMALL
    last = cy * cx - 1

    def chip_at(dy, dx):
        return ((chip_y + dy) % cy) * cx + (chip_x + dx) % cx

    def near_chip(index):
        return chip_at(index // cx, index % cx)

    def ordered_chip(step, d):
        power = 1 + 3 * step + 9 * (step * (step - 1) // 2) + 27 * (step * (step - 1) * (step - 2) // 6)
        code = [sum(order[n * DESTS + d][axis] * 4**n for n in range(steps)) for axis in range(2)]
        return chip_at(*(value // power % 4 for value in code))

    def project(step, parity):
        places = [ordered_chip(step, d) for d in range(DESTS)]

        def rows_of(d):
            dest = 2 * places[d] + parity
            return pl.ds(pl.multiple_of(dest * OWN_ATOMS, OWN_ATOMS), OWN_ATOMS)

        def tile(g):
            whole = [[], [], [], []]
            for piece in range(gt_lanes // LANES):
                lanes = pl.ds(pl.multiple_of(g * gt_lanes + piece * LANES, LANES), LANES)
                m1, m2, m3 = mil[0:1, lanes], mil[1:2, lanes], mil[2:3, lanes]
                pairs, kinds = [], []
                for d in range(DESTS):
                    rows = rows_of(d)
                    p1, p2, p3 = (colb[n, rows, :] for n in range(3))
                    kinds.append(kindb[rows, :])
                    turns = turns_of(p1 * m1 + p2 * m2, nx) + turns_of(p3 * m3, nz)
                    c, s = cos_sin(turns)
                    pairs.append(((c, s), (-s, c), (-c, -s)))
                parts = [[[None] * HALF for d in range(DESTS)] for n in range(4)]
                for i in range(NH):
                    beta = species[i, :, lanes]
                    for d in range(DESTS):
                        radial = jnp.take_along_axis(beta, kinds[d], axis=0)
                        first, second = pairs[d][ELL[i]]
                        h = i // HALF
                        parts[2 * h][d][i % HALF] = radial * first
                        parts[2 * h + 1][d][i % HALF] = radial * second
                for n in range(4):
                    whole[n].append(jnp.concatenate(sum(parts[n], []), axis=0).astype(BF16))
            left = jnp.concatenate(sum(whole, []), axis=1)
            return dot_nn(left, wmat[g])

        together = min(UNROLL, tiles)

        def some(n, carry):
            total = tile(n * together)
            for g in range(1, together):
                total = total + tile(n * together + g)
            acc[...] = total if together == tiles else acc[...] + total
            return carry

        if together == tiles:
            some(0, 0)
        else:
            acc[...] = jnp.zeros(acc.shape, F32)
            lax.fori_loop(0, tiles // together, some, 0)

    def for_partner(step, carry):
        project(step, 1 - core)
        send_p[step] = acc[...]
        return carry

    lax.fori_loop(0, steps, for_partner, 0)
    pl.semaphore_wait(barrier, (nb - 1) + (ng - 1))

    def copy_p(step):
        return pltpu.make_async_remote_copy(
            send_p.at[step],
            recv_p.at[step],
            p_ssem.at[step],
            p_rsem.at[step],
            device_id=(b, chip * 2 + 1 - core),
            device_id_type=MESH,
        )

    def copy_ga(source, target, ssem, rsem, k):
        return pltpu.make_async_remote_copy(
            source,
            target,
            ssem.at[k],
            rsem.at[k],
            device_id=(b, (j + k) % ng),
            device_id_type=MESH,
        )

    def band_offset(k):
        half = nb // 2
        m = (k + 1) // 2
        return half + m * (1 - 2 * (k % 2))

    def copy_band(source, target, ssem, rsem, off):
        return pltpu.make_async_remote_copy(
            source,
            target,
            ssem.at[off],
            rsem.at[off],
            device_id=((b + off) % nb, j),
            device_id_type=MESH,
        )

    def loop(low, high, body):
        def step(k, carry):
            body(k)
            return carry

        lax.fori_loop(low, high, step, 0)

    loop(0, steps, lambda s: copy_p(s).start())
    loop(1, ng, lambda k: copy_ga(send_c, recv_c.at[j], c_ssem, c_rsem, k).start())

    def copy_b(index):
        target = chip_at(*relays.get(index, order[index]))
        landed, sem = (recv_r, r_rsem) if index in relays else (recv_b, b_rsem)
        return pltpu.make_async_remote_copy(
            send_b.at[index],
            landed.at[index],
            b_ssem.at[index],
            sem.at[index],
            device_id=(b, 2 * target + core),
            device_id_type=MESH,
        )

    sent = [n for n in range(len(order)) if order[n] != (0, 0)]
    direct = [n for n in sent if n not in relays]
    own = order.index((0, 0))

    def for_owners(step, carry):
        project(step, core)
        copy_p(step).wait_recv()

        def deliver(now):
            for d in range(DESTS):
                index = now * DESTS + d
                rows = slice(d * ROWS, (d + 1) * ROWS)
                send_b[index] = acc[rows, :] + recv_p[now, rows, :]
                if index != own and index not in added:
                    copy_b(index).start()

        for now in range(steps):
            pl.when(step == now)(functools.partial(deliver, now))
        return carry

    lax.fori_loop(0, steps, for_owners, 0)
    for index in added:
        block = send_b[index]
        for n in added[index]:
            copy_b(n).wait_recv()
            block = block + recv_r[n]
        send_b[index] = block
        copy_b(index).start()

    loop(1, ng, lambda k: copy_ga(send_c, recv_c.at[j], c_ssem, c_rsem, k).wait_recv())
    owners = recv_c[:, 0, :]
    column = jnp.concatenate(
        [jnp.broadcast_to(owners[:, n : n + 1], (ng, LANES)) for n in range(STK)], axis=0
    )
    slot_x = jnp.floor((column + 0.5) * (1.0 / nx))
    hot = (slot_x == lax.broadcasted_iota(jnp.int32, (slots, LANES), 1).astype(F32)).astype(F32)
    onehot[...] = hot.T[0:16].astype(BF16)
    vexp[0] = column - slot_x * nx
    lane_y = (lax.broadcasted_iota(jnp.int32, (1, LANES), 1) % 16).astype(F32)
    some_rows = 32

    def y_phases(r):
        rows = pl.ds(pl.multiple_of(r * some_rows, some_rows), some_rows)
        slot_y = vexp[0, rows, :]
        c, s = cos_sin(turns_of(slot_y * lane_y, nx))
        dc, ds = cos_sin(turns_of(slot_y * float(NXB), nx))
        for n in range(nb):
            ey[n, 0, rows, :] = c
            ey[n, 1, rows, :] = s
            c, s = c * dc - s * ds, s * dc + c * ds

    loop(0, slots // some_rows, y_phases)

    loop(0, steps, lambda s: copy_p(s).wait_send())
    loop(1, ng, lambda k: copy_ga(send_c, recv_c.at[j], c_ssem, c_rsem, k).wait_send())
    for index in direct:
        copy_b(index).wait_recv()
    becp = send_b[own]
    for index in direct:
        becp = becp + recv_b[index]
    occ = occ_row[...]
    occ = sum((pltpu.roll(occ, n * band_dev, 1) for n in range(1, LANES // band_dev)), occ)[0:1]
    lane = lax.broadcasted_iota(jnp.int32, (1, LANES), 1)
    occ = jnp.where(lane < width, occ, 0.0)
    both = jnp.concatenate([becp, pltpu.roll(becp, LANES - width, 1)], axis=0)
    gram = dot_nt(both * occ, both, precision=highest)
    rows = NH * OWN_ATOMS
    row_id = lax.broadcasted_iota(jnp.int32, (rows, rows), 0)
    col_id = lax.broadcasted_iota(jnp.int32, (rows, rows), 1)
    gram = jnp.where(row_id % OWN_ATOMS == col_id % OWN_ATOMS, gram, 0.0)
    pick = (
        lax.broadcasted_iota(jnp.int32, (rows, LANES), 0) // OWN_ATOMS
        == lax.broadcasted_iota(jnp.int32, (rows, LANES), 1)
    ).astype(F32)
    square = dot_nn(gram, pick, precision=highest)
    total = jnp.zeros((OWN_ATOMS, 2 * LANES), F32)
    for i in range(NH):
        factor = jnp.where(lane < i, 0.0, jnp.where(lane == i, 1.0, 2.0))
        factor = jnp.where(lane < NH, factor, 0.0)
        piece = square[i * OWN_ATOMS : (i + 1) * OWN_ATOMS] * factor
        piece = jnp.concatenate([piece, jnp.zeros((OWN_ATOMS, LANES), F32)], axis=1)
        shift = i * NH - i * (i - 1) // 2 - i
        total = total + (pltpu.roll(piece, shift, 1) if shift else piece)
    folded = total[:4, LANES:] + pltpu.roll(total[4:, LANES:], LANES // 2, 1)
    total = jnp.concatenate([total[:, :LANES], folded], axis=0)
    send_z[...] = total
    recv_z[0] = total

    def send_band(k):
        off = band_offset(k)
        copy_band(send_z, recv_z.at[off], z_ssem, z_rsem, off).start()

    loop(0, nb - 1, send_band)

    column = jnp.zeros((1, LANES), F32)
    for n in range(STK):
        column = jnp.where(lane == n, stick[n], column)
    stick_x = jnp.floor((column + 0.5) * (1.0 / nx))
    stick_y = column - stick_x * nx
    stick_x = stick_x + (b * NXB).astype(F32)
    lane_tiles = phase.shape[2] // LANES
    period = min(nz // math.gcd(nz, LANES), lane_tiles)
    heights = []
    for q in range(period):
        g = (lane + q * LANES).astype(F32)
        heights.append(g - nz * jnp.floor((g + 0.5) * (1.0 / nz)))

    def phases(r):
        source = 2 * near_chip(r // 2) + r % 2
        atom = pl.ds(pl.multiple_of(source * 8, 8), 8)
        p1, p2, p3 = (colb[n, atom, :] for n in range(3))
        rows = pl.ds(pl.multiple_of(r * 8, 8), 8)
        flat = cos_sin(turns_of(p1 * stick_x + p2 * stick_y, nx))
        flat = [[jnp.broadcast_to(x[:, n : n + 1], (8, LANES)) for n in range(STK)] for x in flat]
        tall = [cos_sin(turns_of(p3 * z, nz)) for z in heights]
        for t in range(lane_tiles):
            low = t * LANES // nz
            high = min(((t + 1) * LANES - 1) // nz, STK - 1)
            c, s = (x[low] for x in flat)
            for n in range(low + 1, high + 1):
                before = lane < n * nz - t * LANES
                c, s = jnp.where(before, c, flat[0][n]), jnp.where(before, s, flat[1][n])
            cz, sz = tall[t % period]
            lanes = slice(t * LANES, (t + 1) * LANES)
            phase[0, rows, lanes] = c * cz - s * sz
            phase[1, rows, lanes] = s * cz + c * sz

    loop(0, atoms // 8, phases)
    for index in sent:
        copy_b(index).wait_send()
    def wait_band(k):
        off = band_offset(k)
        copy_band(send_z, recv_z.at[off], z_ssem, z_rsem, off).wait_recv()

    loop(0, nb - 1, wait_band)
    total = recv_z[0]
    for n in range(1, nb):
        total = total + recv_z[n]
    send_a[...] = total
    recv_a[j] = total
    loop(1, ng, lambda k: copy_ga(send_a, recv_a.at[j], a_ssem, a_rsem, k).start())
    for copy in local[7:]:
        copy.wait()

    even = even_ref[0:1, :]
    odd = even_ref[1:2, :]
    depth = SPECIES * PAIRS
    part = (last + 1) // 2
    augrow[...] = jnp.zeros(augrow.shape, F32)

    def arrive(k):
        copy_ga(send_a, recv_a.at[j], a_ssem, a_rsem, k).wait_recv()

    def weights(index):
        q = near_chip(index)

        @pl.when(index == 0)
        def _():
            arrive((j - (chip * 2 + 1 - core)) % ng)

        @pl.when(index > 0)
        def _():
            arrive((j - 2 * q) % ng)
            arrive((j - 2 * q - 1) % ng)

        values = []
        for n in range(2):
            got = recv_a[2 * q + n]
            first, rest = got[:OWN_ATOMS], got[OWN_ATOMS:]
            rest = jnp.concatenate([rest, pltpu.roll(rest, LANES // 2, 1)], axis=0)
            values.append(jnp.concatenate([first, rest], axis=1))
        values = jnp.concatenate(values, axis=0)
        position = lax.broadcasted_iota(jnp.int32, values.shape, 1)
        values = jnp.where(position < PAIRS, values, 0.0)
        values = jnp.concatenate([values, jnp.zeros((16, KLANES - 2 * LANES), F32)], axis=1)
        atom = pl.ds(pl.multiple_of(q * 16, 16), 16)
        rows = pl.ds(pl.multiple_of(index * 16, 16), 16)
        kind = wide(colb[3, atom, :], KLANES)
        placed = jnp.where(kind < 0.5, values, 0.0)
        for n in range(1, SPECIES):
            moved = pltpu.roll(values, n * PAIRS, 1)
            placed = jnp.where((kind > n - 0.5) & (kind < n + 0.5), moved, placed)
        wre[rows, :] = (placed * even).astype(BF16)
        wim[rows, :] = (placed * odd).astype(BF16)

    def half(h):
        loop(part * h, part * (h + 1), weights)
        rows = pl.ds(pl.multiple_of(h * part * 16, part * 16), part * 16)
        for t in range(NPL):
            lanes = slice(t * ct, (t + 1) * ct)
            table = tab[:, lanes]
            amp_re = dot_nn(wre[rows, :depth], table)
            amp_im = dot_nn(wim[rows, :depth], table)
            c, s = phase[0, rows, lanes], phase[1, rows, lanes]
            augrow[0:1, lanes] += jnp.sum(amp_re * c + amp_im * s, axis=0, keepdims=True)
            augrow[1:2, lanes] += jnp.sum(amp_im * c - amp_re * s, axis=0, keepdims=True)

    loop(0, 2, half)

    pad_z = tz.shape[2] // 2
    wide_row = round_up(columns, LANES)
    shape = (STK, pad_z)
    slot_id = lax.broadcasted_iota(jnp.int32, shape, 0)
    lane_id = lax.broadcasted_iota(jnp.int32, shape, 1)
    values = []
    for n in range(2):
        row = augrow[n : n + 1, :]
        picked = jnp.zeros(shape, F32)
        for t in range(STK):
            moved = pltpu.roll(row, wide_row - t * nz, 1) if t else row
            picked = jnp.where(slot_id == t, moved[:, :pad_z], picked)
        values.append(jnp.where(lane_id < nz, picked, 0.0))
    a_re, a_im = values
    pair = jnp.concatenate(
        [jnp.concatenate([a_re, -a_im], axis=1), jnp.concatenate([a_im, a_re], axis=1)], axis=0
    )
    hi, lo = split(jnp.concatenate([pair, jnp.zeros((LANES - 2 * STK, 2 * pad_z), F32)], axis=0))
    planes = dot_nt(tz[0], hi) + dot_nt(tz[0], lo) + dot_nt(tz[1], hi)
    plane_id = lax.broadcasted_iota(jnp.int32, planes.shape, 0) % 8
    line = jnp.where(plane_id == 0, planes, 0.0)
    for p in range(1, NPL):
        line = line + pltpu.roll(jnp.where(plane_id == p, planes, 0.0), p * 2 * STK, 1)
    send_v[:, 0, :] = jnp.sum(line.reshape(ng, 8, LANES), axis=1)
    recv_v[j] = send_v[j]

    def copy_v(k):
        return copy_ga(send_v.at[(j + k) % ng], recv_v.at[j], v_ssem, v_rsem, k)

    loop(1, ng, lambda k: copy_v(k).start())
    loop(1, ng, lambda k: copy_v(k).wait_recv())

    hi, lo = split(recv_v[:, 0, :])
    spread = dot_nn(jnp.concatenate([hi, lo], axis=1), spread_ref[...])
    for n in range(2):
        for t in range(STK):
            first = (n * STK + t) * LANES
            vexp[n, t * ng : (t + 1) * ng, :] = spread[:, first : first + LANES]

    def y_block(n):
        c, s = ey[n, 0], ey[n, 1]
        v_re, v_im = vexp[0], vexp[1]
        z = jnp.concatenate([v_re * c - v_im * s, v_re * s + v_im * c], axis=1)
        hi, lo = split(z)
        hot = onehot[...]
        return (dot_nn(hot, hi) + dot_nn(hot, lo))[:NXB]

    def copy_y(k):
        off = band_offset(k)
        return copy_band(send_y.at[off], recv_y.at[b], y_ssem, y_rsem, off)

    def send_block(k):
        off = band_offset(k)
        send_y[off] = y_block((b + off) % nb)
        copy_y(k).start()

    loop(0, nb - 1, send_block)
    recv_y[b] = y_block(b)

    def end_band(k):
        off = band_offset(k)
        copy_band(send_z, recv_z.at[off], z_ssem, z_rsem, off).wait_send()

    def end_ga(k):
        copy_ga(send_a, recv_a.at[j], a_ssem, a_rsem, k).wait_send()
        copy_v(k).wait_send()

    loop(0, nb - 1, end_band)
    loop(1, ng, end_ga)
    loop(0, nb - 1, lambda k: copy_y(k).wait_recv())

    gap = jnp.zeros((1, 2 * LANES), F32)
    field = jnp.concatenate([x for n in range(nb) for x in (recv_y[n], gap)], axis=0).T
    f_re, f_im = field[:LANES], field[LANES:]
    left = jnp.concatenate(
        [jnp.concatenate([f_re, -f_im], axis=1), jnp.concatenate([f_im, f_re], axis=1)], axis=0
    )
    hi, lo = split(left)
    result = dot_nn(hi, tx[0]) + dot_nn(lo, tx[0]) + dot_nn(hi, tx[1])
    for n in range(2):
        for p in range(NPL):
            first = n * LANES + p * 16
            out_ref[n, p] = result[first : first + NXB, :nx]

    loop(0, nb - 1, lambda k: copy_y(k).wait_send())


def both_parts(table):
    hi = table.astype(jnp.bfloat16)
    lo = (table - hi.astype(np.float64)).astype(jnp.bfloat16)
    return np.stack([hi, lo])


def tables(nb, ng):
    nx, nz = NXB * nb, NPL * ng
    pad_z = round_up(nz, LANES)
    plane = np.arange(8 * ng) // 8 * NPL + np.arange(8 * ng) % 8
    angle = (plane[:, None] * np.arange(nz)[None, :] % nz) * (2 * np.pi / nz)
    real = (np.arange(8 * ng) % 8 < NPL)[:, None]
    tz = np.zeros((8 * ng, 2 * pad_z))
    tz[:, :nz] = np.where(real, np.cos(angle), 0.0)
    tz[:, pad_z : pad_z + nz] = np.where(real, np.sin(angle), 0.0)
    pad_x = round_up(nx, LANES)
    row = np.arange(16 * nb)
    x = row // 16 * NXB + row % 16
    angle = (x[:, None] * np.arange(nx)[None, :] % nx) * (2 * np.pi / nx)
    real = (row % 16 < NXB)[:, None]
    tx = np.zeros((2 * 16 * nb, pad_x))
    tx[: 16 * nb, :nx] = np.where(real, np.cos(angle), 0.0)
    tx[16 * nb :, :nx] = np.where(real, np.sin(angle), 0.0)
    first, second = np.triu_indices(NH)
    ell = np.array(ELL)
    parity = np.tile((ell[first] + ell[second]) % 2, SPECIES)
    even = np.zeros((2, KLANES), np.float32)
    even[0, : SPECIES * PAIRS] = 1 - parity
    even[1, : SPECIES * PAIRS] = -parity
    lane = np.arange(2 * STK * LANES)
    source = lane % LANES // 16 * 16 + lane // LANES
    spread = (np.arange(LANES)[:, None] == source[None, :]) & (lane % LANES // 16 < NPL)[None, :]
    spread = np.concatenate([spread, spread]).astype(jnp.bfloat16)
    return (
        jnp.asarray(both_parts(tz)),
        jnp.asarray(both_parts(tx)),
        jnp.asarray(even),
        jnp.asarray(spread),
    )


def on_device(
    waves, occupations, beta_table, wave_miller, atom_kinds, atom_sites, aug_table, stick_columns
):
    nb, ng = lax.axis_size("band"), lax.axis_size("ga")
    nx, nz = NXB * nb, NPL * ng
    atoms, slots = OWN_ATOMS * ng, STK * ng
    wave_count = waves.shape[2]
    gt_lanes = min(256, wave_count)
    tiles = wave_count // gt_lanes
    columns = STK * nz
    steps = ng // 2 // DESTS
    chips = ng // 2
    tz, tx, even, spread = tables(nb, ng)
    vmem = pl.BlockSpec(memory_space=pltpu.VMEM)
    hbm = pl.BlockSpec(memory_space=pltpu.HBM)
    dma = pltpu.SemaphoreType.DMA
    return pl.pallas_call(
        functools.partial(kernel, nb, ng, gt_lanes),
        out_shape=jax.ShapeDtypeStruct((2, NPL, NXB, nx), F32),
        in_specs=[hbm] * 12,
        out_specs=vmem,
        scratch_shapes=[
            pltpu.VMEM(waves.shape, BF16),
            pltpu.VMEM((1, waves.shape[1]), F32),
            pltpu.VMEM(beta_table.shape, F32),
            pltpu.VMEM(wave_miller.shape, jnp.int32),
            pltpu.VMEM((1, atoms), jnp.int32),
            pltpu.VMEM(atom_sites.shape, jnp.int32),
            pltpu.SMEM(stick_columns.shape, jnp.int32),
            pltpu.VMEM(even.shape, F32),
            pltpu.VMEM(spread.shape, BF16),
            pltpu.VMEM(aug_table.shape, BF16),
            pltpu.VMEM(tz.shape, BF16),
            pltpu.VMEM(tx.shape, BF16),
            dma((12,)),
            pltpu.VMEM((4, atoms, LANES), F32),
            pltpu.VMEM((atoms, LANES), jnp.int32),
            pltpu.VMEM((NH, 8, wave_count), F32),
            pltpu.VMEM((8, wave_count), F32),
            pltpu.VMEM((tiles, 4 * gt_lanes, LANES), BF16),
            pltpu.VMEM((DESTS * ROWS, LANES), F32),
            pltpu.VMEM((steps, DESTS * ROWS, LANES), F32),
            pltpu.VMEM((steps, DESTS * ROWS, LANES), F32),
            pltpu.VMEM((chips, ROWS, LANES), F32),
            pltpu.VMEM((chips, ROWS, LANES), F32),
            pltpu.VMEM((6, ROWS, LANES), F32),
            pltpu.VMEM((1, LANES), F32),
            pltpu.VMEM((ng, 1, LANES), F32),
            pltpu.VMEM((8, LANES), F32),
            pltpu.VMEM((2, atoms, round_up(columns, LANES)), F32),
            pltpu.VMEM((FOLD, LANES), F32),
            pltpu.VMEM((nb, FOLD, LANES), F32),
            pltpu.VMEM((FOLD, LANES), F32),
            pltpu.VMEM((ng, FOLD, LANES), F32),
            pltpu.VMEM((atoms, KLANES), BF16),
            pltpu.VMEM((atoms, KLANES), BF16),
            pltpu.VMEM((8, round_up(columns, LANES)), F32),
            pltpu.VMEM((ng, 1, LANES), F32),
            pltpu.VMEM((ng, 1, LANES), F32),
            pltpu.VMEM((nb, 2, slots, LANES), F32),
            pltpu.VMEM((16, slots), BF16),
            pltpu.VMEM((2, slots, LANES), F32),
            pltpu.VMEM((nb, NXB, 2 * LANES), F32),
            pltpu.VMEM((nb, NXB, 2 * LANES), F32),
            dma((steps,)),
            dma((steps,)),
            dma((chips,)),
            dma((chips,)),
            dma((6,)),
            dma((ng,)),
            dma((ng,)),
            dma((nb,)),
            dma((nb,)),
            dma((ng,)),
            dma((ng,)),
            dma((ng,)),
            dma((ng,)),
            dma((nb,)),
            dma((nb,)),
        ],
        compiler_params=pltpu.CompilerParams(
            collective_id=0, has_side_effects=True, vmem_limit_bytes=VMEM_LIMIT
        ),
    )(
        waves,
        occupations[None],
        beta_table,
        wave_miller,
        atom_kinds[None],
        atom_sites,
        aug_table,
        stick_columns,
        tz,
        tx,
        even,
        spread,
    )


def solution(mesh):
    in_specs = (
        P(None, "band", "ga"),
        P("band"),
        P(None, "ga"),
        P(None, "ga"),
        P(),
        P(),
        P(None, ("band", "ga")),
        P(("band", "ga")),
    )
    out_specs = P(None, "ga", "band", None)
    return jax.shard_map(
        on_device, mesh=mesh, in_specs=in_specs, out_specs=out_specs, check_vma=False
    )
```

```python
import functools
import math

import jax
import jax.numpy as jnp
import numpy as np
from jax import lax
from jax.experimental import pallas as pl
from jax.experimental.pallas import tpu as pltpu
from jax.sharding import PartitionSpec as P

NH = 18
PAIRS = 171
SPECIES = 4
NXB = 15
NPL = 7
STK = 8
OWN_ATOMS = 8
HALF = NH // 2
ROWS = HALF * OWN_ATOMS
DESTS = 4
LANES = 128
KLANES = 768
FOLD = OWN_ATOMS * 3 // 2
VMEM_LIMIT = 67043328
UNROLL = 4

ELL = [0] * 2 + [1] * 6 + [2] * 10
COS = (0.999999989, -19.7392045, 64.9391175, -85.4501395, 60.167631, -25.9675992, 6.52865816)
SIN = (6.28318492, -41.3415892, 81.5999433, -76.6144725, 41.3428824, -12.4712435)

FULL = (
    ((0, 2), (1, 2), (2, 2), (3, 2), (2, 0), (2, 3), (0, 3), (3, 0))
    + ((3, 1), (1, 1), (0, 0), (0, 1), (1, 0), (1, 3), (2, 1), (3, 3)),
    {0: (0, 1), 1: (0, 3), 2: (0, 1), 3: (0, 3), 4: (1, 0), 5: (3, 0)},
    {11: (0,), 12: (4,), 13: (1,), 14: (2,), 15: (3, 5)},
)
SMALL = (((1, 1), (1, 0), (0, 1), (0, 0)), {}, {})

MESH = pl.DeviceIdType.MESH
F32 = jnp.float32
BF16 = jnp.bfloat16
highest = lax.Precision.HIGHEST


def round_up(value, step):
    return (value + step - 1) // step * step


def cos_sin(turns):
    u = turns - jnp.floor(turns + 0.5)
    w = u * u
    c = COS[-1]
    for a in COS[-2::-1]:
        c = c * w + a
    s = SIN[-1]
    for a in SIN[-2::-1]:
        s = s * w + a
    return c, s * u


def turns_of(product, length):
    inverse = 1.0 / length
    return (product - length * jnp.floor(product * inverse)) * inverse


def split(x):
    hi = x.astype(BF16)
    return hi, (x - hi.astype(F32)).astype(BF16)


def dot_nt(a, b, **kw):
    return lax.dot_general(a, b, (((1,), (1,)), ((), ())), preferred_element_type=F32, **kw)


def dot_nn(a, b, **kw):
    return lax.dot_general(a, b, (((1,), (0,)), ((), ())), preferred_element_type=F32, **kw)


def kernel(
    nb,
    ng,
    gt_lanes,
    waves_hbm,
    occ_hbm,
    beta_hbm,
    mil_hbm,
    kinds_hbm,
    sites_hbm,
    tab_hbm,
    sticks_hbm,
    tz_hbm,
    tx_hbm,
    even_hbm,
    out_ref,
    waves_ref,
    occ_ref,
    beta_ref,
    mil_ref,
    kinds_ref,
    sites_ref,
    sticks_ref,
    even_ref,
    tab,
    tz,
    tx,
    local_sem,
    colb,
    kindb,
    species,
    mil,
    wmat,
    acc,
    send_p,
    recv_p,
    send_b,
    recv_b,
    recv_r,
    send_c,
    recv_c,
    occ_row,
    phase,
    send_z,
    recv_z,
    send_a,
    recv_a,
    wmix,
    augrow,
    send_v,
    recv_v,
    recv_y,
    ey,
    onehot,
    send_k,
    recv_k,
    field,
    p_ssem,
    p_rsem,
    b_ssem,
    b_rsem,
    r_rsem,
    c_ssem,
    c_rsem,
    z_ssem,
    z_rsem,
    a_ssem,
    a_rsem,
    v_ssem,
    v_rsem,
    y_ssem,
    y_rsem,
    k_ssem,
    k_rsem,
):
    nx, nz = NXB * nb, NPL * ng
    atoms = OWN_ATOMS * ng
    slots = STK * ng
    band_dev, wave_count = waves_ref.shape[1], waves_ref.shape[2]
    tiles = wave_count // gt_lanes
    steps = ng // 2 // DESTS
    cy = 4 if ng == 32 else 2
    cx = ng // 2 // cy
    columns = STK * nz
    ct = columns // NPL
    b = lax.axis_index("band")
    j = lax.axis_index("ga")
    core = j % 2
    chip = j // 2
    chip_y = chip // cx
    chip_x = chip % cx

    ends = [
        (sites_hbm, sites_ref),
        (kinds_hbm, kinds_ref),
        (mil_hbm, mil_ref),
        (sticks_hbm, sticks_ref),
        (waves_hbm, waves_ref),
        (beta_hbm, beta_ref),
        (occ_hbm, occ_ref),
        (even_hbm, even_ref),
        (tz_hbm, tz),
        (tx_hbm, tx),
        (tab_hbm, tab),
    ]
    local = [pltpu.make_async_copy(*pair, local_sem.at[n]) for n, pair in enumerate(ends)]
    for copy in local:
        copy.start()

    barrier = pltpu.get_barrier_semaphore()

    for k in range(1, nb):
        pl.semaphore_signal(barrier, inc=1, device_id=(lax.rem(b + k, nb), j), device_id_type=MESH)
    for k in range(1, ng):
        pl.semaphore_signal(barrier, inc=1, device_id=(b, lax.rem(j + k, ng)), device_id_type=MESH)

    for copy in local[:7]:
        copy.wait()

    cols = jnp.concatenate(
        [
            sites_ref[...].astype(F32),
            kinds_ref[...].astype(F32),
            jnp.zeros((4, atoms), F32),
        ],
        axis=0,
    ).T
    for n in range(4):
        colb[n] = jnp.broadcast_to(cols[:, n : n + 1], (atoms, LANES))
    kindb[...] = colb[3].astype(jnp.int32)
    kind_row = lax.broadcasted_iota(jnp.int32, (8, wave_count), 0)
    for i in range(NH):
        beta = [beta_ref[n * NH + i : n * NH + i + 1, :] for n in range(SPECIES)]
        species[i] = jnp.where(
            kind_row < 2,
            jnp.where(kind_row < 1, beta[0], beta[1]),
            jnp.where(kind_row < 3, beta[2], beta[3]),
        )
    mil[0:3, :] = mil_ref[...].astype(F32)
    occ_row[...] = jnp.zeros(occ_row.shape, F32)
    occ_row[0:1, 0:band_dev] = occ_ref[...]
    stick = [sticks_ref[t].astype(F32) for t in range(STK)]
    mine = jnp.zeros((1, LANES), F32)
    for t in range(STK):
        mine = jnp.where(lax.broadcasted_iota(jnp.int32, (1, LANES), 1) == t, stick[t], mine)
    send_c[...] = mine
    recv_c[j] = mine

    width = 2 * band_dev
    for g in range(tiles):
        lanes = slice(g * gt_lanes, (g + 1) * gt_lanes)
        wr = waves_ref[0, :, lanes].astype(F32)
        wi = waves_ref[1, :, lanes].astype(F32)
        full = jnp.concatenate([wr, wi, -wi, wr], axis=0).T
        swapped = pltpu.roll(full, width, 1)
        low = lax.broadcasted_iota(jnp.int32, full.shape, 1) < width
        for n, part in enumerate(
            (
                jnp.where(low, full, 0.0),
                jnp.where(low, swapped, 0.0),
                jnp.where(low, 0.0, swapped),
                jnp.where(low, 0.0, full),
            )
        ):
            wmat[g, n * gt_lanes : (n + 1) * gt_lanes, :] = part.astype(BF16)

    def wide(x, lanes):
        return jnp.concatenate([x] * (lanes // LANES), axis=1) if lanes > LANES else x[:, :lanes]

    order, relays, added = FULL if ng == 32 else SMALL
    last = cy * cx - 1

    def chip_at(dy, dx):
        return ((chip_y + dy) % cy) * cx + (chip_x + dx) % cx

    def near_chip(index):
        return chip_at(index // cx, index % cx)

    def ordered_chip(step, d):
        power = 1 + 3 * step + 9 * (step * (step - 1) // 2) + 27 * (step * (step - 1) * (step - 2) // 6)
        code = [sum(order[n * DESTS + d][axis] * 4**n for n in range(steps)) for axis in range(2)]
        return chip_at(*(value // power % 4 for value in code))

    def project(step, parity):
        places = [ordered_chip(step, d) for d in range(DESTS)]

        def rows_of(d):
            dest = 2 * places[d] + parity
            return pl.ds(pl.multiple_of(dest * OWN_ATOMS, OWN_ATOMS), OWN_ATOMS)

        def tile(g):
            whole = [[], [], [], []]
            for piece in range(gt_lanes // LANES):
                lanes = pl.ds(pl.multiple_of(g * gt_lanes + piece * LANES, LANES), LANES)
                m1, m2, m3 = mil[0:1, lanes], mil[1:2, lanes], mil[2:3, lanes]
                pairs, kinds = [], []
                for d in range(DESTS):
                    rows = rows_of(d)
                    p1, p2, p3 = (colb[n, rows, :] for n in range(3))
                    kinds.append(kindb[rows, :])
                    turns = turns_of(p1 * m1 + p2 * m2, nx) + turns_of(p3 * m3, nz)
                    c, s = cos_sin(turns)
                    pairs.append(((c, s), (-s, c), (-c, -s)))
                parts = [[[None] * HALF for d in range(DESTS)] for n in range(4)]
                for i in range(NH):
                    beta = species[i, :, lanes]
                    for d in range(DESTS):
                        radial = jnp.take_along_axis(beta, kinds[d], axis=0)
                        first, second = pairs[d][ELL[i]]
                        h = i // HALF
                        parts[2 * h][d][i % HALF] = radial * first
                        parts[2 * h + 1][d][i % HALF] = radial * second
                for n in range(4):
                    whole[n].append(jnp.concatenate(sum(parts[n], []), axis=0).astype(BF16))
            left = jnp.concatenate(sum(whole, []), axis=1)
            return dot_nn(left, wmat[g])

        together = min(UNROLL, tiles)

        def some(n, carry):
            total = tile(n * together)
            for g in range(1, together):
                total = total + tile(n * together + g)
            acc[...] = total if together == tiles else acc[...] + total
            return carry

        if together == tiles:
            some(0, 0)
        else:
            acc[...] = jnp.zeros(acc.shape, F32)
            lax.fori_loop(0, tiles // together, some, 0)

    def for_partner(step, carry):
        project(step, 1 - core)
        send_p[step] = acc[...]
        return carry

    lax.fori_loop(0, steps, for_partner, 0)
    pl.semaphore_wait(barrier, (nb - 1) + (ng - 1))

    def copy_p(step):
        return pltpu.make_async_remote_copy(
            send_p.at[step],
            recv_p.at[step],
            p_ssem.at[step],
            p_rsem.at[step],
            device_id=(b, chip * 2 + 1 - core),
            device_id_type=MESH,
        )

    def copy_ga(source, target, ssem, rsem, k):
        return pltpu.make_async_remote_copy(
            source,
            target,
            ssem.at[k],
            rsem.at[k],
            device_id=(b, (j + k) % ng),
            device_id_type=MESH,
        )

    def band_offset(k):
        half = nb // 2
        m = (k + 1) // 2
        return half + m * (1 - 2 * (k % 2))

    def copy_band(source, target, ssem, rsem, off):
        return pltpu.make_async_remote_copy(
            source,
            target,
            ssem.at[off],
            rsem.at[off],
            device_id=((b + off) % nb, j),
            device_id_type=MESH,
        )

    def loop(low, high, body):
        def step(k, carry):
            body(k)
            return carry

        lax.fori_loop(low, high, step, 0)

    loop(0, steps, lambda s: copy_p(s).start())
    loop(1, ng, lambda k: copy_ga(send_c, recv_c.at[j], c_ssem, c_rsem, k).start())

    def copy_b(index):
        target = chip_at(*relays.get(index, order[index]))
        landed, sem = (recv_r, r_rsem) if index in relays else (recv_b, b_rsem)
        return pltpu.make_async_remote_copy(
            send_b.at[index],
            landed.at[index],
            b_ssem.at[index],
            sem.at[index],
            device_id=(b, 2 * target + core),
            device_id_type=MESH,
        )

    sent = [n for n in range(len(order)) if order[n] != (0, 0)]
    direct = [n for n in sent if n not in relays]
    own = order.index((0, 0))

    def for_owners(step, carry):
        project(step, core)
        copy_p(step).wait_recv()

        def deliver(now):
            for d in range(DESTS):
                index = now * DESTS + d
                rows = slice(d * ROWS, (d + 1) * ROWS)
                send_b[index] = acc[rows, :] + recv_p[now, rows, :]
                if index != own and index not in added:
                    copy_b(index).start()

        for now in range(steps):
            pl.when(step == now)(functools.partial(deliver, now))
        return carry

    lax.fori_loop(0, steps, for_owners, 0)
    for index in added:
        block = send_b[index]
        for n in added[index]:
            copy_b(n).wait_recv()
            block = block + recv_r[n]
        send_b[index] = block
        copy_b(index).start()

    loop(1, ng, lambda k: copy_ga(send_c, recv_c.at[j], c_ssem, c_rsem, k).wait_recv())
    owners = jnp.concatenate([recv_c[:, 0, :], jnp.zeros((LANES - ng, LANES), F32)], axis=0).T
    per_row = min(LANES // ng, STK)
    key_rows = STK // per_row
    keys = []
    for r in range(key_rows):
        row = owners[r * per_row : r * per_row + 1]
        for n in range(1, per_row):
            at = r * per_row + n
            row = row + pltpu.roll(owners[at : at + 1], n * ng, 1)
        keys.append(row)
    send_k[...] = jnp.concatenate(keys, axis=0)
    recv_k[b] = send_k[...]

    def send_keys(k):
        off = band_offset(k)
        copy_band(send_k, recv_k.at[b], k_ssem, k_rsem, off).start()

    loop(0, nb - 1, send_keys)
    loop(0, steps, lambda s: copy_p(s).wait_send())
    loop(1, ng, lambda k: copy_ga(send_c, recv_c.at[j], c_ssem, c_rsem, k).wait_send())
    for index in direct:
        copy_b(index).wait_recv()
    becp = send_b[own]
    for index in direct:
        becp = becp + recv_b[index]
    occ = occ_row[...]
    occ = sum((pltpu.roll(occ, n * band_dev, 1) for n in range(1, LANES // band_dev)), occ)[0:1]
    lane = lax.broadcasted_iota(jnp.int32, (1, LANES), 1)
    occ = jnp.where(lane < width, occ, 0.0)
    both = jnp.concatenate([becp, pltpu.roll(becp, LANES - width, 1)], axis=0)
    gram = dot_nt(both * occ, both, precision=highest)
    rows = NH * OWN_ATOMS
    row_id = lax.broadcasted_iota(jnp.int32, (rows, rows), 0)
    col_id = lax.broadcasted_iota(jnp.int32, (rows, rows), 1)
    gram = jnp.where(row_id % OWN_ATOMS == col_id % OWN_ATOMS, gram, 0.0)
    pick = (
        lax.broadcasted_iota(jnp.int32, (rows, LANES), 0) // OWN_ATOMS
        == lax.broadcasted_iota(jnp.int32, (rows, LANES), 1)
    ).astype(F32)
    square = dot_nn(gram, pick, precision=highest)
    total = jnp.zeros((OWN_ATOMS, 2 * LANES), F32)
    for i in range(NH):
        factor = jnp.where(lane < i, 0.0, jnp.where(lane == i, 1.0, 2.0))
        factor = jnp.where(lane < NH, factor, 0.0)
        piece = square[i * OWN_ATOMS : (i + 1) * OWN_ATOMS] * factor
        piece = jnp.concatenate([piece, jnp.zeros((OWN_ATOMS, LANES), F32)], axis=1)
        shift = i * NH - i * (i - 1) // 2 - i
        total = total + (pltpu.roll(piece, shift, 1) if shift else piece)
    folded = total[:4, LANES:] + pltpu.roll(total[4:, LANES:], LANES // 2, 1)
    total = jnp.concatenate([total[:, :LANES], folded], axis=0)
    send_z[...] = total
    recv_z[0] = total

    def send_band(k):
        off = band_offset(k)
        copy_band(send_z, recv_z.at[off], z_ssem, z_rsem, off).start()

    loop(0, nb - 1, send_band)

    column = jnp.zeros((1, LANES), F32)
    for n in range(STK):
        column = jnp.where(lane == n, stick[n], column)
    stick_x = jnp.floor((column + 0.5) * (1.0 / nx))
    stick_y = column - stick_x * nx
    stick_x = stick_x + (b * NXB).astype(F32)
    lane_tiles = phase.shape[2] // LANES
    period = min(nz // math.gcd(nz, LANES), lane_tiles)
    heights = []
    for q in range(period):
        g = (lane + q * LANES).astype(F32)
        heights.append(g - nz * jnp.floor((g + 0.5) * (1.0 / nz)))

    def phases(r):
        source = 2 * near_chip(r // 2) + r % 2
        atom = pl.ds(pl.multiple_of(source * 8, 8), 8)
        p1, p2, p3 = (colb[n, atom, :] for n in range(3))
        rows = pl.ds(pl.multiple_of(r * 8, 8), 8)
        flat = cos_sin(turns_of(p1 * stick_x + p2 * stick_y, nx))
        flat = [[jnp.broadcast_to(x[:, n : n + 1], (8, LANES)) for n in range(STK)] for x in flat]
        tall = [cos_sin(turns_of(p3 * z, nz)) for z in heights]
        for t in range(lane_tiles):
            low = t * LANES // nz
            high = min(((t + 1) * LANES - 1) // nz, STK - 1)
            c, s = (x[low] for x in flat)
            for n in range(low + 1, high + 1):
                before = lane < n * nz - t * LANES
                c, s = jnp.where(before, c, flat[0][n]), jnp.where(before, s, flat[1][n])
            cz, sz = tall[t % period]
            lanes = slice(t * LANES, (t + 1) * LANES)
            phase[0, rows, lanes] = c * cz - s * sz
            phase[1, rows, lanes] = s * cz + c * sz

    loop(0, atoms // 8, phases)
    for index in sent:
        copy_b(index).wait_send()
    def wait_band(k):
        off = band_offset(k)
        copy_band(send_z, recv_z.at[off], z_ssem, z_rsem, off).wait_recv()

    loop(0, nb - 1, wait_band)
    total = recv_z[0]
    for n in range(1, nb):
        total = total + recv_z[n]
    send_a[...] = total
    recv_a[j] = total
    loop(1, ng, lambda k: copy_ga(send_a, recv_a.at[j], a_ssem, a_rsem, k).start())
    for copy in local[7:]:
        copy.wait()

    even = even_ref[0:1, :]
    odd = even_ref[1:2, :]
    depth = SPECIES * PAIRS
    part = (last + 1) // 2
    augrow[...] = jnp.zeros(augrow.shape, F32)

    def arrive(k):
        copy_ga(send_a, recv_a.at[j], a_ssem, a_rsem, k).wait_recv()

    crowd = min(4, part)

    def weights(n):
        for index in range(crowd):
            index = index + n * crowd
            q = near_chip(index)

            @pl.when(index == 0)
            def _():
                arrive((j - (chip * 2 + 1 - core)) % ng)

            @pl.when(index > 0)
            def _():
                arrive((j - 2 * q) % ng)
                arrive((j - 2 * q - 1) % ng)

        for index in range(crowd):
            weigh(index + n * crowd)

    def weigh(index):
        q = near_chip(index)
        values = []
        for n in range(2):
            got = recv_a[2 * q + n]
            first, rest = got[:OWN_ATOMS], got[OWN_ATOMS:]
            rest = jnp.concatenate([rest, pltpu.roll(rest, LANES // 2, 1)], axis=0)
            values.append(jnp.concatenate([first, rest], axis=1))
        values = jnp.concatenate(values, axis=0)
        position = lax.broadcasted_iota(jnp.int32, values.shape, 1)
        values = jnp.where(position < PAIRS, values, 0.0)
        values = jnp.concatenate([values, jnp.zeros((16, KLANES - 2 * LANES), F32)], axis=1)
        atom = pl.ds(pl.multiple_of(q * 16, 16), 16)
        first_im = (index // part + 1) * (part * 16)
        rows = pl.ds(pl.multiple_of(first_im - part * 16 + index * 16, 16), 16)
        kind = wide(colb[3, atom, :], KLANES)
        placed = jnp.where(kind < 0.5, values, 0.0)
        for n in range(1, SPECIES):
            moved = pltpu.roll(values, n * PAIRS, 1)
            placed = jnp.where((kind > n - 0.5) & (kind < n + 0.5), moved, placed)
        wmix[rows, :] = (placed * even).astype(BF16)
        rows = pl.ds(pl.multiple_of(first_im + index * 16, 16), 16)
        wmix[rows, :] = (placed * odd).astype(BF16)

    def half(h):
        loop(part // crowd * h, part // crowd * (h + 1), weights)
        rows = pl.ds(pl.multiple_of(h * part * 16, part * 16), part * 16)
        both_rows = pl.ds(pl.multiple_of(h * part * 32, part * 32), part * 32)
        for t in range(NPL):
            lanes = slice(t * ct, (t + 1) * ct)
            table = tab[:, lanes]
            amp = dot_nn(wmix[both_rows, :depth], table)
            amp_re, amp_im = amp[: part * 16], amp[part * 16 :]
            c, s = phase[0, rows, lanes], phase[1, rows, lanes]
            augrow[0:1, lanes] += jnp.sum(amp_re * c + amp_im * s, axis=0, keepdims=True)
            augrow[1:2, lanes] += jnp.sum(amp_im * c - amp_re * s, axis=0, keepdims=True)

    loop(0, 2, half)

    pad_z = tz.shape[2] // 2
    wide_row = round_up(columns, LANES)
    shape = (STK, pad_z)
    slot_id = lax.broadcasted_iota(jnp.int32, shape, 0)
    lane_id = lax.broadcasted_iota(jnp.int32, shape, 1)
    values = []
    for n in range(2):
        row = augrow[n : n + 1, :]
        picked = jnp.zeros(shape, F32)
        for t in range(STK):
            moved = pltpu.roll(row, wide_row - t * nz, 1) if t else row
            picked = jnp.where(slot_id == t, moved[:, :pad_z], picked)
        values.append(jnp.where(lane_id < nz, picked, 0.0))
    a_re, a_im = values
    pair = jnp.concatenate(
        [jnp.concatenate([a_re, -a_im], axis=1), jnp.concatenate([a_im, a_re], axis=1)], axis=0
    )
    hi, lo = split(jnp.concatenate([pair, jnp.zeros((LANES - 2 * STK, 2 * pad_z), F32)], axis=0))
    planes = dot_nt(tz[0], hi) + dot_nt(tz[0], lo) + dot_nt(tz[1], hi)
    plane_id = lax.broadcasted_iota(jnp.int32, planes.shape, 0) % 8
    line = jnp.where(plane_id == 0, planes, 0.0)
    for p in range(1, NPL):
        line = line + pltpu.roll(jnp.where(plane_id == p, planes, 0.0), p * 2 * STK, 1)
    send_v[:, 0, :] = jnp.sum(line.reshape(ng, 8, LANES), axis=1)
    recv_v[j] = send_v[j]

    def copy_v(k):
        return copy_ga(send_v.at[(j + k) % ng], recv_v.at[j], v_ssem, v_rsem, k)

    loop(1, ng, lambda k: copy_v(k).start())

    def end_band(k):
        off = band_offset(k)
        copy_band(send_z, recv_z.at[off], z_ssem, z_rsem, off).wait_send()

    def end_ga(k):
        copy_ga(send_a, recv_a.at[j], a_ssem, a_rsem, k).wait_send()
        copy_v(k).wait_send()

    def wait_keys(k):
        off = band_offset(k)
        copy_band(send_k, recv_k.at[b], k_ssem, k_rsem, off).wait_recv()
        copy_band(send_k, recv_k.at[b], k_ssem, k_rsem, off).wait_send()

    loop(0, nb - 1, wait_keys)
    keys = jnp.concatenate([recv_k[n] for n in range(nb)], axis=0)
    slot_x = jnp.floor((keys + 0.5) * (1.0 / nx))
    slot_y = keys - slot_x * nx
    spare = jnp.zeros((LANES - nb * key_rows, LANES), F32)
    slot_y = jnp.concatenate([slot_y, spare], axis=0).T
    row_x = lax.broadcasted_iota(jnp.int32, (16, LANES), 0).astype(F32)
    held = per_row * ng
    for n in range(nb):
        for r in range(key_rows):
            at = n * key_rows + r
            hot = jnp.where(row_x == slot_x[at : at + 1], 1.0, 0.0).astype(BF16)
            onehot[n, :, r * held : (r + 1) * held] = hot[:, :held]
            onehot[n, :, slots + r * held : slots + (r + 1) * held] = hot[:, :held]
            ey[n, 0, r * held : (r + 1) * held, :] = jnp.broadcast_to(
                slot_y[:held, at : at + 1], (held, LANES)
            )
    lane_y = (lax.broadcasted_iota(jnp.int32, (1, LANES), 1) % 16).astype(F32) + (b * NXB).astype(F32)
    some_rows = 64

    def y_phases(r):
        n = r // (slots // some_rows)
        rows = pl.ds(pl.multiple_of(r % (slots // some_rows) * some_rows, some_rows), some_rows)
        c, s = cos_sin(turns_of(ey[n, 0, rows, :] * lane_y, nx))
        ey[n, 0, rows, :] = c
        ey[n, 1, rows, :] = s

    loop(0, nb * (slots // some_rows), y_phases)
    loop(0, nb - 1, end_band)
    loop(1, ng, lambda k: copy_v(k).wait_recv())

    if nb == 16:
        hops = {n: (0, n) for n in (5, -5, 1, -1, 2, -2)}
        hops.update({5 + n: (5, n) for n in (3, 2, -2, 1, -1)})
        hops.update({-5 + n: (-5, n) for n in (2, -2, 1, -1)})
    else:
        hops = {n: (0, n) for n in range(1, nb)}

    def copy_y(off):
        back, hop = hops[off]
        slot = recv_y.at[(b + nb - back) % nb]
        return pltpu.make_async_remote_copy(
            slot,
            slot,
            y_ssem.at[off % nb],
            y_rsem.at[off % nb],
            device_id=((b + nb + hop) % nb, j),
            device_id_type=MESH,
        )

    def pass_on(back):
        for off in hops:
            if hops[off][0] == back:
                copy_y(off).start()

    recv_y[b] = recv_v[:, 0, :]
    pass_on(0)
    loop(1, ng, end_ga)

    group = lax.broadcasted_iota(jnp.int32, (2 * ng, LANES), 1) // 16 * 16

    def take_blocks(sources):
        values = jnp.concatenate([recv_y[source] for source in sources], axis=0)
        pick = group[: len(sources) * ng]
        picked = [jnp.take_along_axis(values, pick + n, axis=1) for n in range(2 * STK)]
        for k, source in enumerate(sources):
            own = [x[k * ng : (k + 1) * ng] for x in picked]
            v_re, v_im = jnp.concatenate(own[:STK], axis=0), jnp.concatenate(own[STK:], axis=0)
            c, s = ey[source, 0], ey[source, 1]
            z = jnp.concatenate([v_re * c - v_im * s, v_re * s + v_im * c], axis=1)
            rows = pl.ds(pl.multiple_of(source * 16, 16), 16)
            field[rows, :] = dot_nn(onehot[source], jnp.concatenate(split(z), axis=0))

    take_blocks([b])
    groups_of = [(5, -5), (1, -1), (2, -2), (3, -3), (4, -4), (6, -6), (7, -7), (8,)]
    for offs in groups_of if nb == 16 else [(n,) for n in range(1, nb)]:
        for off in offs:
            copy_y(off).wait_recv()
            pass_on(off)
        take_blocks([(b + nb - off) % nb for off in offs])

    turned = field[...].T
    f_re, f_im = turned[:LANES], turned[LANES:]
    left = jnp.concatenate(
        [jnp.concatenate([f_re, -f_im], axis=1), jnp.concatenate([f_im, f_re], axis=1)], axis=0
    )
    hi, lo = split(left)
    result = dot_nn(hi, tx[0]) + dot_nn(lo, tx[0]) + dot_nn(hi, tx[1])
    for n in range(2):
        for p in range(NPL):
            first = n * LANES + p * 16
            out_ref[n, p] = result[first : first + NXB, :nx]

    for off in hops:
        copy_y(off).wait_send()


def both_parts(table):
    hi = table.astype(jnp.bfloat16)
    lo = (table - hi.astype(np.float64)).astype(jnp.bfloat16)
    return np.stack([hi, lo])


def tables(nb, ng):
    nx, nz = NXB * nb, NPL * ng
    pad_z = round_up(nz, LANES)
    plane = np.arange(8 * ng) // 8 * NPL + np.arange(8 * ng) % 8
    angle = (plane[:, None] * np.arange(nz)[None, :] % nz) * (2 * np.pi / nz)
    real = (np.arange(8 * ng) % 8 < NPL)[:, None]
    tz = np.zeros((8 * ng, 2 * pad_z))
    tz[:, :nz] = np.where(real, np.cos(angle), 0.0)
    tz[:, pad_z : pad_z + nz] = np.where(real, np.sin(angle), 0.0)
    pad_x = round_up(nx, LANES)
    row = np.arange(16 * nb)
    x = row // 16 * NXB + row % 16
    angle = (x[:, None] * np.arange(nx)[None, :] % nx) * (2 * np.pi / nx)
    real = (row % 16 < NXB)[:, None]
    tx = np.zeros((2 * 16 * nb, pad_x))
    tx[: 16 * nb, :nx] = np.where(real, np.cos(angle), 0.0)
    tx[16 * nb :, :nx] = np.where(real, np.sin(angle), 0.0)
    first, second = np.triu_indices(NH)
    ell = np.array(ELL)
    parity = np.tile((ell[first] + ell[second]) % 2, SPECIES)
    even = np.zeros((2, KLANES), np.float32)
    even[0, : SPECIES * PAIRS] = 1 - parity
    even[1, : SPECIES * PAIRS] = -parity
    return (
        jnp.asarray(both_parts(tz)),
        jnp.asarray(both_parts(tx)),
        jnp.asarray(even),
    )


def on_device(
    waves, occupations, beta_table, wave_miller, atom_kinds, atom_sites, aug_table, stick_columns
):
    nb, ng = lax.axis_size("band"), lax.axis_size("ga")
    nx, nz = NXB * nb, NPL * ng
    atoms, slots = OWN_ATOMS * ng, STK * ng
    wave_count = waves.shape[2]
    gt_lanes = min(256, wave_count)
    tiles = wave_count // gt_lanes
    columns = STK * nz
    steps = ng // 2 // DESTS
    chips = ng // 2
    key_rows = STK // min(LANES // ng, STK)
    tz, tx, even = tables(nb, ng)
    vmem = pl.BlockSpec(memory_space=pltpu.VMEM)
    hbm = pl.BlockSpec(memory_space=pltpu.HBM)
    dma = pltpu.SemaphoreType.DMA
    return pl.pallas_call(
        functools.partial(kernel, nb, ng, gt_lanes),
        out_shape=jax.ShapeDtypeStruct((2, NPL, NXB, nx), F32),
        in_specs=[hbm] * 11,
        out_specs=vmem,
        scratch_shapes=[
            pltpu.VMEM(waves.shape, BF16),
            pltpu.VMEM((1, waves.shape[1]), F32),
            pltpu.VMEM(beta_table.shape, F32),
            pltpu.VMEM(wave_miller.shape, jnp.int32),
            pltpu.VMEM((1, atoms), jnp.int32),
            pltpu.VMEM(atom_sites.shape, jnp.int32),
            pltpu.SMEM(stick_columns.shape, jnp.int32),
            pltpu.VMEM(even.shape, F32),
            pltpu.VMEM(aug_table.shape, BF16),
            pltpu.VMEM(tz.shape, BF16),
            pltpu.VMEM(tx.shape, BF16),
            dma((11,)),
            pltpu.VMEM((4, atoms, LANES), F32),
            pltpu.VMEM((atoms, LANES), jnp.int32),
            pltpu.VMEM((NH, 8, wave_count), F32),
            pltpu.VMEM((8, wave_count), F32),
            pltpu.VMEM((tiles, 4 * gt_lanes, LANES), BF16),
            pltpu.VMEM((DESTS * ROWS, LANES), F32),
            pltpu.VMEM((steps, DESTS * ROWS, LANES), F32),
            pltpu.VMEM((steps, DESTS * ROWS, LANES), F32),
            pltpu.VMEM((chips, ROWS, LANES), F32),
            pltpu.VMEM((chips, ROWS, LANES), F32),
            pltpu.VMEM((6, ROWS, LANES), F32),
            pltpu.VMEM((1, LANES), F32),
            pltpu.VMEM((ng, 1, LANES), F32),
            pltpu.VMEM((8, LANES), F32),
            pltpu.VMEM((2, atoms, round_up(columns, LANES)), F32),
            pltpu.VMEM((FOLD, LANES), F32),
            pltpu.VMEM((nb, FOLD, LANES), F32),
            pltpu.VMEM((FOLD, LANES), F32),
            pltpu.VMEM((ng, FOLD, LANES), F32),
            pltpu.VMEM((2 * atoms, KLANES), BF16),
            pltpu.VMEM((8, round_up(columns, LANES)), F32),
            pltpu.VMEM((ng, 1, LANES), F32),
            pltpu.VMEM((ng, 1, LANES), F32),
            pltpu.VMEM((nb, ng, LANES), F32),
            pltpu.VMEM((nb, 2, slots, LANES), F32),
            pltpu.VMEM((nb, 16, 2 * slots), BF16),
            pltpu.VMEM((key_rows, LANES), F32),
            pltpu.VMEM((nb, key_rows, LANES), F32),
            pltpu.VMEM((nb * 16, 2 * LANES), F32),
            dma((steps,)),
            dma((steps,)),
            dma((chips,)),
            dma((chips,)),
            dma((6,)),
            dma((ng,)),
            dma((ng,)),
            dma((nb,)),
            dma((nb,)),
            dma((ng,)),
            dma((ng,)),
            dma((ng,)),
            dma((ng,)),
            dma((nb,)),
            dma((nb,)),
            dma((nb,)),
            dma((nb,)),
        ],
        compiler_params=pltpu.CompilerParams(
            collective_id=0, has_side_effects=True, vmem_limit_bytes=VMEM_LIMIT
        ),
    )(
        waves,
        occupations[None],
        beta_table,
        wave_miller,
        atom_kinds[None],
        atom_sites,
        aug_table,
        stick_columns,
        tz,
        tx,
        even,
    )


def solution(mesh):
    in_specs = (
        P(None, "band", "ga"),
        P("band"),
        P(None, "ga"),
        P(None, "ga"),
        P(),
        P(),
        P(None, ("band", "ga")),
        P(("band", "ga")),
    )
    out_specs = P(None, "ga", "band", None)
    return jax.shard_map(
        on_device, mesh=mesh, in_specs=in_specs, out_specs=out_specs, check_vma=False
    )
```

```python
import functools
import math

import jax
import jax.numpy as jnp
import numpy as np
from jax import lax
from jax.experimental import pallas as pl
from jax.experimental.pallas import tpu as pltpu
from jax.sharding import PartitionSpec as P

NH = 18
PAIRS = 171
SPECIES = 4
NXB = 15
NPL = 7
STK = 8
OWN_ATOMS = 8
HALF = NH // 2
ROWS = HALF * OWN_ATOMS
DESTS = 4
LANES = 128
KLANES = 768
FOLD = OWN_ATOMS * 3 // 2
VMEM_LIMIT = 67043328
UNROLL = 4

ELL = [0] * 2 + [1] * 6 + [2] * 10
COS = (0.999999989, -19.7392045, 64.9391175, -85.4501395, 60.167631, -25.9675992, 6.52865816)
SIN = (6.28318492, -41.3415892, 81.5999433, -76.6144725, 41.3428824, -12.4712435)

FULL = (
    ((0, 2), (1, 2), (2, 2), (3, 2), (2, 0), (2, 3), (0, 3), (3, 0))
    + ((3, 1), (1, 1), (0, 0), (0, 1), (1, 0), (1, 3), (2, 1), (3, 3)),
    {0: (0, 1), 1: (0, 3), 2: (0, 1), 3: (0, 3), 4: (1, 0), 5: (3, 0)},
    {11: (0,), 12: (4,), 13: (1,), 14: (2,), 15: (3, 5)},
)
SMALL = (((1, 1), (1, 0), (0, 1), (0, 0)), {}, {})

MESH = pl.DeviceIdType.MESH
F32 = jnp.float32
BF16 = jnp.bfloat16


def round_up(value, step):
    return (value + step - 1) // step * step


def cos_sin(turns):
    u = turns - jnp.floor(turns + 0.5)
    w = u * u
    c = COS[-1]
    for a in COS[-2::-1]:
        c = c * w + a
    s = SIN[-1]
    for a in SIN[-2::-1]:
        s = s * w + a
    return c, s * u


def turns_of(product, length):
    inverse = 1.0 / length
    return (product - length * jnp.floor(product * inverse)) * inverse


def split(x):
    hi = x.astype(BF16)
    return hi, (x - hi.astype(F32)).astype(BF16)


def dot_nt(a, b):
    return lax.dot_general(a, b, (((1,), (1,)), ((), ())), preferred_element_type=F32)


def dot_nn(a, b):
    return lax.dot_general(a, b, (((1,), (0,)), ((), ())), preferred_element_type=F32)


def kernel(
    nb,
    ng,
    gt_lanes,
    waves_hbm,
    occ_hbm,
    beta_hbm,
    mil_hbm,
    kinds_hbm,
    sites_hbm,
    tab_hbm,
    sticks_hbm,
    tz_hbm,
    tx_hbm,
    even_hbm,
    out_ref,
    waves_ref,
    occ_ref,
    beta_ref,
    mil_ref,
    kinds_ref,
    sites_ref,
    sticks_ref,
    even_ref,
    tab,
    tz,
    tx,
    local_sem,
    colb,
    kindb,
    species,
    mil,
    wmat,
    acc,
    send_p,
    recv_p,
    send_b,
    recv_b,
    recv_r,
    send_c,
    recv_c,
    occ_row,
    phase,
    send_z,
    recv_z,
    send_a,
    recv_a,
    wmix,
    augrow,
    send_v,
    recv_v,
    recv_y,
    ey,
    onehot,
    send_k,
    recv_k,
    field,
    p_ssem,
    p_rsem,
    b_ssem,
    b_rsem,
    r_rsem,
    c_ssem,
    c_rsem,
    z_ssem,
    z_rsem,
    a_ssem,
    a_rsem,
    v_ssem,
    v_rsem,
    y_ssem,
    y_rsem,
    k_ssem,
    k_rsem,
):
    nx, nz = NXB * nb, NPL * ng
    atoms = OWN_ATOMS * ng
    slots = STK * ng
    band_dev, wave_count = waves_ref.shape[1], waves_ref.shape[2]
    tiles = wave_count // gt_lanes
    steps = ng // 2 // DESTS
    cy = 4 if ng == 32 else 2
    cx = ng // 2 // cy
    columns = STK * nz
    ct = columns // NPL
    b = lax.axis_index("band")
    j = lax.axis_index("ga")
    core = j % 2
    chip = j // 2
    chip_y = chip // cx
    chip_x = chip % cx

    ends = [
        (sites_hbm, sites_ref),
        (kinds_hbm, kinds_ref),
        (mil_hbm, mil_ref),
        (sticks_hbm, sticks_ref),
        (waves_hbm, waves_ref),
        (beta_hbm, beta_ref),
        (occ_hbm, occ_ref),
        (even_hbm, even_ref),
        (tz_hbm, tz),
        (tx_hbm, tx),
        (tab_hbm, tab),
    ]
    local = [pltpu.make_async_copy(*pair, local_sem.at[n]) for n, pair in enumerate(ends)]
    for copy in local:
        copy.start()

    barrier = pltpu.get_barrier_semaphore()

    for k in range(1, nb):
        pl.semaphore_signal(barrier, inc=1, device_id=(lax.rem(b + k, nb), j), device_id_type=MESH)
    for k in range(1, ng):
        pl.semaphore_signal(barrier, inc=1, device_id=(b, lax.rem(j + k, ng)), device_id_type=MESH)

    for copy in local[:7]:
        copy.wait()

    cols = jnp.concatenate(
        [
            sites_ref[...].astype(F32),
            kinds_ref[...].astype(F32),
            jnp.zeros((4, atoms), F32),
        ],
        axis=0,
    ).T
    for n in range(4):
        colb[n] = jnp.broadcast_to(cols[:, n : n + 1], (atoms, LANES))
    kindb[...] = colb[3].astype(jnp.int32)
    kind_row = lax.broadcasted_iota(jnp.int32, (8, wave_count), 0)
    for i in range(NH):
        beta = [beta_ref[n * NH + i : n * NH + i + 1, :] for n in range(SPECIES)]
        species[i] = jnp.where(
            kind_row < 2,
            jnp.where(kind_row < 1, beta[0], beta[1]),
            jnp.where(kind_row < 3, beta[2], beta[3]),
        )
    mil[0:3, :] = mil_ref[...].astype(F32)
    occ_row[...] = jnp.zeros(occ_row.shape, F32)
    occ_row[0:1, 0:band_dev] = occ_ref[...]
    stick = [sticks_ref[t].astype(F32) for t in range(STK)]
    mine = jnp.zeros((1, LANES), F32)
    for t in range(STK):
        mine = jnp.where(lax.broadcasted_iota(jnp.int32, (1, LANES), 1) == t, stick[t], mine)
    send_c[...] = mine
    recv_c[j] = mine

    width = 2 * band_dev
    for g in range(tiles):
        lanes = slice(g * gt_lanes, (g + 1) * gt_lanes)
        wr = waves_ref[0, :, lanes].astype(F32)
        wi = waves_ref[1, :, lanes].astype(F32)
        full = jnp.concatenate([wr, wi, -wi, wr], axis=0).T
        swapped = pltpu.roll(full, width, 1)
        low = lax.broadcasted_iota(jnp.int32, full.shape, 1) < width
        for n, part in enumerate(
            (
                jnp.where(low, full, 0.0),
                jnp.where(low, swapped, 0.0),
                jnp.where(low, 0.0, swapped),
                jnp.where(low, 0.0, full),
            )
        ):
            wmat[g, n * gt_lanes : (n + 1) * gt_lanes, :] = part.astype(BF16)

    def wide(x, lanes):
        return jnp.concatenate([x] * (lanes // LANES), axis=1) if lanes > LANES else x[:, :lanes]

    order, relays, added = FULL if ng == 32 else SMALL
    last = cy * cx - 1

    def chip_at(dy, dx):
        return ((chip_y + dy) % cy) * cx + (chip_x + dx) % cx

    def near_chip(index):
        return chip_at(index // cx, index % cx)

    def ordered_chip(step, d):
        power = 1 + 3 * step + 9 * (step * (step - 1) // 2) + 27 * (step * (step - 1) * (step - 2) // 6)
        code = [sum(order[n * DESTS + d][axis] * 4**n for n in range(steps)) for axis in range(2)]
        return chip_at(*(value // power % 4 for value in code))

    def project(step, parity):
        places = [ordered_chip(step, d) for d in range(DESTS)]

        def rows_of(d):
            dest = 2 * places[d] + parity
            return pl.ds(pl.multiple_of(dest * OWN_ATOMS, OWN_ATOMS), OWN_ATOMS)

        def tile(g):
            whole = [[], [], [], []]
            for piece in range(gt_lanes // LANES):
                lanes = pl.ds(pl.multiple_of(g * gt_lanes + piece * LANES, LANES), LANES)
                m1, m2, m3 = mil[0:1, lanes], mil[1:2, lanes], mil[2:3, lanes]
                pairs, kinds = [], []
                for d in range(DESTS):
                    rows = rows_of(d)
                    p1, p2, p3 = (colb[n, rows, :] for n in range(3))
                    kinds.append(kindb[rows, :])
                    turns = turns_of(p1 * m1 + p2 * m2, nx) + turns_of(p3 * m3, nz)
                    c, s = cos_sin(turns)
                    pairs.append(((c, s), (-s, c), (-c, -s)))
                parts = [[[None] * HALF for d in range(DESTS)] for n in range(4)]
                for i in range(NH):
                    beta = species[i, :, lanes]
                    for d in range(DESTS):
                        radial = jnp.take_along_axis(beta, kinds[d], axis=0)
                        first, second = pairs[d][ELL[i]]
                        h = i // HALF
                        parts[2 * h][d][i % HALF] = radial * first
                        parts[2 * h + 1][d][i % HALF] = radial * second
                for n in range(4):
                    whole[n].append(jnp.concatenate(sum(parts[n], []), axis=0).astype(BF16))
            left = jnp.concatenate(sum(whole, []), axis=1)
            return dot_nn(left, wmat[g])

        together = min(UNROLL, tiles)

        def some(n, carry):
            total = tile(n * together)
            for g in range(1, together):
                total = total + tile(n * together + g)
            acc[...] = total if together == tiles else acc[...] + total
            return carry

        if together == tiles:
            some(0, 0)
        else:
            acc[...] = jnp.zeros(acc.shape, F32)
            lax.fori_loop(0, tiles // together, some, 0)

    def for_partner(step, carry):
        project(step, 1 - core)
        send_p[step] = acc[...]
        return carry

    lax.fori_loop(0, steps, for_partner, 0)
    pl.semaphore_wait(barrier, (nb - 1) + (ng - 1))

    def copy_p(step):
        return pltpu.make_async_remote_copy(
            send_p.at[step],
            recv_p.at[step],
            p_ssem.at[step],
            p_rsem.at[step],
            device_id=(b, chip * 2 + 1 - core),
            device_id_type=MESH,
        )

    def copy_ga(source, target, ssem, rsem, k):
        return pltpu.make_async_remote_copy(
            source,
            target,
            ssem.at[k],
            rsem.at[k],
            device_id=(b, lax.rem(j + k, ng)),
            device_id_type=MESH,
        )

    def band_offset(k):
        half = nb // 2
        m = (k + 1) // 2
        return half + m * (1 - 2 * (k % 2))

    def copy_band(source, target, ssem, rsem, off):
        return pltpu.make_async_remote_copy(
            source,
            target,
            ssem.at[off],
            rsem.at[off],
            device_id=((b + off) % nb, j),
            device_id_type=MESH,
        )

    def loop(low, high, body):
        def step(k, carry):
            body(k)
            return carry

        lax.fori_loop(low, high, step, 0)

    loop(0, steps, lambda s: copy_p(s).start())
    for k in range(1, ng):
        copy_ga(send_c, recv_c.at[j], c_ssem, c_rsem, k).start()

    def copy_b(index):
        target = chip_at(*relays.get(index, order[index]))
        landed, sem = (recv_r, r_rsem) if index in relays else (recv_b, b_rsem)
        return pltpu.make_async_remote_copy(
            send_b.at[index],
            landed.at[index],
            b_ssem.at[index],
            sem.at[index],
            device_id=(b, 2 * target + core),
            device_id_type=MESH,
        )

    sent = [n for n in range(len(order)) if order[n] != (0, 0)]
    direct = [n for n in sent if n not in relays]
    own = order.index((0, 0))

    def for_owners(step, carry):
        project(step, core)
        copy_p(step).wait_recv()

        def deliver(now):
            for d in range(DESTS):
                index = now * DESTS + d
                rows = slice(d * ROWS, (d + 1) * ROWS)
                send_b[index] = acc[rows, :] + recv_p[now, rows, :]
                if index != own and index not in added:
                    copy_b(index).start()

        for now in range(steps):
            pl.when(step == now)(functools.partial(deliver, now))
        return carry

    lax.fori_loop(0, steps, for_owners, 0)
    for index in added:
        block = send_b[index]
        for n in added[index]:
            copy_b(n).wait_recv()
            block = block + recv_r[n]
        send_b[index] = block
        copy_b(index).start()

    loop(1, ng, lambda k: copy_ga(send_c, recv_c.at[j], c_ssem, c_rsem, k).wait_recv())
    owners = jnp.concatenate([recv_c[:, 0, :], jnp.zeros((LANES - ng, LANES), F32)], axis=0).T
    per_row = min(LANES // ng, STK)
    key_rows = STK // per_row
    keys = []
    for r in range(key_rows):
        row = owners[r * per_row : r * per_row + 1]
        for n in range(1, per_row):
            at = r * per_row + n
            row = row + pltpu.roll(owners[at : at + 1], n * ng, 1)
        keys.append(row)
    send_k[...] = jnp.concatenate(keys, axis=0)
    recv_k[b] = send_k[...]

    def send_keys(k):
        off = band_offset(k)
        copy_band(send_k, recv_k.at[b], k_ssem, k_rsem, off).start()

    loop(0, nb - 1, send_keys)
    loop(0, steps, lambda s: copy_p(s).wait_send())
    loop(1, ng, lambda k: copy_ga(send_c, recv_c.at[j], c_ssem, c_rsem, k).wait_send())
    for index in direct:
        copy_b(index).wait_recv()
    becp = send_b[own]
    for index in direct:
        becp = becp + recv_b[index]
    occ = occ_row[...]
    occ = sum((pltpu.roll(occ, n * band_dev, 1) for n in range(1, LANES // band_dev)), occ)[0:1]
    lane = lax.broadcasted_iota(jnp.int32, (1, LANES), 1)
    occ = jnp.where(lane < width, occ, 0.0)
    both = jnp.concatenate([becp, pltpu.roll(becp, LANES - width, 1)], axis=0)
    hi, lo = split(both)
    occ_hi, occ_lo = split(both * occ)
    gram = dot_nt(
        jnp.concatenate([occ_hi, occ_hi, occ_lo], axis=1), jnp.concatenate([hi, lo, hi], axis=1)
    )
    rows = NH * OWN_ATOMS
    row_id = lax.broadcasted_iota(jnp.int32, (rows, rows), 0)
    col_id = lax.broadcasted_iota(jnp.int32, (rows, rows), 1)
    gram = jnp.where(row_id % OWN_ATOMS == col_id % OWN_ATOMS, gram, 0.0)
    pick = (
        lax.broadcasted_iota(jnp.int32, (rows, LANES), 0) // OWN_ATOMS
        == lax.broadcasted_iota(jnp.int32, (rows, LANES), 1)
    ).astype(BF16)
    square = dot_nn(jnp.concatenate(split(gram), axis=1), jnp.concatenate([pick, pick], axis=0))
    total = jnp.zeros((OWN_ATOMS, 2 * LANES), F32)
    for i in range(NH):
        factor = jnp.where(lane < i, 0.0, jnp.where(lane == i, 1.0, 2.0))
        factor = jnp.where(lane < NH, factor, 0.0)
        piece = square[i * OWN_ATOMS : (i + 1) * OWN_ATOMS] * factor
        piece = jnp.concatenate([piece, jnp.zeros((OWN_ATOMS, LANES), F32)], axis=1)
        shift = i * NH - i * (i - 1) // 2 - i
        total = total + (pltpu.roll(piece, shift, 1) if shift else piece)
    folded = total[:4, LANES:] + pltpu.roll(total[4:, LANES:], LANES // 2, 1)
    total = jnp.concatenate([total[:, :LANES], folded], axis=0)
    send_z[...] = total
    recv_z[0] = total

    def send_band(k):
        off = band_offset(k)
        copy_band(send_z, recv_z.at[off], z_ssem, z_rsem, off).start()

    loop(0, nb - 1, send_band)

    column = jnp.zeros((1, LANES), F32)
    for n in range(STK):
        column = jnp.where(lane == n, stick[n], column)
    stick_x = jnp.floor((column + 0.5) * (1.0 / nx))
    stick_y = column - stick_x * nx
    stick_x = stick_x + (b * NXB).astype(F32)
    lane_tiles = phase.shape[2] // LANES
    period = min(nz // math.gcd(nz, LANES), lane_tiles)
    heights = []
    for q in range(period):
        g = (lane + q * LANES).astype(F32)
        heights.append(g - nz * jnp.floor((g + 0.5) * (1.0 / nz)))

    def phases(r):
        source = 2 * near_chip(r // 2) + r % 2
        atom = pl.ds(pl.multiple_of(source * 8, 8), 8)
        p1, p2, p3 = (colb[n, atom, :] for n in range(3))
        rows = pl.ds(pl.multiple_of(r * 8, 8), 8)
        flat = cos_sin(turns_of(p1 * stick_x + p2 * stick_y, nx))
        flat = [[jnp.broadcast_to(x[:, n : n + 1], (8, LANES)) for n in range(STK)] for x in flat]
        tall = [cos_sin(turns_of(p3 * z, nz)) for z in heights]
        for t in range(lane_tiles):
            low = t * LANES // nz
            high = min(((t + 1) * LANES - 1) // nz, STK - 1)
            c, s = (x[low] for x in flat)
            for n in range(low + 1, high + 1):
                before = lane < n * nz - t * LANES
                c, s = jnp.where(before, c, flat[0][n]), jnp.where(before, s, flat[1][n])
            cz, sz = tall[t % period]
            lanes = slice(t * LANES, (t + 1) * LANES)
            phase[0, rows, lanes] = c * cz - s * sz
            phase[1, rows, lanes] = s * cz + c * sz

    loop(0, atoms // 8, phases)
    for index in sent:
        copy_b(index).wait_send()
    def wait_band(k):
        off = band_offset(k)
        copy_band(send_z, recv_z.at[off], z_ssem, z_rsem, off).wait_recv()

    loop(0, nb - 1, wait_band)
    total = recv_z[0]
    for n in range(1, nb):
        total = total + recv_z[n]
    send_a[...] = total
    recv_a[j] = total
    for k in range(1, ng):
        copy_ga(send_a, recv_a.at[j], a_ssem, a_rsem, k).start()
    for copy in local[7:]:
        copy.wait()

    even = even_ref[0:1, :]
    odd = even_ref[1:2, :]
    depth = SPECIES * PAIRS
    part = last + 1
    augrow[...] = jnp.zeros(augrow.shape, F32)

    def arrive(k):
        copy_ga(send_a, recv_a.at[j], a_ssem, a_rsem, k).wait_recv()

    crowd = min(4, part)

    def weights(n):
        for index in range(crowd):
            index = index + n * crowd
            q = near_chip(index)

            @pl.when(index == 0)
            def _():
                arrive((j - (chip * 2 + 1 - core)) % ng)

            @pl.when(index > 0)
            def _():
                arrive((j - 2 * q) % ng)
                arrive((j - 2 * q - 1) % ng)

        for index in range(crowd):
            weigh(index + n * crowd)

    def weigh(index):
        q = near_chip(index)
        values = []
        for n in range(2):
            got = recv_a[2 * q + n]
            first, rest = got[:OWN_ATOMS], got[OWN_ATOMS:]
            rest = jnp.concatenate([rest, pltpu.roll(rest, LANES // 2, 1)], axis=0)
            values.append(jnp.concatenate([first, rest], axis=1))
        values = jnp.concatenate(values, axis=0)
        position = lax.broadcasted_iota(jnp.int32, values.shape, 1)
        values = jnp.where(position < PAIRS, values, 0.0)
        values = jnp.concatenate([values, jnp.zeros((16, KLANES - 2 * LANES), F32)], axis=1)
        atom = pl.ds(pl.multiple_of(q * 16, 16), 16)
        first_im = (index // part + 1) * (part * 16)
        rows = pl.ds(pl.multiple_of(first_im - part * 16 + index * 16, 16), 16)
        kind = wide(colb[3, atom, :], KLANES)
        placed = jnp.where(kind < 0.5, values, 0.0)
        for n in range(1, SPECIES):
            moved = pltpu.roll(values, n * PAIRS, 1)
            placed = jnp.where((kind > n - 0.5) & (kind < n + 0.5), moved, placed)
        wmix[rows, :] = (placed * even).astype(BF16)
        rows = pl.ds(pl.multiple_of(first_im + index * 16, 16), 16)
        wmix[rows, :] = (placed * odd).astype(BF16)

    def half(h):
        loop(part // crowd * h, part // crowd * (h + 1), weights)
        rows = pl.ds(pl.multiple_of(h * part * 16, part * 16), part * 16)
        both_rows = pl.ds(pl.multiple_of(h * part * 32, part * 32), part * 32)
        for t in range(NPL):
            lanes = slice(t * ct, (t + 1) * ct)
            table = tab[:, lanes]
            amp = dot_nn(wmix[both_rows, :depth], table)
            amp_re, amp_im = amp[: part * 16], amp[part * 16 :]
            c, s = phase[0, rows, lanes], phase[1, rows, lanes]
            augrow[0:1, lanes] += jnp.sum(amp_re * c + amp_im * s, axis=0, keepdims=True)
            augrow[1:2, lanes] += jnp.sum(amp_im * c - amp_re * s, axis=0, keepdims=True)

    loop(0, (last + 1) // part, half)

    pad_z = tz.shape[2] // 2
    wide_row = round_up(columns, LANES)
    shape = (STK, pad_z)
    slot_id = lax.broadcasted_iota(jnp.int32, shape, 0)
    lane_id = lax.broadcasted_iota(jnp.int32, shape, 1)
    values = []
    for n in range(2):
        row = augrow[n : n + 1, :]
        picked = jnp.zeros(shape, F32)
        for t in range(STK):
            moved = pltpu.roll(row, wide_row - t * nz, 1) if t else row
            picked = jnp.where(slot_id == t, moved[:, :pad_z], picked)
        values.append(jnp.where(lane_id < nz, picked, 0.0))
    a_re, a_im = values
    pair = jnp.concatenate(
        [jnp.concatenate([a_re, -a_im], axis=1), jnp.concatenate([a_im, a_re], axis=1)], axis=0
    )
    hi, lo = split(jnp.concatenate([pair, jnp.zeros((LANES - 2 * STK, 2 * pad_z), F32)], axis=0))
    planes = dot_nt(tz[0], hi) + dot_nt(tz[0], lo) + dot_nt(tz[1], hi)
    plane_id = lax.broadcasted_iota(jnp.int32, planes.shape, 0) % 8
    line = jnp.where(plane_id == 0, planes, 0.0)
    for p in range(1, NPL):
        line = line + pltpu.roll(jnp.where(plane_id == p, planes, 0.0), p * 2 * STK, 1)
    send_v[:, 0, :] = jnp.sum(line.reshape(ng, 8, LANES), axis=1)
    recv_v[j] = send_v[j]

    def copy_v(k):
        return copy_ga(send_v.at[lax.rem(j + k, ng)], recv_v.at[j], v_ssem, v_rsem, k)

    for k in range(1, ng):
        copy_v(k).start()

    def end_band(k):
        off = band_offset(k)
        copy_band(send_z, recv_z.at[off], z_ssem, z_rsem, off).wait_send()

    def end_ga(k):
        copy_ga(send_a, recv_a.at[j], a_ssem, a_rsem, k).wait_send()
        copy_v(k).wait_send()

    def wait_keys(k):
        off = band_offset(k)
        copy_band(send_k, recv_k.at[b], k_ssem, k_rsem, off).wait_recv()
        copy_band(send_k, recv_k.at[b], k_ssem, k_rsem, off).wait_send()

    loop(0, nb - 1, wait_keys)
    keys = jnp.concatenate([recv_k[n] for n in range(nb)], axis=0)
    slot_x = jnp.floor((keys + 0.5) * (1.0 / nx))
    slot_y = keys - slot_x * nx
    spare = jnp.zeros((LANES - nb * key_rows, LANES), F32)
    slot_y = jnp.concatenate([slot_y, spare], axis=0).T
    row_x = lax.broadcasted_iota(jnp.int32, (16, LANES), 0).astype(F32)
    held = per_row * ng
    for n in range(nb):
        for r in range(key_rows):
            at = n * key_rows + r
            hot = jnp.where(row_x == slot_x[at : at + 1], 1.0, 0.0).astype(BF16)
            onehot[n, :, r * held : (r + 1) * held] = hot[:, :held]
            onehot[n, :, slots + r * held : slots + (r + 1) * held] = hot[:, :held]
            ey[n, 0, r * held : (r + 1) * held, :] = jnp.broadcast_to(
                slot_y[:held, at : at + 1], (held, LANES)
            )
    lane_y = (lax.broadcasted_iota(jnp.int32, (1, LANES), 1) % 16).astype(F32) + (b * NXB).astype(F32)
    some_rows = 64

    def y_phases(r):
        n = r // (slots // some_rows)
        rows = pl.ds(pl.multiple_of(r % (slots // some_rows) * some_rows, some_rows), some_rows)
        c, s = cos_sin(turns_of(ey[n, 0, rows, :] * lane_y, nx))
        ey[n, 0, rows, :] = c
        ey[n, 1, rows, :] = s

    loop(0, nb * (slots // some_rows), y_phases)
    loop(0, nb - 1, end_band)
    loop(1, ng, lambda k: copy_v(k).wait_recv())

    if nb == 16:
        hops = {n: (0, n) for n in (5, -5, 1, -1, 2, -2)}
        hops.update({5 + n: (5, n) for n in (3, 2, -2, 1, -1)})
        hops.update({-5 + n: (-5, n) for n in (2, -2, 1, -1)})
    else:
        hops = {n: (0, n) for n in range(1, nb)}

    def copy_y(off):
        back, hop = hops[off]
        slot = recv_y.at[(b + nb - back) % nb]
        return pltpu.make_async_remote_copy(
            slot,
            slot,
            y_ssem.at[off % nb],
            y_rsem.at[off % nb],
            device_id=((b + nb + hop) % nb, j),
            device_id_type=MESH,
        )

    def pass_on(back):
        for off in hops:
            if hops[off][0] == back:
                copy_y(off).start()

    recv_y[b] = recv_v[:, 0, :]
    pass_on(0)
    loop(1, ng, end_ga)

    group = lax.broadcasted_iota(jnp.int32, (2 * ng, LANES), 1) // 16 * 16

    def take_blocks(sources):
        values = jnp.concatenate([recv_y[source] for source in sources], axis=0)
        pick = group[: len(sources) * ng]
        picked = [jnp.take_along_axis(values, pick + n, axis=1) for n in range(2 * STK)]
        for k, source in enumerate(sources):
            own = [x[k * ng : (k + 1) * ng] for x in picked]
            v_re, v_im = jnp.concatenate(own[:STK], axis=0), jnp.concatenate(own[STK:], axis=0)
            c, s = ey[source, 0], ey[source, 1]
            z = jnp.concatenate([v_re * c - v_im * s, v_re * s + v_im * c], axis=1)
            rows = pl.ds(pl.multiple_of(source * 16, 16), 16)
            field[rows, :] = dot_nn(onehot[source], jnp.concatenate(split(z), axis=0))

    take_blocks([b])
    groups_of = [(5, -5), (1, -1, 2, -2), (3, -3, 4, -4, 6, -6, 7, -7, 8)]
    for offs in groups_of if nb == 16 else [(n,) for n in range(1, nb)]:
        for off in offs:
            copy_y(off).wait_recv()
            pass_on(off)
        for n in range(0, len(offs), 2):
            take_blocks([(b + nb - off) % nb for off in offs[n : n + 2]])

    turned = field[...].T
    f_re, f_im = turned[:LANES], turned[LANES:]
    left = jnp.concatenate(
        [jnp.concatenate([f_re, -f_im], axis=1), jnp.concatenate([f_im, f_re], axis=1)], axis=0
    )
    hi, lo = split(left)
    result = dot_nn(jnp.concatenate([hi, lo], axis=0), tx[0])
    result = result[: 2 * LANES] + result[2 * LANES :] + dot_nn(hi, tx[1])
    for n in range(2):
        for p in range(NPL):
            first = n * LANES + p * 16
            out_ref[n, p] = result[first : first + NXB, :nx]

    for off in hops:
        copy_y(off).wait_send()


def both_parts(table):
    hi = table.astype(jnp.bfloat16)
    lo = (table - hi.astype(np.float64)).astype(jnp.bfloat16)
    return np.stack([hi, lo])


def tables(nb, ng):
    nx, nz = NXB * nb, NPL * ng
    pad_z = round_up(nz, LANES)
    plane = np.arange(8 * ng) // 8 * NPL + np.arange(8 * ng) % 8
    angle = (plane[:, None] * np.arange(nz)[None, :] % nz) * (2 * np.pi / nz)
    real = (np.arange(8 * ng) % 8 < NPL)[:, None]
    tz = np.zeros((8 * ng, 2 * pad_z))
    tz[:, :nz] = np.where(real, np.cos(angle), 0.0)
    tz[:, pad_z : pad_z + nz] = np.where(real, np.sin(angle), 0.0)
    pad_x = round_up(nx, LANES)
    row = np.arange(16 * nb)
    x = row // 16 * NXB + row % 16
    angle = (x[:, None] * np.arange(nx)[None, :] % nx) * (2 * np.pi / nx)
    real = (row % 16 < NXB)[:, None]
    tx = np.zeros((2 * 16 * nb, pad_x))
    tx[: 16 * nb, :nx] = np.where(real, np.cos(angle), 0.0)
    tx[16 * nb :, :nx] = np.where(real, np.sin(angle), 0.0)
    first, second = np.triu_indices(NH)
    ell = np.array(ELL)
    parity = np.tile((ell[first] + ell[second]) % 2, SPECIES)
    even = np.zeros((2, KLANES), np.float32)
    even[0, : SPECIES * PAIRS] = 1 - parity
    even[1, : SPECIES * PAIRS] = -parity
    return (
        jnp.asarray(both_parts(tz)),
        jnp.asarray(both_parts(tx)),
        jnp.asarray(even),
    )


def on_device(
    waves, occupations, beta_table, wave_miller, atom_kinds, atom_sites, aug_table, stick_columns
):
    nb, ng = lax.axis_size("band"), lax.axis_size("ga")
    nx, nz = NXB * nb, NPL * ng
    atoms, slots = OWN_ATOMS * ng, STK * ng
    wave_count = waves.shape[2]
    gt_lanes = min(256, wave_count)
    tiles = wave_count // gt_lanes
    columns = STK * nz
    steps = ng // 2 // DESTS
    chips = ng // 2
    key_rows = STK // min(LANES // ng, STK)
    tz, tx, even = tables(nb, ng)
    vmem = pl.BlockSpec(memory_space=pltpu.VMEM)
    hbm = pl.BlockSpec(memory_space=pltpu.HBM)
    dma = pltpu.SemaphoreType.DMA
    return pl.pallas_call(
        functools.partial(kernel, nb, ng, gt_lanes),
        out_shape=jax.ShapeDtypeStruct((2, NPL, NXB, nx), F32),
        in_specs=[hbm] * 11,
        out_specs=vmem,
        scratch_shapes=[
            pltpu.VMEM(waves.shape, BF16),
            pltpu.VMEM((1, waves.shape[1]), F32),
            pltpu.VMEM(beta_table.shape, F32),
            pltpu.VMEM(wave_miller.shape, jnp.int32),
            pltpu.VMEM((1, atoms), jnp.int32),
            pltpu.VMEM(atom_sites.shape, jnp.int32),
            pltpu.SMEM(stick_columns.shape, jnp.int32),
            pltpu.VMEM(even.shape, F32),
            pltpu.VMEM(aug_table.shape, BF16),
            pltpu.VMEM(tz.shape, BF16),
            pltpu.VMEM(tx.shape, BF16),
            dma((11,)),
            pltpu.VMEM((4, atoms, LANES), F32),
            pltpu.VMEM((atoms, LANES), jnp.int32),
            pltpu.VMEM((NH, 8, wave_count), F32),
            pltpu.VMEM((8, wave_count), F32),
            pltpu.VMEM((tiles, 4 * gt_lanes, LANES), BF16),
            pltpu.VMEM((DESTS * ROWS, LANES), F32),
            pltpu.VMEM((steps, DESTS * ROWS, LANES), F32),
            pltpu.VMEM((steps, DESTS * ROWS, LANES), F32),
            pltpu.VMEM((chips, ROWS, LANES), F32),
            pltpu.VMEM((chips, ROWS, LANES), F32),
            pltpu.VMEM((6, ROWS, LANES), F32),
            pltpu.VMEM((1, LANES), F32),
            pltpu.VMEM((ng, 1, LANES), F32),
            pltpu.VMEM((8, LANES), F32),
            pltpu.VMEM((2, atoms, round_up(columns, LANES)), F32),
            pltpu.VMEM((FOLD, LANES), F32),
            pltpu.VMEM((nb, FOLD, LANES), F32),
            pltpu.VMEM((FOLD, LANES), F32),
            pltpu.VMEM((ng, FOLD, LANES), F32),
            pltpu.VMEM((2 * atoms, KLANES), BF16),
            pltpu.VMEM((8, round_up(columns, LANES)), F32),
            pltpu.VMEM((ng, 1, LANES), F32),
            pltpu.VMEM((ng, 1, LANES), F32),
            pltpu.VMEM((nb, ng, LANES), F32),
            pltpu.VMEM((nb, 2, slots, LANES), F32),
            pltpu.VMEM((nb, 16, 2 * slots), BF16),
            pltpu.VMEM((key_rows, LANES), F32),
            pltpu.VMEM((nb, key_rows, LANES), F32),
            pltpu.VMEM((nb * 16, 2 * LANES), F32),
            dma((steps,)),
            dma((steps,)),
            dma((chips,)),
            dma((chips,)),
            dma((6,)),
            dma((ng,)),
            dma((ng,)),
            dma((nb,)),
            dma((nb,)),
            dma((ng,)),
            dma((ng,)),
            dma((ng,)),
            dma((ng,)),
            dma((nb,)),
            dma((nb,)),
            dma((nb,)),
            dma((nb,)),
        ],
        compiler_params=pltpu.CompilerParams(
            collective_id=0, has_side_effects=True, vmem_limit_bytes=VMEM_LIMIT
        ),
    )(
        waves,
        occupations[None],
        beta_table,
        wave_miller,
        atom_kinds[None],
        atom_sites,
        aug_table,
        stick_columns,
        tz,
        tx,
        even,
    )


def solution(mesh):
    in_specs = (
        P(None, "band", "ga"),
        P("band"),
        P(None, "ga"),
        P(None, "ga"),
        P(),
        P(),
        P(None, ("band", "ga")),
        P(("band", "ga")),
    )
    out_specs = P(None, "ga", "band", None)
    return jax.shard_map(
        on_device, mesh=mesh, in_specs=in_specs, out_specs=out_specs, check_vma=False
    )
```

```python
import functools
import math

import jax
import jax.numpy as jnp
import numpy as np
from jax import lax
from jax.experimental import pallas as pl
from jax.experimental.pallas import tpu as pltpu
from jax.sharding import PartitionSpec as P

NH = 18
PAIRS = 171
SPECIES = 4
NXB = 15
NPL = 7
STK = 8
OWN_ATOMS = 8
HALF = NH // 2
ROWS = HALF * OWN_ATOMS
DESTS = 4
LANES = 128
KLANES = 768
FOLD = OWN_ATOMS * 3 // 2
VMEM_LIMIT = 67043328
UNROLL = 4

ELL = [0] * 2 + [1] * 6 + [2] * 10
COS = (0.999999989, -19.7392045, 64.9391175, -85.4501395, 60.167631, -25.9675992, 6.52865816)
SIN = (6.28318492, -41.3415892, 81.5999433, -76.6144725, 41.3428824, -12.4712435)

FULL = (
    ((0, 2), (1, 2), (2, 2), (3, 2), (2, 0), (2, 3), (0, 3), (3, 0))
    + ((3, 1), (1, 1), (0, 0), (0, 1), (1, 0), (1, 3), (2, 1), (3, 3)),
    {0: (0, 1), 1: (0, 3), 2: (0, 1), 3: (0, 3), 4: (1, 0), 5: (3, 0)},
    {11: (0,), 12: (4,), 13: (1,), 14: (2,), 15: (3, 5)},
)
SMALL = (((1, 1), (1, 0), (0, 1), (0, 0)), {}, {})

MESH = pl.DeviceIdType.MESH
F32 = jnp.float32
BF16 = jnp.bfloat16


def round_up(value, step):
    return (value + step - 1) // step * step


def cos_sin(turns):
    u = turns - jnp.floor(turns + 0.5)
    w = u * u
    c = COS[-1]
    for a in COS[-2::-1]:
        c = c * w + a
    s = SIN[-1]
    for a in SIN[-2::-1]:
        s = s * w + a
    return c, s * u


def turns_of(product, length):
    inverse = 1.0 / length
    return (product - length * jnp.floor(product * inverse)) * inverse


def split(x):
    hi = x.astype(BF16)
    return hi, (x - hi.astype(F32)).astype(BF16)


def dot_nt(a, b):
    return lax.dot_general(a, b, (((1,), (1,)), ((), ())), preferred_element_type=F32)


def dot_nn(a, b):
    return lax.dot_general(a, b, (((1,), (0,)), ((), ())), preferred_element_type=F32)


def kernel(
    nb,
    ng,
    gt_lanes,
    waves_hbm,
    occ_hbm,
    beta_hbm,
    mil_hbm,
    kinds_hbm,
    sites_hbm,
    tab_hbm,
    sticks_hbm,
    tz_hbm,
    tx_hbm,
    even_hbm,
    out_ref,
    waves_ref,
    occ_ref,
    beta_ref,
    mil_ref,
    kinds_ref,
    sites_ref,
    sticks_ref,
    even_ref,
    tab,
    tz,
    tx,
    local_sem,
    colb,
    kindb,
    species,
    mil,
    wmat,
    acc,
    send_p,
    recv_p,
    send_b,
    recv_b,
    recv_r,
    send_c,
    recv_c,
    occ_row,
    phase,
    send_z,
    recv_z,
    send_a,
    recv_a,
    wmix,
    augrow,
    send_v,
    recv_v,
    recv_y,
    ey,
    onehot,
    send_k,
    recv_k,
    field,
    p_ssem,
    p_rsem,
    b_ssem,
    b_rsem,
    r_rsem,
    c_ssem,
    c_rsem,
    z_ssem,
    z_rsem,
    a_ssem,
    a_rsem,
    v_ssem,
    v_rsem,
    y_ssem,
    y_rsem,
    k_ssem,
    k_rsem,
):
    nx, nz = NXB * nb, NPL * ng
    atoms = OWN_ATOMS * ng
    slots = STK * ng
    band_dev, wave_count = waves_ref.shape[1], waves_ref.shape[2]
    tiles = wave_count // gt_lanes
    steps = ng // 2 // DESTS
    cy = 4 if ng == 32 else 2
    cx = ng // 2 // cy
    columns = STK * nz
    ct = columns // NPL
    b = lax.axis_index("band")
    j = lax.axis_index("ga")
    core = j % 2
    chip = j // 2
    chip_y = chip // cx
    chip_x = chip % cx

    ends = [
        (sites_hbm, sites_ref),
        (kinds_hbm, kinds_ref),
        (mil_hbm, mil_ref),
        (sticks_hbm, sticks_ref),
        (waves_hbm, waves_ref),
        (beta_hbm, beta_ref),
        (occ_hbm, occ_ref),
        (even_hbm, even_ref),
        (tz_hbm, tz),
        (tx_hbm, tx),
        (tab_hbm, tab),
    ]
    local = [pltpu.make_async_copy(*pair, local_sem.at[n]) for n, pair in enumerate(ends)]
    for copy in local:
        copy.start()

    barrier = pltpu.get_barrier_semaphore()

    for k in range(1, nb):
        pl.semaphore_signal(barrier, inc=1, device_id=(lax.rem(b + k, nb), j), device_id_type=MESH)
    for k in range(1, ng):
        pl.semaphore_signal(barrier, inc=1, device_id=(b, lax.rem(j + k, ng)), device_id_type=MESH)

    for copy in local[:7]:
        copy.wait()

    cols = jnp.concatenate(
        [
            sites_ref[...].astype(F32),
            kinds_ref[...].astype(F32),
            jnp.zeros((4, atoms), F32),
        ],
        axis=0,
    ).T
    for n in range(4):
        colb[n] = jnp.broadcast_to(cols[:, n : n + 1], (atoms, LANES))
    kindb[...] = colb[3].astype(jnp.int32)
    kind_row = lax.broadcasted_iota(jnp.int32, (8, wave_count), 0)
    for i in range(NH):
        beta = [beta_ref[n * NH + i : n * NH + i + 1, :] for n in range(SPECIES)]
        species[i] = jnp.where(
            kind_row < 2,
            jnp.where(kind_row < 1, beta[0], beta[1]),
            jnp.where(kind_row < 3, beta[2], beta[3]),
        )
    mil[0:3, :] = mil_ref[...].astype(F32)
    occ_row[...] = jnp.zeros(occ_row.shape, F32)
    occ_row[0:1, 0:band_dev] = occ_ref[...]
    stick = [sticks_ref[t].astype(F32) for t in range(STK)]
    mine = jnp.zeros((1, LANES), F32)
    for t in range(STK):
        mine = jnp.where(lax.broadcasted_iota(jnp.int32, (1, LANES), 1) == t, stick[t], mine)
    send_c[...] = mine
    recv_c[j] = mine

    width = 2 * band_dev
    for g in range(tiles):
        lanes = slice(g * gt_lanes, (g + 1) * gt_lanes)
        wr = waves_ref[0, :, lanes].astype(F32)
        wi = waves_ref[1, :, lanes].astype(F32)
        full = jnp.concatenate([wr, wi, -wi, wr], axis=0).T
        swapped = pltpu.roll(full, width, 1)
        low = lax.broadcasted_iota(jnp.int32, full.shape, 1) < width
        for n, part in enumerate(
            (
                jnp.where(low, full, 0.0),
                jnp.where(low, swapped, 0.0),
                jnp.where(low, 0.0, swapped),
                jnp.where(low, 0.0, full),
            )
        ):
            wmat[g, n * gt_lanes : (n + 1) * gt_lanes, :] = part.astype(BF16)

    def wide(x, lanes):
        return jnp.concatenate([x] * (lanes // LANES), axis=1) if lanes > LANES else x[:, :lanes]

    order, relays, added = FULL if ng == 32 else SMALL
    last = cy * cx - 1

    def chip_at(dy, dx):
        return ((chip_y + dy) % cy) * cx + (chip_x + dx) % cx

    def near_chip(index):
        return chip_at(index // cx, index % cx)

    def ordered_chip(step, d):
        power = 1 + 3 * step + 9 * (step * (step - 1) // 2) + 27 * (step * (step - 1) * (step - 2) // 6)
        code = [sum(order[n * DESTS + d][axis] * 4**n for n in range(steps)) for axis in range(2)]
        return chip_at(*(value // power % 4 for value in code))

    def project(step, parity):
        places = [ordered_chip(step, d) for d in range(DESTS)]

        def rows_of(d):
            dest = 2 * places[d] + parity
            return pl.ds(pl.multiple_of(dest * OWN_ATOMS, OWN_ATOMS), OWN_ATOMS)

        def tile(g):
            whole = [[], [], [], []]
            for piece in range(gt_lanes // LANES):
                lanes = pl.ds(pl.multiple_of(g * gt_lanes + piece * LANES, LANES), LANES)
                m1, m2, m3 = mil[0:1, lanes], mil[1:2, lanes], mil[2:3, lanes]
                pairs, kinds = [], []
                for d in range(DESTS):
                    rows = rows_of(d)
                    p1, p2, p3 = (colb[n, rows, :] for n in range(3))
                    kinds.append(kindb[rows, :])
                    turns = turns_of(p1 * m1 + p2 * m2, nx) + turns_of(p3 * m3, nz)
                    c, s = cos_sin(turns)
                    pairs.append(((c, s), (-s, c), (-c, -s)))
                parts = [[[None] * HALF for d in range(DESTS)] for n in range(4)]
                for i in range(NH):
                    beta = species[i, :, lanes]
                    for d in range(DESTS):
                        radial = jnp.take_along_axis(beta, kinds[d], axis=0)
                        first, second = pairs[d][ELL[i]]
                        h = i // HALF
                        parts[2 * h][d][i % HALF] = radial * first
                        parts[2 * h + 1][d][i % HALF] = radial * second
                for n in range(4):
                    whole[n].append(jnp.concatenate(sum(parts[n], []), axis=0).astype(BF16))
            left = jnp.concatenate(sum(whole, []), axis=1)
            return dot_nn(left, wmat[g])

        together = min(UNROLL, tiles)

        def some(n, carry):
            total = tile(n * together)
            for g in range(1, together):
                total = total + tile(n * together + g)
            acc[...] = total if together == tiles else acc[...] + total
            return carry

        if together == tiles:
            some(0, 0)
        else:
            acc[...] = jnp.zeros(acc.shape, F32)
            lax.fori_loop(0, tiles // together, some, 0)

    def for_partner(step, carry):
        project(step, 1 - core)
        send_p[step] = acc[...]
        return carry

    lax.fori_loop(0, steps, for_partner, 0)
    pl.semaphore_wait(barrier, (nb - 1) + (ng - 1))

    def copy_p(step):
        return pltpu.make_async_remote_copy(
            send_p.at[step],
            recv_p.at[step],
            p_ssem.at[step],
            p_rsem.at[step],
            device_id=(b, chip * 2 + 1 - core),
            device_id_type=MESH,
        )

    def copy_ga(source, target, ssem, rsem, k):
        return pltpu.make_async_remote_copy(
            source,
            target,
            ssem.at[k],
            rsem.at[k],
            device_id=(b, lax.rem(j + k, ng)),
            device_id_type=MESH,
        )

    def band_offset(k):
        half = nb // 2
        m = (k + 1) // 2
        return half + m * (1 - 2 * (k % 2))

    def copy_band(source, target, ssem, rsem, off):
        return pltpu.make_async_remote_copy(
            source,
            target,
            ssem.at[off],
            rsem.at[off],
            device_id=((b + off) % nb, j),
            device_id_type=MESH,
        )

    def loop(low, high, body):
        def step(k, carry):
            body(k)
            return carry

        lax.fori_loop(low, high, step, 0)

    loop(0, steps, lambda s: copy_p(s).start())
    for k in range(1, ng):
        copy_ga(send_c, recv_c.at[j], c_ssem, c_rsem, k).start()

    def copy_b(index):
        target = chip_at(*relays.get(index, order[index]))
        landed, sem = (recv_r, r_rsem) if index in relays else (recv_b, b_rsem)
        return pltpu.make_async_remote_copy(
            send_b.at[index],
            landed.at[index],
            b_ssem.at[index],
            sem.at[index],
            device_id=(b, 2 * target + core),
            device_id_type=MESH,
        )

    sent = [n for n in range(len(order)) if order[n] != (0, 0)]
    direct = [n for n in sent if n not in relays]
    own = order.index((0, 0))

    def for_owners(step, carry):
        project(step, core)
        copy_p(step).wait_recv()

        def deliver(now):
            for d in range(DESTS):
                index = now * DESTS + d
                rows = slice(d * ROWS, (d + 1) * ROWS)
                send_b[index] = acc[rows, :] + recv_p[now, rows, :]
                if index != own and index not in added:
                    copy_b(index).start()

        for now in range(steps):
            pl.when(step == now)(functools.partial(deliver, now))
        return carry

    lax.fori_loop(0, steps, for_owners, 0)
    for index in added:
        block = send_b[index]
        for n in added[index]:
            copy_b(n).wait_recv()
            block = block + recv_r[n]
        send_b[index] = block
        copy_b(index).start()

    loop(1, ng, lambda k: copy_ga(send_c, recv_c.at[j], c_ssem, c_rsem, k).wait_recv())
    owners = jnp.concatenate([recv_c[:, 0, :], jnp.zeros((LANES - ng, LANES), F32)], axis=0).T
    per_row = min(LANES // ng, STK)
    key_rows = STK // per_row
    keys = []
    for r in range(key_rows):
        row = owners[r * per_row : r * per_row + 1]
        for n in range(1, per_row):
            at = r * per_row + n
            row = row + pltpu.roll(owners[at : at + 1], n * ng, 1)
        keys.append(row)
    send_k[...] = jnp.concatenate(keys, axis=0)
    recv_k[b] = send_k[...]

    def send_keys(k):
        off = band_offset(k)
        copy_band(send_k, recv_k.at[b], k_ssem, k_rsem, off).start()

    loop(0, nb - 1, send_keys)
    loop(0, steps, lambda s: copy_p(s).wait_send())
    loop(1, ng, lambda k: copy_ga(send_c, recv_c.at[j], c_ssem, c_rsem, k).wait_send())
    for index in direct:
        copy_b(index).wait_recv()
    becp = send_b[own]
    for index in direct:
        becp = becp + recv_b[index]
    occ = occ_row[...]
    occ = sum((pltpu.roll(occ, n * band_dev, 1) for n in range(1, LANES // band_dev)), occ)[0:1]
    lane = lax.broadcasted_iota(jnp.int32, (1, LANES), 1)
    occ = jnp.where(lane < width, occ, 0.0)
    both = jnp.concatenate([becp, pltpu.roll(becp, LANES - width, 1)], axis=0)
    hi, lo = split(both)
    occ_hi, occ_lo = split(both * occ)
    gram = dot_nt(
        jnp.concatenate([occ_hi, occ_hi, occ_lo], axis=1), jnp.concatenate([hi, lo, hi], axis=1)
    )
    rows = NH * OWN_ATOMS
    row_id = lax.broadcasted_iota(jnp.int32, (rows, rows), 0)
    col_id = lax.broadcasted_iota(jnp.int32, (rows, rows), 1)
    gram = jnp.where(row_id % OWN_ATOMS == col_id % OWN_ATOMS, gram, 0.0)
    pick = (
        lax.broadcasted_iota(jnp.int32, (rows, LANES), 0) // OWN_ATOMS
        == lax.broadcasted_iota(jnp.int32, (rows, LANES), 1)
    ).astype(BF16)
    square = dot_nn(jnp.concatenate(split(gram), axis=1), jnp.concatenate([pick, pick], axis=0))
    total = jnp.zeros((OWN_ATOMS, 2 * LANES), F32)
    for i in range(NH):
        factor = jnp.where(lane < i, 0.0, jnp.where(lane == i, 1.0, 2.0))
        factor = jnp.where(lane < NH, factor, 0.0)
        piece = square[i * OWN_ATOMS : (i + 1) * OWN_ATOMS] * factor
        piece = jnp.concatenate([piece, jnp.zeros((OWN_ATOMS, LANES), F32)], axis=1)
        shift = i * NH - i * (i - 1) // 2 - i
        total = total + (pltpu.roll(piece, shift, 1) if shift else piece)
    folded = total[:4, LANES:] + pltpu.roll(total[4:, LANES:], LANES // 2, 1)
    total = jnp.concatenate([total[:, :LANES], folded], axis=0)
    send_z[...] = total
    recv_z[0] = total

    def send_band(k):
        off = band_offset(k)
        copy_band(send_z, recv_z.at[off], z_ssem, z_rsem, off).start()

    loop(0, nb - 1, send_band)

    column = jnp.zeros((1, LANES), F32)
    for n in range(STK):
        column = jnp.where(lane == n, stick[n], column)
    stick_x = jnp.floor((column + 0.5) * (1.0 / nx))
    stick_y = column - stick_x * nx
    stick_x = stick_x + (b * NXB).astype(F32)
    lane_tiles = phase.shape[2] // LANES
    period = min(nz // math.gcd(nz, LANES), lane_tiles)
    heights = []
    for q in range(period):
        g = (lane + q * LANES).astype(F32)
        heights.append(g - nz * jnp.floor((g + 0.5) * (1.0 / nz)))

    def phases(r):
        source = 2 * near_chip(r // 2) + r % 2
        atom = pl.ds(pl.multiple_of(source * 8, 8), 8)
        p1, p2, p3 = (colb[n, atom, :] for n in range(3))
        rows = pl.ds(pl.multiple_of(r * 8, 8), 8)
        flat = cos_sin(turns_of(p1 * stick_x + p2 * stick_y, nx))
        flat = [[jnp.broadcast_to(x[:, n : n + 1], (8, LANES)) for n in range(STK)] for x in flat]
        tall = [cos_sin(turns_of(p3 * z, nz)) for z in heights]
        for t in range(lane_tiles):
            low = t * LANES // nz
            high = min(((t + 1) * LANES - 1) // nz, STK - 1)
            c, s = (x[low] for x in flat)
            for n in range(low + 1, high + 1):
                before = lane < n * nz - t * LANES
                c, s = jnp.where(before, c, flat[0][n]), jnp.where(before, s, flat[1][n])
            cz, sz = tall[t % period]
            lanes = slice(t * LANES, (t + 1) * LANES)
            phase[0, rows, lanes] = c * cz - s * sz
            phase[1, rows, lanes] = s * cz + c * sz

    loop(0, atoms // 8, phases)
    for index in sent:
        copy_b(index).wait_send()
    def wait_band(k):
        off = band_offset(k)
        copy_band(send_z, recv_z.at[off], z_ssem, z_rsem, off).wait_recv()

    loop(0, nb - 1, wait_band)
    total = recv_z[0]
    for n in range(1, nb):
        total = total + recv_z[n]
    send_a[...] = total
    recv_a[j] = total
    for k in range(1, ng):
        copy_ga(send_a, recv_a.at[j], a_ssem, a_rsem, k).start()
    for copy in local[7:]:
        copy.wait()

    even = even_ref[0:1, :]
    odd = even_ref[1:2, :]
    depth = SPECIES * PAIRS
    part = last + 1
    augrow[...] = jnp.zeros(augrow.shape, F32)

    def arrive(k):
        copy_ga(send_a, recv_a.at[j], a_ssem, a_rsem, k).wait_recv()

    crowd = min(4, part)

    def weights(n):
        for index in range(crowd):
            index = index + n * crowd
            q = near_chip(index)

            @pl.when(index == 0)
            def _():
                arrive((j - (chip * 2 + 1 - core)) % ng)

            @pl.when(index > 0)
            def _():
                arrive((j - 2 * q) % ng)
                arrive((j - 2 * q - 1) % ng)

        for index in range(crowd):
            weigh(index + n * crowd)

    def weigh(index):
        q = near_chip(index)
        values = []
        for n in range(2):
            got = recv_a[2 * q + n]
            first, rest = got[:OWN_ATOMS], got[OWN_ATOMS:]
            rest = jnp.concatenate([rest, pltpu.roll(rest, LANES // 2, 1)], axis=0)
            values.append(jnp.concatenate([first, rest], axis=1))
        values = jnp.concatenate(values, axis=0)
        position = lax.broadcasted_iota(jnp.int32, values.shape, 1)
        values = jnp.where(position < PAIRS, values, 0.0)
        values = jnp.concatenate([values, jnp.zeros((16, KLANES - 2 * LANES), F32)], axis=1)
        atom = pl.ds(pl.multiple_of(q * 16, 16), 16)
        first_im = (index // part + 1) * (part * 16)
        rows = pl.ds(pl.multiple_of(first_im - part * 16 + index * 16, 16), 16)
        kind = wide(colb[3, atom, :], KLANES)
        placed = jnp.where(kind < 0.5, values, 0.0)
        for n in range(1, SPECIES):
            moved = pltpu.roll(values, n * PAIRS, 1)
            placed = jnp.where((kind > n - 0.5) & (kind < n + 0.5), moved, placed)
        wmix[rows, :] = (placed * even).astype(BF16)
        rows = pl.ds(pl.multiple_of(first_im + index * 16, 16), 16)
        wmix[rows, :] = (placed * odd).astype(BF16)

    def half(h):
        loop(part // crowd * h, part // crowd * (h + 1), weights)
        rows = pl.ds(pl.multiple_of(h * part * 16, part * 16), part * 16)
        both_rows = pl.ds(pl.multiple_of(h * part * 32, part * 32), part * 32)
        for t in range(NPL):
            lanes = slice(t * ct, (t + 1) * ct)
            table = tab[:, lanes]
            amp = dot_nn(wmix[both_rows, :depth], table)
            amp_re, amp_im = amp[: part * 16], amp[part * 16 :]
            c, s = phase[0, rows, lanes], phase[1, rows, lanes]
            augrow[0:1, lanes] += jnp.sum(amp_re * c + amp_im * s, axis=0, keepdims=True)
            augrow[1:2, lanes] += jnp.sum(amp_im * c - amp_re * s, axis=0, keepdims=True)

    loop(0, (last + 1) // part, half)

    pad_z = tz.shape[2] // 2
    wide_row = round_up(columns, LANES)
    shape = (STK, pad_z)
    slot_id = lax.broadcasted_iota(jnp.int32, shape, 0)
    lane_id = lax.broadcasted_iota(jnp.int32, shape, 1)
    values = []
    for n in range(2):
        row = augrow[n : n + 1, :]
        picked = jnp.zeros(shape, F32)
        for t in range(STK):
            moved = pltpu.roll(row, wide_row - t * nz, 1) if t else row
            picked = jnp.where(slot_id == t, moved[:, :pad_z], picked)
        values.append(jnp.where(lane_id < nz, picked, 0.0))
    a_re, a_im = values
    pair = jnp.concatenate(
        [jnp.concatenate([a_re, -a_im], axis=1), jnp.concatenate([a_im, a_re], axis=1)], axis=0
    )
    hi, lo = split(jnp.concatenate([pair, jnp.zeros((LANES - 2 * STK, 2 * pad_z), F32)], axis=0))
    planes = dot_nt(tz[0], hi) + dot_nt(tz[0], lo) + dot_nt(tz[1], hi)
    plane_id = lax.broadcasted_iota(jnp.int32, planes.shape, 0) % 8
    line = jnp.where(plane_id == 0, planes, 0.0)
    for p in range(1, NPL):
        line = line + pltpu.roll(jnp.where(plane_id == p, planes, 0.0), p * 2 * STK, 1)
    send_v[:, 0, :] = jnp.sum(line.reshape(ng, 8, LANES), axis=1)
    straight = (5, -5, 0, 1, -1, 2, -2) if nb == 16 else tuple(range(nb))
    rows_sent = [ng - 1 if off == 0 else ng for off in straight]
    recv_v[straight.index(0), j] = send_v[j]

    def copy_v(n, k):
        place = lax.rem(j + k, ng)
        return pltpu.make_async_remote_copy(
            send_v.at[place],
            recv_v.at[n, j],
            v_ssem.at[n],
            v_rsem.at[n],
            device_id=(lax.rem(b + nb + straight[n], nb), place),
            device_id_type=MESH,
        )

    def copy_rows(n):
        rows = recv_v.at[n, pl.ds(0, rows_sent[n])]
        return pltpu.make_async_remote_copy(
            rows,
            rows,
            v_ssem.at[n],
            v_rsem.at[n],
            device_id=(lax.rem(b + nb + 1, nb), j),
            device_id_type=MESH,
        )

    for n, off in enumerate(straight):
        for k in range(ng - rows_sent[n], ng):
            copy_v(n, k).start()

    def end_band(k):
        off = band_offset(k)
        copy_band(send_z, recv_z.at[off], z_ssem, z_rsem, off).wait_send()

    def end_ga(k):
        copy_ga(send_a, recv_a.at[j], a_ssem, a_rsem, k).wait_send()

    def wait_keys(k):
        off = band_offset(k)
        copy_band(send_k, recv_k.at[b], k_ssem, k_rsem, off).wait_recv()
        copy_band(send_k, recv_k.at[b], k_ssem, k_rsem, off).wait_send()

    loop(0, nb - 1, wait_keys)
    keys = jnp.concatenate([recv_k[n] for n in range(nb)], axis=0)
    slot_x = jnp.floor((keys + 0.5) * (1.0 / nx))
    slot_y = keys - slot_x * nx
    spare = jnp.zeros((LANES - nb * key_rows, LANES), F32)
    slot_y = jnp.concatenate([slot_y, spare], axis=0).T
    row_x = lax.broadcasted_iota(jnp.int32, (16, LANES), 0).astype(F32)
    held = per_row * ng
    for n in range(nb):
        for r in range(key_rows):
            at = n * key_rows + r
            hot = jnp.where(row_x == slot_x[at : at + 1], 1.0, 0.0).astype(BF16)
            onehot[n, :, r * held : (r + 1) * held] = hot[:, :held]
            onehot[n, :, slots + r * held : slots + (r + 1) * held] = hot[:, :held]
            ey[n, 0, r * held : (r + 1) * held, :] = jnp.broadcast_to(
                slot_y[:held, at : at + 1], (held, LANES)
            )
    lane_y = (lax.broadcasted_iota(jnp.int32, (1, LANES), 1) % 16).astype(F32) + (b * NXB).astype(F32)
    some_rows = 64

    def y_phases(r):
        n = r // (slots // some_rows)
        rows = pl.ds(pl.multiple_of(r % (slots // some_rows) * some_rows, some_rows), some_rows)
        c, s = cos_sin(turns_of(ey[n, 0, rows, :] * lane_y, nx))
        ey[n, 0, rows, :] = c
        ey[n, 1, rows, :] = s

    loop(0, nb * (slots // some_rows), y_phases)
    loop(0, nb - 1, end_band)
    loop(1, ng, end_ga)

    hops = {}
    if nb == 16:
        hops = {5 + n: (5, n) for n in (3, 2, -2, 1, -1)}
        hops.update({-5 + n: (-5, n) for n in (2, -2, 1, -1)})

    def copy_y(off):
        back, hop = hops[off]
        slot = recv_y.at[(b + nb - back) % nb]
        return pltpu.make_async_remote_copy(
            slot,
            slot,
            y_ssem.at[off % nb],
            y_rsem.at[off % nb],
            device_id=((b + nb + hop) % nb, j),
            device_id_type=MESH,
        )

    def pass_on(back):
        for off in hops:
            if hops[off][0] == back:
                copy_y(off).start()

    group = lax.broadcasted_iota(jnp.int32, (2 * ng, LANES), 1) // 16 * 16

    def take_blocks(sources):
        values = jnp.concatenate([recv_y[source] for source in sources], axis=0)
        pick = group[: len(sources) * ng]
        picked = [jnp.take_along_axis(values, pick + n, axis=1) for n in range(2 * STK)]
        for k, source in enumerate(sources):
            own = [x[k * ng : (k + 1) * ng] for x in picked]
            v_re, v_im = jnp.concatenate(own[:STK], axis=0), jnp.concatenate(own[STK:], axis=0)
            c, s = ey[source, 0], ey[source, 1]
            z = jnp.concatenate([v_re * c - v_im * s, v_re * s + v_im * c], axis=1)
            rows = pl.ds(pl.multiple_of(source * 16, 16), 16)
            field[rows, :] = dot_nn(onehot[source], jnp.concatenate(split(z), axis=0))

    def source_of(off):
        return lax.rem(b + nb - off, nb)

    def arrived(off):
        n = straight.index(off)
        copy_rows(n).wait_recv()
        recv_y[source_of(off)] = recv_v[n, :, 0, :]

    def take_all(offs):
        for n in range(0, len(offs), 2):
            take_blocks([source_of(off) for off in offs[n : n + 2]])

    if nb == 16:
        arrived(0)
        take_all((0,))
        for off in (5, -5):
            arrived(off)
            pass_on(off)
        for off in (1, -1, 2, -2):
            arrived(off)
        take_all((5, -5, 1, -1, 2, -2))
    else:
        for off in straight:
            arrived(off)
        take_all(straight)
    for off in hops:
        copy_y(off).wait_recv()
    take_all(tuple(hops))

    turned = field[...].T
    f_re, f_im = turned[:LANES], turned[LANES:]
    left = jnp.concatenate(
        [jnp.concatenate([f_re, -f_im], axis=1), jnp.concatenate([f_im, f_re], axis=1)], axis=0
    )
    hi, lo = split(left)
    result = dot_nn(jnp.concatenate([hi, lo], axis=0), tx[0])
    result = result[: 2 * LANES] + result[2 * LANES :] + dot_nn(hi, tx[1])
    for n in range(2):
        for p in range(NPL):
            first = n * LANES + p * 16
            out_ref[n, p] = result[first : first + NXB, :nx]

    for off in hops:
        copy_y(off).wait_send()
    for n in range(len(straight)):
        copy_rows(n).wait_send()


def both_parts(table):
    hi = table.astype(jnp.bfloat16)
    lo = (table - hi.astype(np.float64)).astype(jnp.bfloat16)
    return np.stack([hi, lo])


def tables(nb, ng):
    nx, nz = NXB * nb, NPL * ng
    pad_z = round_up(nz, LANES)
    plane = np.arange(8 * ng) // 8 * NPL + np.arange(8 * ng) % 8
    angle = (plane[:, None] * np.arange(nz)[None, :] % nz) * (2 * np.pi / nz)
    real = (np.arange(8 * ng) % 8 < NPL)[:, None]
    tz = np.zeros((8 * ng, 2 * pad_z))
    tz[:, :nz] = np.where(real, np.cos(angle), 0.0)
    tz[:, pad_z : pad_z + nz] = np.where(real, np.sin(angle), 0.0)
    pad_x = round_up(nx, LANES)
    row = np.arange(16 * nb)
    x = row // 16 * NXB + row % 16
    angle = (x[:, None] * np.arange(nx)[None, :] % nx) * (2 * np.pi / nx)
    real = (row % 16 < NXB)[:, None]
    tx = np.zeros((2 * 16 * nb, pad_x))
    tx[: 16 * nb, :nx] = np.where(real, np.cos(angle), 0.0)
    tx[16 * nb :, :nx] = np.where(real, np.sin(angle), 0.0)
    first, second = np.triu_indices(NH)
    ell = np.array(ELL)
    parity = np.tile((ell[first] + ell[second]) % 2, SPECIES)
    even = np.zeros((2, KLANES), np.float32)
    even[0, : SPECIES * PAIRS] = 1 - parity
    even[1, : SPECIES * PAIRS] = -parity
    return (
        jnp.asarray(both_parts(tz)),
        jnp.asarray(both_parts(tx)),
        jnp.asarray(even),
    )


def on_device(
    waves, occupations, beta_table, wave_miller, atom_kinds, atom_sites, aug_table, stick_columns
):
    nb, ng = lax.axis_size("band"), lax.axis_size("ga")
    nx, nz = NXB * nb, NPL * ng
    atoms, slots = OWN_ATOMS * ng, STK * ng
    wave_count = waves.shape[2]
    gt_lanes = min(256, wave_count)
    tiles = wave_count // gt_lanes
    columns = STK * nz
    steps = ng // 2 // DESTS
    chips = ng // 2
    key_rows = STK // min(LANES // ng, STK)
    tz, tx, even = tables(nb, ng)
    vmem = pl.BlockSpec(memory_space=pltpu.VMEM)
    hbm = pl.BlockSpec(memory_space=pltpu.HBM)
    dma = pltpu.SemaphoreType.DMA
    return pl.pallas_call(
        functools.partial(kernel, nb, ng, gt_lanes),
        out_shape=jax.ShapeDtypeStruct((2, NPL, NXB, nx), F32),
        in_specs=[hbm] * 11,
        out_specs=vmem,
        scratch_shapes=[
            pltpu.VMEM(waves.shape, BF16),
            pltpu.VMEM((1, waves.shape[1]), F32),
            pltpu.VMEM(beta_table.shape, F32),
            pltpu.VMEM(wave_miller.shape, jnp.int32),
            pltpu.VMEM((1, atoms), jnp.int32),
            pltpu.VMEM(atom_sites.shape, jnp.int32),
            pltpu.SMEM(stick_columns.shape, jnp.int32),
            pltpu.VMEM(even.shape, F32),
            pltpu.VMEM(aug_table.shape, BF16),
            pltpu.VMEM(tz.shape, BF16),
            pltpu.VMEM(tx.shape, BF16),
            dma((11,)),
            pltpu.VMEM((4, atoms, LANES), F32),
            pltpu.VMEM((atoms, LANES), jnp.int32),
            pltpu.VMEM((NH, 8, wave_count), F32),
            pltpu.VMEM((8, wave_count), F32),
            pltpu.VMEM((tiles, 4 * gt_lanes, LANES), BF16),
            pltpu.VMEM((DESTS * ROWS, LANES), F32),
            pltpu.VMEM((steps, DESTS * ROWS, LANES), F32),
            pltpu.VMEM((steps, DESTS * ROWS, LANES), F32),
            pltpu.VMEM((chips, ROWS, LANES), F32),
            pltpu.VMEM((chips, ROWS, LANES), F32),
            pltpu.VMEM((6, ROWS, LANES), F32),
            pltpu.VMEM((1, LANES), F32),
            pltpu.VMEM((ng, 1, LANES), F32),
            pltpu.VMEM((8, LANES), F32),
            pltpu.VMEM((2, atoms, round_up(columns, LANES)), F32),
            pltpu.VMEM((FOLD, LANES), F32),
            pltpu.VMEM((nb, FOLD, LANES), F32),
            pltpu.VMEM((FOLD, LANES), F32),
            pltpu.VMEM((ng, FOLD, LANES), F32),
            pltpu.VMEM((2 * atoms, KLANES), BF16),
            pltpu.VMEM((8, round_up(columns, LANES)), F32),
            pltpu.VMEM((ng, 1, LANES), F32),
            pltpu.VMEM((min(nb, 7), ng, 1, LANES), F32),
            pltpu.VMEM((nb, ng, LANES), F32),
            pltpu.VMEM((nb, 2, slots, LANES), F32),
            pltpu.VMEM((nb, 16, 2 * slots), BF16),
            pltpu.VMEM((key_rows, LANES), F32),
            pltpu.VMEM((nb, key_rows, LANES), F32),
            pltpu.VMEM((nb * 16, 2 * LANES), F32),
            dma((steps,)),
            dma((steps,)),
            dma((chips,)),
            dma((chips,)),
            dma((6,)),
            dma((ng,)),
            dma((ng,)),
            dma((nb,)),
            dma((nb,)),
            dma((ng,)),
            dma((ng,)),
            dma((ng,)),
            dma((ng,)),
            dma((nb,)),
            dma((nb,)),
            dma((nb,)),
            dma((nb,)),
        ],
        compiler_params=pltpu.CompilerParams(
            collective_id=0, has_side_effects=True, vmem_limit_bytes=VMEM_LIMIT
        ),
    )(
        waves,
        occupations[None],
        beta_table,
        wave_miller,
        atom_kinds[None],
        atom_sites,
        aug_table,
        stick_columns,
        tz,
        tx,
        even,
    )


def solution(mesh):
    in_specs = (
        P(None, "band", "ga"),
        P("band"),
        P(None, "ga"),
        P(None, "ga"),
        P(),
        P(),
        P(None, ("band", "ga")),
        P(("band", "ga")),
    )
    out_specs = P(None, "ga", "band", None)
    return jax.shard_map(
        on_device, mesh=mesh, in_specs=in_specs, out_specs=out_specs, check_vma=False
    )
```
